32 devices in a mesh: dp: 8 (over z, y), tp: 4 (over x, core).
Axes of the slice: x: 2, y: 2, z: 4, core: 2. Of those that a mesh axis runs over, the one named last changes fastest.
Arguments:
- tokens: bfloat16 [768, 2880], P('dp', 'tp'), may hold values from -100 to 100
- attn_gain: float32 [2880], replicated, may hold values from 0.1 to 1.9
- w_query: bfloat16 [2880, 2048], P(None, 'tp'), may hold values from -0.109375 to 0.109375
- w_keyvalue: bfloat16 [2880, 8, 128], P(None, 'tp'), may hold values from -0.109375 to 0.109375
- attn_sinks: float32 [32], P('tp'), may hold values from 2 to 6
- w_out: bfloat16 [2048, 2880], P('tp'), may hold values from -0.125 to 0.125
- window_cache: bfloat16 [768, 8, 128, 128], P('dp', 'tp'), may hold values from -1000 to 1000
- positions: int32 [768], P('dp'), may hold values from 0 to 511
- moe_gain: float32 [2880], replicated, may hold values from 0.1 to 1.9
- router: bfloat16 [2880, 8], P('tp'), may hold values from -0.109375 to 0.109375
- gate_up: bfloat16 [8, 2880, 2, 2880], P('dp', None, None, 'tp'), may hold values from -0.109375 to 0.109375
- w_down: bfloat16 [8, 2880, 2880], P('dp', None, 'tp'), may hold values from -0.109375 to 0.109375
- expert_ids: int32 [768, 4], P('dp'), may hold values from 0 to 7, all different within a row; in each aligned block of 96 rows (0 to 95, 96 to 191, ...) at most 96 rows name the same one
Outputs:
- layer_out: float32 [768, 2880], P('dp', 'tp')
The draws below stay inside these ranges and needn't reach their ends.
Inputs may be any that keep to these rules, and one draw needn't show every extreme that they name: `expert_ids`: each row names 4 different experts. Within the rows of one index of dp no expert is named by more than 96 rows, a bound that some of these blocks reach.
All inputs are finite; a program needn't handle non-finite values.
Results may differ from the reference program's by a relative error of at most 0.0066.
Values may be sent and summed in bfloat16 or wider, within the bound.
A program may use at most 128 MiB of HBM per device.

```python
import math
import jax
import jax.numpy as jnp
import numpy as np
from jax import lax

D = 2880
QH = 32
KVH = 8
HD = 64
WINDOW = 128
TOP = 4
FF = 2880
TOK_DEV = 96
EXPERTS = 8
TOKENS = 768
CAP = 96
N_DP = 8


def draw_tokens(key, part):
    base_key, col_key, row_key = jax.random.split(key, 3)
    places = jnp.arange(D, dtype=jnp.float32) / D
    col_scale = jnp.power(10.0, 0.5 * places + 0.5 * jax.random.uniform(col_key, (D,)))
    base = jnp.clip(jax.random.normal(base_key, (TOKENS, D)), -4.0, 4.0)
    row_scale = jnp.power(10.0, jax.random.uniform(row_key, (TOKENS, 1)))
    return (0.1 * base * row_scale * col_scale[None, :]).astype(jnp.bfloat16)


def draw_window_cache(key, part):
    normal_key = jax.random.fold_in(key, 0)
    entries = jnp.clip(jax.random.normal(normal_key, (TOKENS, KVH, WINDOW, 2 * HD)), -6.0, 6.0)
    return entries.astype(jnp.bfloat16)


def touch_ends(result, key, smallest, high):
    spot = [jax.random.randint(jax.random.fold_in(key, axis), (), 0, length) for axis, length in enumerate(result.shape)]
    main_axis = result.shape.index(max(result.shape))
    next_to = spot[:main_axis] + [(spot[main_axis] + 1) % result.shape[main_axis]] + spot[main_axis + 1:]
    return result.at[tuple(spot)].set(smallest).at[tuple(next_to)].set(high)


def block_levels(key, extent, shards, smallest, high):
    loudness, own = 1.0, jax.random.fold_in(key, 6)
    for dim, parts in shards:
        draws = jnp.exp(jax.random.uniform(jax.random.fold_in(own, dim), (parts,), jnp.float32, smallest / len(shards), high / len(shards)))
        loudness = loudness * jnp.repeat(draws, extent[dim] // parts).reshape([-1 if axis == dim else 1 for axis in range(len(extent))])
    return loudness


def routed_block(own_key, own, number, rows, number_of, top, reach, slope):
    ranking = jax.random.permutation(own_key, number_of)
    crowded, ordinary = load_shares(number_of, rows * top, reach, slope, True), load_shares(number_of, rows * top, reach, slope, False)
    places = jnp.arange(number_of)

    def named(sizes, turn):
        used = int((sizes > 0).sum())
        fixed = max(1, used // 4)
        moved = fixed + (places - fixed + turn * (used - fixed)) % max(1, number_of - fixed)
        return jnp.zeros((number_of,), jnp.int32).at[ranking[jnp.where(places < fixed, places, moved)]].set(jnp.asarray(sizes, jnp.int32))

    sizes = jnp.where(number % 4 == 0, named(crowded, number // 4), named(ordinary, number - number // 4 - 1))
    mixed = jax.random.permutation(jax.random.fold_in(own, 3), number_of)
    donor, sink = mixed[0:number_of // 2 * 2:2], mixed[1:number_of // 2 * 2:2]
    slack = jnp.minimum(sizes[donor] - 1, reach - sizes[sink]) // 2
    slack = jnp.where((donor == ranking[0]) | (sink == ranking[0]) | (sizes[sink] == 0), 0, jnp.maximum(slack, 0))
    moved = jax.random.randint(jax.random.fold_in(own, 4), (number_of // 2,), 0, 1 << 20) % (slack + 1)
    sizes = sizes.at[donor].add(-moved).at[sink].add(moved)
    items = jnp.searchsorted(jnp.cumsum(sizes), jnp.arange(rows * top), side="right").astype(jnp.int32)
    listing = items.reshape(top, rows).T
    listing = listing[jax.random.permutation(jax.random.fold_in(own, 1), rows)]
    turn = jax.random.randint(jax.random.fold_in(own, 2), (rows, 1), 0, top)
    return jnp.take_along_axis(listing, (jnp.arange(top)[None, :] + turn) % top, axis=1)


def load_shares(number_of, total, limit, lean, full):
    weights = [(1 << 20) // math.isqrt(rank ** lean) + 1 for rank in range(1, number_of + 1)]
    largest = limit if full else min(limit, max(-(-total // number_of), total * weights[0] // sum(weights)))
    least = 1 if total - largest >= number_of - 1 else 0
    counts, surplus = [largest] + [least] * (number_of - 1), total - largest - least * (number_of - 1)
    while surplus > 0:
        candidates = [i for i in range(1, number_of) if counts[i] < largest] or [i for i in range(1, number_of) if counts[i] < limit]
        mass, left = sum([weights[i] for i in candidates]), surplus
        for i in candidates:
            more = min(limit - counts[i], max(1, left * weights[i] // mass), surplus)
            counts[i] = counts[i] + more
            surplus = surplus - more
    return np.array(counts)


def gaussian(stream_key, shape, spread, most, cuts=(), kind=jnp.bfloat16):
    drawn = spread * jax.random.normal(stream_key, shape, jnp.float32)
    if cuts:
        drawn = drawn * block_levels(stream_key, shape, cuts, -0.22, 0.18)
    return jnp.clip(drawn, -most, most).astype(kind)


def setup_inputs(seed: int = 0) -> dict:
    splits = jax.random.split(jax.random.key(seed), 14)
    tokens = draw_tokens(jax.random.fold_in(splits[13], 71), 0)
    attn_gain = jnp.clip(1.0 + 0.18 * jax.random.normal(splits[1], (D,), jnp.float32), 0.1, 1.9)
    w_query = gaussian(splits[2], (D, QH * HD), D ** -0.5, 0.109375, ((1, 4),))
    w_keyvalue = gaussian(splits[3], (D, KVH, 2 * HD), D ** -0.5, 0.109375, ((1, 4),))
    attn_sinks = jnp.clip(2.0 + 4.0 * jax.random.uniform(splits[4], (QH,), jnp.float32) ** block_levels(splits[4], (QH,), ((0, 4),), -0.2, 0.2), 2.0, 6.0)
    w_out = gaussian(splits[5], (QH * HD, D), (QH * HD) ** -0.5, 0.125, ((0, 4),))
    window_cache = draw_window_cache(jax.random.fold_in(splits[13], 71), 0)
    positions = touch_ends(jax.random.randint(splits[7], (TOKENS,), 0, 4 * WINDOW), jax.random.fold_in(splits[7], 1), 0, (4 * WINDOW) - 1).astype(jnp.int32)
    moe_gain = jnp.clip(1.0 + 0.18 * jax.random.normal(splits[8], (D,), jnp.float32), 0.1, 1.9)
    router = gaussian(splits[9], (D, EXPERTS), D ** -0.5, 0.109375, ((0, 4),))
    gate_up = gaussian(splits[10], (EXPERTS, D, 2, FF), D ** -0.5, 0.109375, ((0, 8), (3, 4)))
    w_down = gaussian(splits[11], (EXPERTS, FF, D), FF ** -0.5, 0.109375, ((0, 8), (2, 4)))
    expert_ids_keys = jax.random.split(jax.random.fold_in(splits[12], 1), TOKENS // TOK_DEV)
    expert_ids_turns = jax.random.permutation(jax.random.fold_in(splits[12], 3), TOKENS // TOK_DEV)
    expert_ids = jax.vmap(lambda own, number: routed_block(jax.random.fold_in(splits[12], 2), own, number, TOK_DEV, EXPERTS, TOP, CAP, 2))(expert_ids_keys, expert_ids_turns).reshape((TOKENS, TOP))
    return {"tokens": tokens, "attn_gain": attn_gain, "w_query": w_query, "w_keyvalue": w_keyvalue, "attn_sinks": attn_sinks, "w_out": w_out, "window_cache": window_cache, "positions": positions, "moe_gain": moe_gain, "router": router, "gate_up": gate_up, "w_down": w_down, "expert_ids": expert_ids}


norm_eps = 1e-05
rope_base = 150000.0
glu_alpha = 1.702

def rope_tables(positions, head_size):
    half_size = head_size // 2
    exponent = jnp.arange(half_size, dtype=jnp.float32) * (2.0 / head_size)
    inverse = jnp.power(jnp.float32(rope_base), -exponent)
    angles = positions.astype(jnp.float32)[:, None] * inverse[None, :]
    return (jnp.cos(angles), jnp.sin(angles))

def rotate(values, cosine, sine_table):
    half_size = values.shape[-1] // 2
    first_half = values[..., :half_size]
    second_half = values[..., half_size:]
    return jnp.concatenate([first_half * cosine - second_half * sine_table, second_half * cosine + first_half * sine_table], axis=-1)

def reference(tokens, attn_gain, w_query, w_keyvalue, attn_sinks, w_out, window_cache, positions, moe_gain, router, gate_up, w_down, expert_ids):
    seq_count, full_width = tokens.shape
    head_size = w_keyvalue.shape[2] // 2
    kv_heads = w_keyvalue.shape[1]
    q_heads = w_query.shape[1] // head_size
    group_size = q_heads // kv_heads
    window = window_cache.shape[2]
    tok_wide = tokens.astype(jnp.float32)
    attn_mean = lax.optimization_barrier(jnp.mean(tok_wide * tok_wide, axis=1, keepdims=True))
    normed = (tok_wide * lax.rsqrt(attn_mean + norm_eps) * attn_gain[None, :]).astype(jnp.bfloat16)
    queries = jnp.dot(normed, w_query, preferred_element_type=jnp.float32).reshape(seq_count, q_heads, head_size)
    fresh_rows = jnp.dot(normed, w_keyvalue.reshape(full_width, kv_heads * 2 * head_size), preferred_element_type=jnp.float32)
    fresh_rows = fresh_rows.reshape(seq_count, kv_heads, 2 * head_size)
    cosine, sine_table = rope_tables(positions, head_size)
    rot_queries = rotate(queries, cosine[:, None, :], sine_table[:, None, :]).astype(jnp.bfloat16)
    new_key = rotate(fresh_rows[..., :head_size], cosine[:, None, :], sine_table[:, None, :])
    new_entry = jnp.concatenate([new_key, fresh_rows[..., head_size:]], axis=-1).astype(jnp.bfloat16)
    slot_ids = jnp.arange(window, dtype=jnp.int32)
    is_current = slot_ids[None, :] == (positions % window)[:, None]
    cache_now = jnp.where(is_current[:, None, :, None], new_entry[:, :, None, :], window_cache)
    is_valid = (positions[:, None] - slot_ids[None, :]) % window <= positions[:, None]
    score_scale = head_size ** (-0.5)

    def attend_head(inputs):
        head_cache, head_query, head_sinks = inputs
        key_part = head_cache[..., :head_size].astype(jnp.float32)
        value_part = head_cache[..., head_size:].astype(jnp.float32)
        scores = jnp.einsum('sgh,swh->sgw', head_query.astype(jnp.float32), key_part) * score_scale
        scores = jnp.where(is_valid[:, None, :], scores, -jnp.inf)
        sink_col = head_sinks[None, :, None]
        peak_score = jnp.maximum(lax.optimization_barrier(jnp.max(scores, axis=-1, keepdims=True)), sink_col)
        raised = jnp.exp(scores - peak_score)
        denominator = lax.optimization_barrier(jnp.sum(raised, axis=-1, keepdims=True)) + jnp.exp(sink_col - peak_score)
        prob_bf = (raised / denominator).astype(jnp.bfloat16)
        return jnp.einsum('sgw,swh->sgh', prob_bf.astype(jnp.float32), value_part).astype(jnp.bfloat16)
    grouped = rot_queries.reshape(seq_count, kv_heads, group_size, head_size)
    attended = lax.map(attend_head, (jnp.transpose(cache_now, (1, 0, 2, 3)), jnp.transpose(grouped, (1, 0, 2, 3)), attn_sinks.reshape(kv_heads, group_size)))
    attended = jnp.transpose(attended, (1, 0, 2, 3)).reshape(seq_count, q_heads * head_size)
    residual = tok_wide + jnp.dot(attended, w_out, preferred_element_type=jnp.float32)
    moe_mean = lax.optimization_barrier(jnp.mean(residual * residual, axis=1, keepdims=True))
    scaled = residual * lax.rsqrt(moe_mean + norm_eps) * moe_gain[None, :]
    logits = jnp.dot(scaled, router.astype(jnp.float32), precision=lax.Precision.HIGHEST)
    hidden_rows = scaled.astype(jnp.bfloat16)
    experts = router.shape[1]
    expert_iota = jnp.arange(experts, dtype=jnp.int32)
    chosen = expert_ids[:, :, None] == expert_iota[None, None, :]
    picked = lax.optimization_barrier(jnp.sum(jnp.where(chosen, logits[:, None, :], 0.0), axis=-1))
    raised_logits = jnp.exp(picked)
    route_weights = raised_logits / lax.optimization_barrier(jnp.sum(raised_logits, axis=1, keepdims=True))
    per_group = seq_count // N_DP
    group_ids = expert_ids.reshape(N_DP, per_group * TOP)
    onehot = (group_ids[:, :, None] == expert_iota[None, None, :]).astype(jnp.int32)
    earlier = jnp.cumsum(onehot, axis=1) - onehot
    slot_of = lax.optimization_barrier(jnp.sum(earlier * onehot, axis=2))
    column = (jnp.arange(N_DP, dtype=jnp.int32)[:, None] * CAP + slot_of).reshape(-1).astype(jnp.int32)
    expert_flat = group_ids.reshape(-1).astype(jnp.int32)
    repeated = jnp.repeat(hidden_rows, TOP, axis=0)
    buffer_rows = jnp.zeros((experts, N_DP * CAP, full_width), jnp.bfloat16).at[expert_flat, column].set(repeated)
    ff_width = w_down.shape[1]

    def one_expert(inputs):
        block_rows, weights_in, weights_down = inputs
        mixed_in = jnp.dot(block_rows, weights_in.reshape(full_width, 2 * ff_width), preferred_element_type=jnp.float32)
        gate_part = mixed_in[:, :ff_width]
        up_part = mixed_in[:, ff_width:]
        act_rows = (gate_part * jax.nn.sigmoid(glu_alpha * gate_part) * (up_part + 1.0)).astype(jnp.bfloat16)
        return jnp.dot(act_rows, weights_down, preferred_element_type=jnp.float32).astype(jnp.bfloat16)
    outputs = lax.map(one_expert, (buffer_rows, gate_up, w_down))
    gathered = outputs[expert_flat, column].reshape(seq_count, TOP, full_width).astype(jnp.float32)
    combined = lax.optimization_barrier(jnp.sum(route_weights[:, :, None] * gathered, axis=1))
    return residual + combined
```

```python
import functools
import math

import jax
import jax.numpy as jnp
from jax import lax
from jax.experimental import pallas as pl
from jax.experimental.pallas import tpu as pltpu
from jax.sharding import PartitionSpec as P

norm_eps = 1e-05
rope_base = 150000.0
glu_alpha = 1.702


def rope_tables(positions, head_size):
    half_size = head_size // 2
    exponent = jnp.arange(half_size, dtype=jnp.float32) * (2.0 / head_size)
    inverse = jnp.power(jnp.float32(rope_base), -exponent)
    angles = positions.astype(jnp.float32)[:, None] * inverse[None, :]
    return (jnp.cos(angles), jnp.sin(angles))


def rotate(values, cosine, sine_table):
    half_size = values.shape[-1] // 2
    first_half = values[..., :half_size]
    second_half = values[..., half_size:]
    return jnp.concatenate(
        [
            first_half * cosine - second_half * sine_table,
            second_half * cosine + first_half * sine_table,
        ],
        axis=-1,
    )


MESH = pl.DeviceIdType.MESH
CORES = 2


def greet(partners):
    barrier = pltpu.get_barrier_semaphore()
    for partner in partners:
        pl.semaphore_signal(barrier, inc=1, device_id=partner, device_id_type=MESH)
    pl.semaphore_wait(barrier, len(partners))


def feature_gather_kernel(tp, chunks, x_ref, out_ref, buf, own_sem, send_x, send_c, recv):
    chips = tp // CORES
    dp_id = lax.axis_index("dp")
    me = lax.axis_index("tp")
    core = lax.rem(me, CORES)
    chip = me // CORES
    rows, cols = x_ref.shape
    step = rows // chunks
    twin = (dp_id, chip * CORES + (1 - core))
    others = [lax.rem(chip + d, chips) * CORES + core for d in range(1, chips)]
    sources = [lax.rem(chip + chips - d, chips) * CORES + core for d in range(1, chips)]
    own = pltpu.make_async_copy(x_ref, buf.at[me], own_sem)
    own.start()
    greet([twin] + [(dp_id, other) for other in others])

    def piece(k):
        return pl.ds(k * step, step)

    def send(src, origin, k, sem, target):
        return pltpu.make_async_remote_copy(
            src_ref=src, dst_ref=buf.at[origin, piece(k)], send_sem=sem,
            recv_sem=recv.at[origin, k], device_id=target, device_id_type=MESH)

    sent = []
    for k in range(chunks):
        for d in range(chips - 1):
            sent.append(send(x_ref.at[piece(k)], me, k, send_x.at[d, k], (dp_id, others[d])))
            sent[-1].start()
    for k in range(chunks):
        sent.append(send(x_ref.at[piece(k)], me, k, send_c.at[0, k], twin))
        sent[-1].start()
    own.wait()
    for k in range(chunks):
        for d in range(chips - 1):
            origin = sources[d]
            forward = send(buf.at[origin, piece(k)], origin, k, send_c.at[d + 1, k], twin)
            forward.wait_recv()
            forward.start()
            sent.append(forward)
        if k:
            finish(tp, k - 1, step, chip, core, chips, buf, recv, out_ref, send, twin)
    finish(tp, chunks - 1, step, chip, core, chips, buf, recv, out_ref, send, twin)
    for copy in sent:
        copy.wait_send()


def finish(tp, k, step, chip, core, chips, buf, recv, out_ref, send, twin):
    cols = buf.shape[2]
    part = pl.ds(k * step, step)
    for d in range(chips):
        origin = lax.rem(chip + d, chips) * CORES + (1 - core)
        pltpu.make_async_remote_copy(
            src_ref=buf.at[origin, part], dst_ref=buf.at[origin, part], send_sem=recv.at[origin, k],
            recv_sem=recv.at[origin, k], device_id=twin, device_id_type=MESH).wait_recv()
    for t in range(tp):
        out_ref[part, t * cols:(t + 1) * cols] = buf[t, part, :]


def feature_gather(x, tp, chunks, collective_id):
    rows, cols = x.shape
    chips = tp // CORES
    return pl.pallas_call(
        functools.partial(feature_gather_kernel, tp, chunks),
        out_shape=jax.ShapeDtypeStruct((rows, tp * cols), x.dtype),
        in_specs=[pl.BlockSpec(memory_space=pltpu.VMEM)],
        out_specs=pl.BlockSpec(memory_space=pltpu.VMEM),
        scratch_shapes=[
            pltpu.VMEM((tp, rows, cols), x.dtype),
            pltpu.SemaphoreType.DMA,
            pltpu.SemaphoreType.DMA((max(chips - 1, 1), chunks)),
            pltpu.SemaphoreType.DMA((chips, chunks)),
            pltpu.SemaphoreType.DMA((tp, chunks)),
        ],
        compiler_params=pltpu.CompilerParams(
            collective_id=collective_id, has_side_effects=True, vmem_limit_bytes=48 * 2**20),
        cost_estimate=pl.CostEstimate(flops=0, bytes_accessed=rows * cols * tp * 16, transcendentals=0),
    )(x)


def share_sum_kernel(tp, scatter, x_ref, out_ref, buf, send_sem, recv_sem):
    chips = tp // CORES
    dp_id = lax.axis_index("dp")
    me = lax.axis_index("tp")
    core = lax.rem(me, CORES)
    chip = me // CORES
    others = [
        lax.rem(chip + d, chips) * CORES + c for d in range(1, chips) for c in range(CORES)
    ] + [chip * CORES + (1 - core)]
    greet([(dp_id, other) for other in others])
    sent = []
    for i, other in enumerate(others):
        sent.append(pltpu.make_async_remote_copy(
            src_ref=x_ref.at[other if scatter else 0], dst_ref=buf.at[me], send_sem=send_sem.at[i],
            recv_sem=recv_sem.at[me], device_id=(dp_id, other), device_id_type=MESH))
        sent[-1].start()
    total = x_ref[me if scatter else 0].astype(jnp.float32)
    for i in reversed(range(len(others))):
        other = others[i]
        pltpu.make_async_remote_copy(
            src_ref=buf.at[other], dst_ref=buf.at[other], send_sem=send_sem.at[i],
            recv_sem=recv_sem.at[other], device_id=(dp_id, other), device_id_type=MESH).wait_recv()
        total = total + buf[other].astype(jnp.float32)
    out_ref[...] = total
    for copy in sent:
        copy.wait_send()


def share_sum(x, tp, scatter, collective_id):
    rows, cols = x.shape[1:]
    return pl.pallas_call(
        functools.partial(share_sum_kernel, tp, scatter),
        out_shape=jax.ShapeDtypeStruct((rows, cols), jnp.float32),
        in_specs=[pl.BlockSpec(memory_space=pltpu.VMEM)],
        out_specs=pl.BlockSpec(memory_space=pltpu.VMEM),
        scratch_shapes=[
            pltpu.VMEM((tp, rows, cols), x.dtype),
            pltpu.SemaphoreType.DMA((tp - 1,)),
            pltpu.SemaphoreType.DMA((tp,)),
        ],
        compiler_params=pltpu.CompilerParams(
            collective_id=collective_id, has_side_effects=True, vmem_limit_bytes=16 * 2**20),
        cost_estimate=pl.CostEstimate(flops=0, bytes_accessed=rows * cols * tp * 16, transcendentals=0),
    )(x)


def full_gather_kernel(dp, ny, tp, x_ref, out_ref, buf, own_sem, send_z, send_x, send_y, send_c, recv):
    nz, nx = dp // ny, tp // CORES
    dp_id = lax.axis_index("dp")
    me = lax.axis_index("tp")
    core, x = lax.rem(me, CORES), me // CORES
    z, y = dp_id // ny, lax.rem(dp_id, ny)
    rows, cols = x_ref.shape
    half = rows // 2

    def place(pz, py, px, pc=core):
        return (pz * ny + py, px * CORES + pc)

    def around(v, d, n):
        return lax.rem(v + d, n)

    own = pltpu.make_async_copy(x_ref, buf.at[dp_id, me], own_sem)
    own.start()
    twin = place(z, y, x, 1 - core)
    x_others = [place(z, y, around(x, d, nx)) for d in range(1, nx)]
    y_others = [place(z, around(y, d, ny), x) for d in range(1, ny)]
    ring = [place(lax.rem(z + d, nz), y, x) for d in sorted({1 % nz, nz - 1} - {0})]
    greet([twin] + x_others + y_others + ring)
    own.wait()

    def copy(origin, h, sem, target):
        view = buf.at[origin[0], origin[1], pl.ds(h * half, half)]
        return pltpu.make_async_remote_copy(
            src_ref=view, dst_ref=view, send_sem=sem.at[origin[0], origin[1] // CORES, h],
            recv_sem=recv.at[origin[0], origin[1], h], device_id=target, device_id_type=MESH)

    def arrived(origin, h):
        view = buf.at[origin[0], origin[1], pl.ds(h * half, half)]
        pltpu.make_async_remote_copy(
            src_ref=view, dst_ref=view, send_sem=recv.at[origin[0], origin[1], h],
            recv_sem=recv.at[origin[0], origin[1], h], device_id=twin, device_id_type=MESH).wait_recv()

    def to_x(origin, h, act):
        for d in range(nx - 1):
            act(copy(origin, h, send_x.at[d], x_others[d]))

    def to_y(origin, h, act):
        for d in range(ny - 1):
            act(copy(origin, h, send_y.at[d], y_others[d]))

    def to_twin(origin, h, act):
        act(copy(origin, h, send_c, twin))

    def start(c):
        c.start()

    def ended(c):
        c.wait_send()

    def spread(origin, act):
        to_x(origin, 0, act)
        to_y(origin, 1, act)
        to_y(origin, 0, act)
        to_x(origin, 1, act)
        for h in range(2):
            to_twin(origin, h, act)

    def sideways(pz, act, wait):
        for d in range(1, nx):
            origin = place(pz, y, around(x, d, nx))
            if wait:
                arrived(origin, 0)
            to_y(origin, 0, act)
            to_twin(origin, 0, act)
        for d in range(1, ny):
            origin = place(pz, around(y, d, ny), x)
            if wait:
                arrived(origin, 1)
            to_x(origin, 1, act)
            to_twin(origin, 1, act)

    def last(pz, act, wait):
        for d in range(1, ny):
            for e in range(nx):
                origin = place(pz, around(y, d, ny), around(x, e, nx))
                if wait:
                    arrived(origin, 0)
                to_twin(origin, 0, act)
        for d in range(1, nx):
            for e in range(ny):
                origin = place(pz, around(y, e, ny), around(x, d, nx))
                if wait:
                    arrived(origin, 1)
                to_twin(origin, 1, act)

    def above(pz, act):
        @pl.when(z > 0)
        def _():
            for h in range(2):
                act(copy(place(pz, y, x), h, send_z.at[0], place(z - 1, y, x)))

    def below(pz, act):
        @pl.when(z < nz - 1)
        def _():
            for h in range(2):
                act(copy(place(pz, y, x), h, send_z.at[1], place(z + 1, y, x)))

    mine = place(z, y, x)
    above(z, start)
    below(z, start)
    spread(mine, start)

    def first_wave(pz, onward):
        origin = place(pz, y, x)
        arrived(origin, 0)
        arrived(origin, 1)
        onward(pz, start)
        spread(origin, start)

    sideways(z, start, True)
    for s in range(1, nz):
        for pz, ok, onward in ((z - s, z - s >= 0, below), (z + s, z + s < nz, above)):
            pl.when(ok)(functools.partial(first_wave, pz, onward))
        for pz, ok in ((z - s, z - s >= 0), (z + s, z + s < nz)):
            pl.when(ok)(functools.partial(sideways, pz, start, True))
        if s == 1:
            last(z, start, True)
        else:
            for pz, ok in ((z - s + 1, z - s + 1 >= 0), (z + s - 1, z + s - 1 < nz)):
                pl.when(ok)(functools.partial(last, pz, start, True))
    for pz, ok in ((z - nz + 1, z - nz + 1 >= 0), (z + nz - 1, z + nz - 1 < nz)):
        pl.when(ok)(functools.partial(last, pz, start, True))

    for b in range(dp):
        for px in range(nx):
            for h in range(2):
                arrived((b, px * CORES + 1 - core), h)
        for h in range(2):
            start_row = (h * dp + b) * half
            for t in range(tp):
                out_ref[start_row:start_row + half, t * cols:(t + 1) * cols] = buf[
                    b, t, h * half:(h + 1) * half
                ]

    def ends(pz, onward=None):
        if onward is not None:
            onward(pz, ended)
        spread(place(pz, y, x), ended)
        sideways(pz, ended, False)
        last(pz, ended, False)

    above(z, ended)
    below(z, ended)
    ends(z)
    for s in range(1, nz):
        for pz, ok, onward in ((z - s, z - s >= 0, below), (z + s, z + s < nz, above)):
            pl.when(ok)(functools.partial(ends, pz, onward))


def full_gather(x, dp, tp, collective_id):
    rows, cols = x.shape
    nx = tp // CORES
    ny = 2 ** (int(math.log2(dp)) // 2)
    per_piece = (dp, nx, 2)
    return pl.pallas_call(
        functools.partial(full_gather_kernel, dp, ny, tp),
        out_shape=jax.ShapeDtypeStruct((dp * rows, tp * cols), x.dtype),
        in_specs=[pl.BlockSpec(memory_space=pltpu.VMEM)],
        out_specs=pl.BlockSpec(memory_space=pltpu.VMEM),
        scratch_shapes=[
            pltpu.VMEM((dp, tp, rows, cols), x.dtype),
            pltpu.SemaphoreType.DMA,
            pltpu.SemaphoreType.DMA((2,) + per_piece),
            pltpu.SemaphoreType.DMA((max(nx - 1, 1),) + per_piece),
            pltpu.SemaphoreType.DMA((max(ny - 1, 1),) + per_piece),
            pltpu.SemaphoreType.DMA(per_piece),
            pltpu.SemaphoreType.DMA((dp, tp, 2)),
        ],
        compiler_params=pltpu.CompilerParams(
            collective_id=collective_id, has_side_effects=True, vmem_limit_bytes=48 * 2**20),
        cost_estimate=pl.CostEstimate(flops=0, bytes_accessed=rows * cols * dp * tp * 8, transcendentals=0),
    )(x)


LANE = 128


def pad_up(n, m):
    return -(-n // m) * m


def dot_t(a, b):
    return lax.dot_general(a, b, (((1,), (1,)), ((), ())), preferred_element_type=jnp.float32)


def moe_kernel(
    dp, ny, tp, experts,
    res_ref, gain_ref, router_ref, chosen_ref, gu_hbm, wd_hbm, out_ref,
    rows_buf, gu_raw, gu_pad, wd_raw, wd_pad, act_buf, out_buf, back_buf,
    load_sem, s_twin, s_x, s_y, s_z, r_rows, s_act, r_act, s_out, r_out,
):
    nz = dp // ny
    dp_id = lax.axis_index("dp")
    me = lax.axis_index("tp")
    core, chip = lax.rem(me, CORES), me // CORES
    z, y = dp_id // ny, lax.rem(dp_id, ny)
    seq, wide = res_ref.shape
    cols = out_ref.shape[1]
    full = gu_hbm.shape[2]
    twin_t = chip * CORES + 1 - core
    across_t = (1 - chip) * CORES + core
    corner_t = (1 - chip) * CORES + 1 - core
    twin, across = (dp_id, twin_t), (dp_id, across_t)
    y_peer = (z * ny + 1 - y, me)

    gu_load = pltpu.make_async_copy(gu_hbm, gu_raw, load_sem.at[0])
    wd_load = pltpu.make_async_copy(wd_hbm, wd_raw, load_sem.at[1])
    gu_load.start()
    wd_load.start()

    barrier = pltpu.get_barrier_semaphore()
    for d in range(1, dp):
        pl.semaphore_signal(barrier, inc=1, device_id=(lax.rem(dp_id + d, dp), me), device_id_type=MESH)
    for other in (twin, across):
        pl.semaphore_signal(barrier, inc=1, device_id=other, device_id_type=MESH)

    res = res_ref[...]
    gained = res * gain_ref[...]
    values = [jnp.sum(res * res, axis=1, keepdims=True)]
    for e in range(experts):
        values.append(jnp.sum(gained * router_ref[e:e + 1, :], axis=1, keepdims=True))
    tail = cols - (wide - LANE)
    lanes = lax.broadcasted_iota(jnp.int32, (seq, LANE), 1)
    group = (LANE - tail) // 3
    spread = jnp.zeros((seq, LANE), jnp.float32)
    for j, v in enumerate(values):
        for g in range(3):
            spread = jnp.where(lanes == tail + g * group + j, v, spread)
    high = spread.astype(jnp.bfloat16).astype(jnp.float32)
    middle = (spread - high).astype(jnp.bfloat16).astype(jnp.float32)
    low = spread - high - middle
    last = jnp.where(lanes < tail, gained[:, wide - LANE:], jnp.where(
        lanes < tail + group, high, jnp.where(lanes < tail + 2 * group, middle, low)))
    rows_buf[dp_id, me, :, :wide - LANE] = gained[:, :wide - LANE].astype(jnp.bfloat16)
    rows_buf[dp_id, me, :, wide - LANE:] = last.astype(jnp.bfloat16)

    pl.semaphore_wait(barrier, dp + 1)

    def piece(b, t, sem, target):
        view = rows_buf.at[b, t]
        return pltpu.make_async_remote_copy(
            src_ref=view, dst_ref=view, send_sem=sem, recv_sem=r_rows.at[b, t],
            device_id=target, device_id_type=MESH)

    def to_twin(b, t):
        return piece(b, t, s_twin.at[b, t], twin)

    def to_y(b, t):
        return piece(b, t, s_y.at[b, t // CORES], y_peer)

    def to_z(t, d):
        return piece(dp_id, t, s_z.at[t // CORES, d], (lax.rem(z + d, nz) * ny + y, me))

    def arrived(b, t):
        piece(b, t, r_rows.at[b, t], twin).wait_recv()

    def plane(k):
        near = jnp.minimum(z, nz - 1 - z)
        step = (k + 1) // 2
        swing = jnp.where(lax.rem(k, 2) == 1, z - step, z + step)
        rest = jnp.where(z < nz - 1 - z, k, nz - 1 - k)
        return jnp.where(k <= 2 * near, swing, rest)

    piece(dp_id, me, s_x, across).start()
    to_y(dp_id, me).start()
    to_twin(dp_id, me).start()

    def send_far(t):
        def body(k, carry):
            d = lax.rem(plane(k) - z + nz, nz)
            to_z(t, d).start()
            return carry
        lax.fori_loop(1, nz, body, 0)

    send_far(me)

    gu_load.wait()
    wd_load.wait()

    def widen(raw, padded, lead):
        block = 48
        blocks = raw.shape[-2] // block

        def body(i, carry):
            at = pl.ds(pl.multiple_of(i * block, 16), block)
            v = raw[lead + (at, slice(None))]
            for t in range(tp):
                part = v[:, t * cols:(t + 1) * cols]
                padded[lead + (at, pl.ds(t * wide, wide))] = jnp.concatenate(
                    [part, jnp.zeros((block, wide - cols), v.dtype)], axis=1)
            return carry
        lax.fori_loop(0, blocks, body, 0)
        rest = padded.shape[-2] - raw.shape[-2]
        padded[lead + (pl.ds(raw.shape[-2], rest), slice(None))] = jnp.zeros((rest, tp * wide), padded.dtype)

    widen(gu_raw, gu_pad, (0,))
    widen(gu_raw, gu_pad, (1,))

    arrived(dp_id, across_t)
    to_y(dp_id, across_t).start()
    to_twin(dp_id, across_t).start()
    send_far(across_t)
    widen(wd_raw, wd_pad, ())

    def far_arrival(k, t):
        b = plane(k) * ny + y
        arrived(b, t)
        to_y(b, t).start()
        to_twin(b, t).start()

    def act_copy(t, p, sem, target):
        view = act_buf.at[t, p]
        return pltpu.make_async_remote_copy(
            src_ref=view, dst_ref=view, send_sem=sem, recv_sem=r_act.at[t, p],
            device_id=target, device_id_type=MESH)

    def act_arrived(t, p):
        act_copy(t, p, r_act.at[t, p], twin).wait_recv()

    def out_copy(b):
        return pltpu.make_async_remote_copy(
            src_ref=out_buf.at[b], dst_ref=back_buf.at[dp_id], send_sem=s_out.at[b],
            recv_sem=r_out.at[dp_id], device_id=(b, me), device_id_type=MESH)

    def stats_tile(b):
        total = rows_buf[b, 0, :, wide - LANE:].astype(jnp.float32)
        for t in range(1, tp):
            total = total + rows_buf[b, t, :, wide - LANE:].astype(jnp.float32)
        total = jnp.where(lanes >= tail, total, 0.0)
        return total

    def row_scale(total):
        hit = (lanes == tail) | (lanes == tail + group) | (lanes == tail + 2 * group)
        squares = jnp.sum(jnp.where(hit, total, 0.0), axis=1, keepdims=True)
        return lax.rsqrt(squares / full + norm_eps)

    tile_n = 256
    n_tiles = wide // tile_n

    def up_project(p):
        scale = jnp.concatenate([row_scale(stats_tile(p * ny + b)) for b in range(ny)], axis=0)

        def body(n, carry):
            at = pl.ds(pl.multiple_of(n * tile_n, tile_n), tile_n)
            lhs = jnp.concatenate([
                jnp.concatenate([rows_buf[p * ny + b, t] for t in range(tp)], axis=1)
                for b in range(ny)], axis=0)
            gate = dot_t(lhs, gu_pad[0, at, :]) * scale
            up = dot_t(lhs, gu_pad[1, at, :]) * scale
            act_buf[me, p, :, at] = (gate * jax.nn.sigmoid(glu_alpha * gate) * (up + 1.0)).astype(jnp.bfloat16)
            return carry
        lax.fori_loop(0, n_tiles, body, 0)

    def down_project(p):
        def body(n, carry):
            at = pl.ds(pl.multiple_of(n * tile_n, tile_n), tile_n)
            lhs = jnp.concatenate([act_buf[t, p] for t in range(tp)], axis=1)
            out = dot_t(lhs, wd_pad[at, :]).astype(jnp.bfloat16)
            for b in range(ny):
                out_buf[p * ny + b, :, at] = out[b * seq:(b + 1) * seq]
            return carry
        lax.fori_loop(0, n_tiles, body, 0)

    def stage(k, carry):
        @pl.when(k < nz - 1)
        def _():
            far_arrival(k + 1, me)

        @pl.when(k < nz)
        def _():
            p = plane(k)
            for t in (me, across_t):
                b = p * ny + 1 - y
                arrived(b, t)
                to_twin(b, t).start()
            for b in range(ny):
                for t in (twin_t, corner_t):
                    arrived(p * ny + b, t)
            up_project(p)
            act_copy(me, p, s_act.at[0, p], across).start()
            act_copy(me, p, s_act.at[1, p], twin).start()

        @pl.when(k < nz - 1)
        def _():
            far_arrival(k + 1, across_t)

        @pl.when(k > 0)
        def _():
            p = plane(k - 1)
            act_arrived(across_t, p)
            act_copy(across_t, p, s_act.at[2, p], twin).start()
            act_arrived(twin_t, p)
            act_arrived(corner_t, p)
            down_project(p)
            for b in range(ny):
                @pl.when(p * ny + b != dp_id)
                def _():
                    out_copy(p * ny + b).start()

                @pl.when(p * ny + b == dp_id)
                def _():
                    back_buf[dp_id] = out_buf[dp_id]
        return carry

    lax.fori_loop(0, nz + 1, stage, 0)

    total = stats_tile(dp_id)
    scale = row_scale(total)
    shift = LANE - group
    summed = total + pltpu.roll(total, shift, 1) + pltpu.roll(pltpu.roll(total, shift, 1), shift, 1)
    chosen = chosen_ref[...]
    raised = jnp.where(chosen > 0.0, jnp.exp(jnp.where(chosen > 0.0, summed * scale, 0.0)), 0.0)
    weights = raised / jnp.sum(raised, axis=1, keepdims=True)

    def wait_out(d, carry):
        b = lax.rem(dp_id + d, dp)
        pltpu.make_async_remote_copy(
            src_ref=back_buf.at[b], dst_ref=back_buf.at[b], send_sem=r_out.at[b],
            recv_sem=r_out.at[b], device_id=twin, device_id_type=MESH).wait_recv()
        return carry

    lax.fori_loop(1, dp, wait_out, 0)
    answer = res
    for e in range(dp):
        answer = answer + weights[:, tail + 1 + e:tail + 2 + e] * back_buf[e].astype(jnp.float32)
    out_ref[...] = answer[:, :cols]

    piece(dp_id, me, s_x, across).wait_send()
    for t in (me, across_t):
        for d in range(1, nz):
            to_z(t, d).wait_send()
        for p in range(nz):
            to_y(p * ny + y, t).wait_send()
            for b in range(ny):
                to_twin(p * ny + b, t).wait_send()
    for p in range(nz):
        act_copy(me, p, s_act.at[0, p], across).wait_send()
        act_copy(me, p, s_act.at[1, p], twin).wait_send()
        act_copy(across_t, p, s_act.at[2, p], twin).wait_send()
    for d in range(1, dp):
        out_copy(lax.rem(dp_id + d, dp)).wait_send()


def moe(res, gain, router, chosen, gate_up, w_down, dp, ny, tp, collective_id):
    seq, cols = res.shape
    wide = pad_up(cols, 256)
    full = gate_up.shape[2]
    experts = router.shape[0]
    nz = dp // ny
    pad = ((0, 0), (0, wide - cols))
    bf = jnp.bfloat16
    dma = pltpu.SemaphoreType.DMA
    return pl.pallas_call(
        functools.partial(moe_kernel, dp, ny, tp, experts),
        out_shape=jax.ShapeDtypeStruct((seq, cols), jnp.float32),
        in_specs=[pl.BlockSpec(memory_space=pltpu.VMEM)] * 4 + [pl.BlockSpec(memory_space=pl.ANY)] * 2,
        out_specs=pl.BlockSpec(memory_space=pltpu.VMEM),
        scratch_shapes=[
            pltpu.VMEM((dp, tp, seq, wide), bf),
            pltpu.VMEM((2, cols, full), bf),
            pltpu.VMEM((2, wide, tp * wide), bf),
            pltpu.VMEM((cols, full), bf),
            pltpu.VMEM((wide, tp * wide), bf),
            pltpu.VMEM((tp, nz, ny * seq, wide), bf),
            pltpu.VMEM((dp, seq, wide), bf),
            pltpu.VMEM((dp, seq, wide), bf),
            dma((2,)), dma((dp, tp)), dma, dma((dp, tp // CORES)), dma((tp // CORES, nz)), dma((dp, tp)),
            dma((3, nz)), dma((tp, nz)), dma((dp,)), dma((dp,)),
        ],
        compiler_params=pltpu.CompilerParams(
            collective_id=collective_id, has_side_effects=True, vmem_limit_bytes=56 * 2**20),
        cost_estimate=pl.CostEstimate(flops=6 * dp * seq * full * cols, bytes_accessed=6 * full * cols, transcendentals=0),
    )(jnp.pad(res, pad), jnp.pad(gain[None, :], pad), jnp.pad(router, pad), chosen, gate_up, w_down)


def activate(mixed_in, ff_local):
    gate_part = mixed_in[..., :ff_local]
    up_part = mixed_in[..., ff_local:]
    return (gate_part * jax.nn.sigmoid(glu_alpha * gate_part) * (up_part + 1.0)).astype(
        jnp.bfloat16
    )


def on_device(
    tokens,
    attn_gain,
    w_query,
    w_keyvalue,
    attn_sinks,
    w_out,
    window_cache,
    positions,
    moe_gain,
    router,
    gate_up,
    w_down,
    expert_ids,
):
    tp_count = lax.axis_size("tp")
    dp_count = lax.axis_size("dp")
    seq_count, col_count = tokens.shape
    full_width = col_count * tp_count
    col_start = lax.axis_index("tp") * col_count
    head_size = w_keyvalue.shape[2] // 2
    kv_local = w_keyvalue.shape[1]
    q_local = w_query.shape[1] // head_size
    group_size = q_local // kv_local
    window = window_cache.shape[2]
    moe_slice = lax.dynamic_slice_in_dim(moe_gain, col_start, col_count)
    tok_wide = tokens.astype(jnp.float32)
    kv_flat = w_keyvalue.reshape(full_width, kv_local * 2 * head_size)
    whole_rows = feature_gather(tokens, tp_count, 2, 0).astype(jnp.float32)
    attn_sq = jnp.sum(whole_rows * whole_rows, axis=1, keepdims=True)
    piece_rows = (
        whole_rows * lax.rsqrt(attn_sq / full_width + norm_eps) * attn_gain[None, :]
    ).astype(jnp.bfloat16)
    queries = jnp.dot(piece_rows, w_query, preferred_element_type=jnp.float32)
    fresh_rows = jnp.dot(piece_rows, kv_flat, preferred_element_type=jnp.float32)
    cosine, sine_table = rope_tables(positions, head_size)
    rot_queries = rotate(
        queries.reshape(seq_count, q_local, head_size), cosine[:, None, :], sine_table[:, None, :]
    ).astype(jnp.bfloat16)
    fresh_rows = fresh_rows.reshape(seq_count, kv_local, 2 * head_size)
    new_key = rotate(fresh_rows[..., :head_size], cosine[:, None, :], sine_table[:, None, :])
    new_entry = jnp.concatenate([new_key, fresh_rows[..., head_size:]], axis=-1).astype(
        jnp.bfloat16
    )
    slot_ids = jnp.arange(window, dtype=jnp.int32)
    is_current = slot_ids[None, :] == (positions % window)[:, None]
    is_valid = (positions[:, None] - slot_ids[None, :]) % window <= positions[:, None]
    is_valid = is_valid & ~is_current
    grouped = rot_queries.reshape(seq_count, kv_local, group_size, head_size)
    scores = jnp.einsum(
        "skgh,skwh->skgw", grouped, window_cache[..., :head_size], preferred_element_type=jnp.float32
    ) * head_size ** (-0.5)
    scores = jnp.where(is_valid[:, None, None, :], scores, -jnp.inf)
    new_wide = new_entry.astype(jnp.float32)[:, :, None, :]
    new_score = jnp.sum(
        grouped.astype(jnp.float32) * new_wide[..., :head_size], axis=-1, keepdims=True
    ) * head_size ** (-0.5)
    sink_col = attn_sinks.reshape(kv_local, group_size)[None, :, :, None]
    peak_score = jnp.maximum(
        jnp.maximum(jnp.max(scores, axis=-1, keepdims=True), new_score), sink_col
    )
    raised = jnp.exp(scores - peak_score)
    raised_new = jnp.exp(new_score - peak_score)
    denominator = (
        jnp.sum(raised, axis=-1, keepdims=True) + raised_new + jnp.exp(sink_col - peak_score)
    )
    prob_bf = (raised / denominator).astype(jnp.bfloat16)
    prob_new = (raised_new / denominator).astype(jnp.bfloat16).astype(jnp.float32)
    attended = jnp.einsum(
        "skgw,skwh->skgh", prob_bf, window_cache[..., head_size:], preferred_element_type=jnp.float32
    )
    attended = (attended + prob_new * new_wide[..., head_size:]).astype(jnp.bfloat16)
    partial_out = jnp.einsum(
        "sh,htc->tsc",
        attended.reshape(seq_count, q_local * head_size),
        w_out.reshape(q_local * head_size, tp_count, col_count),
        preferred_element_type=jnp.float32,
    ).astype(jnp.bfloat16)
    residual = tok_wide + share_sum(partial_out, tp_count, True, 2)
    experts = router.shape[1]
    top_count = expert_ids.shape[1]
    local_experts = gate_up.shape[0]
    ff_local = gate_up.shape[3]
    capacity = min(seq_count, max(2, 8 * seq_count * top_count // (3 * experts)))
    expert_iota = jnp.arange(experts, dtype=jnp.int32)
    nz_ny = 2 ** (int(math.log2(dp_count)) // 2)
    if capacity >= seq_count and local_experts == 1 and nz_ny == 2 and tp_count == 2 * CORES:
        wide = pad_up(col_count, 256)
        first = col_count - (wide - LANE) + 1
        lane_iota = jnp.arange(LANE, dtype=jnp.int32) - first
        chosen_lanes = jnp.any(expert_ids[:, :, None] == lane_iota[None, None, :], axis=1).astype(jnp.float32)
        return moe(
            residual, moe_slice, router.T.astype(jnp.float32), chosen_lanes,
            jnp.transpose(gate_up[0], (1, 2, 0)), w_down[0].T, dp_count, nz_ny, tp_count, 1)
    moe_sq = jnp.sum(residual * residual, axis=1)
    router_wide = router.astype(jnp.float32)
    gained = residual * moe_slice[None, :]
    raw_logits = jnp.dot(gained, router_wide, precision=lax.Precision.HIGHEST)
    stats = share_sum(
        jnp.concatenate([moe_sq[:, None], raw_logits], axis=1)[None], tp_count, False, 3
    )
    moe_scale = lax.rsqrt(stats[:, :1] / full_width + norm_eps)
    logits = stats[:, 1:] * moe_scale
    hidden_rows = (gained * moe_scale).astype(jnp.bfloat16)
    chosen = expert_ids[:, :, None] == expert_iota[None, None, :]
    picked = jnp.sum(jnp.where(chosen, logits[:, None, :], 0.0), axis=-1)
    raised_logits = jnp.exp(picked)
    route_weights = raised_logits / jnp.sum(raised_logits, axis=1, keepdims=True)
    gate_up_flat = gate_up.reshape(local_experts, full_width, 2 * ff_local)
    if capacity >= seq_count:
        token_weights = jnp.sum(jnp.where(chosen, route_weights[:, :, None], 0.0), axis=1)
        all_rows = full_gather(hidden_rows, dp_count, tp_count, 1)
        half = seq_count // 2
        part = dp_count * half
        acts = [
            activate(
                jnp.dot(all_rows, gate_up_flat[e], preferred_element_type=jnp.float32), ff_local
            )
            for e in range(local_experts)
        ]
        pieces = []
        for h in range(2):
            outs = []
            for e in range(local_experts):
                act_all = feature_gather(
                    acts[e][h * part : (h + 1) * part], tp_count, dp_count // 2, 4 + 2 * e + h
                )
                out = jnp.dot(act_all, w_down[e], preferred_element_type=jnp.float32)
                outs.append(out.astype(jnp.bfloat16).reshape(dp_count, half, col_count))
            returned = lax.all_to_all(
                jnp.stack(outs, axis=1), "dp", split_axis=0, concat_axis=0, tiled=True
            )
            back = returned.reshape(experts, half, col_count)
            mine = slice(h * half, (h + 1) * half)
            total = residual[mine]
            for e in range(experts):
                total = total + token_weights[mine, e : e + 1] * back[e].astype(jnp.float32)
            pieces.append(total)
        total = jnp.concatenate(pieces, axis=0)
        return total
    assign = expert_ids.reshape(-1)
    onehot = (assign[:, None] == expert_iota[None, :]).astype(jnp.int32)
    earlier = jnp.cumsum(onehot, axis=0) - onehot
    slot_of = jnp.sum(earlier * onehot, axis=1)
    target = (assign * capacity + slot_of).reshape(seq_count, top_count)
    spot_ids = jnp.arange(experts * capacity, dtype=jnp.int32)
    slot_hits = target[:, :, None] == spot_ids[None, None, :]
    placer = jnp.transpose(jnp.any(slot_hits, axis=1)).astype(jnp.bfloat16)
    combiner = jnp.sum(jnp.where(slot_hits, route_weights[:, :, None], 0.0), axis=1)
    placed = jnp.dot(placer, hidden_rows, preferred_element_type=jnp.float32).astype(jnp.bfloat16)
    mixed_in = jnp.einsum(
        "gecd,edf->gecf",
        lax.all_gather(
            lax.all_to_all(
                placed.reshape(dp_count, local_experts, capacity, hidden_rows.shape[1]),
                "dp",
                split_axis=0,
                concat_axis=0,
                tiled=True,
            ),
            "tp",
            axis=3,
            tiled=True,
        ),
        gate_up_flat,
        preferred_element_type=jnp.float32,
    )
    act_rows = activate(mixed_in, ff_local)
    answered = jnp.einsum(
        "gecf,efd->gecd",
        lax.all_gather(act_rows, "tp", axis=3, tiled=True),
        w_down,
        preferred_element_type=jnp.float32,
    ).astype(jnp.bfloat16)
    returned = lax.all_to_all(answered, "dp", split_axis=0, concat_axis=0, tiled=True)
    flat_back = returned.reshape(experts * capacity, col_count).astype(jnp.float32)
    moe_out = jnp.dot(combiner, flat_back, precision=lax.Precision.HIGHEST)
    return residual + moe_out


def solution(mesh):
    in_specs = (
        P("dp", "tp"),
        P(),
        P(None, "tp"),
        P(None, "tp", None),
        P("tp"),
        P("tp", None),
        P("dp", "tp", None, None),
        P("dp"),
        P(),
        P("tp", None),
        P("dp", None, None, "tp"),
        P("dp", None, "tp"),
        P("dp", None),
    )
    out_specs = P("dp", "tp")
    return jax.shard_map(
        on_device, mesh=mesh, in_specs=in_specs, out_specs=out_specs, check_vma=False
    )
```

```python
import functools
import math

import jax
import jax.numpy as jnp
import numpy as np
from jax import lax
from jax.experimental import pallas as pl
from jax.experimental.pallas import tpu as pltpu
from jax.sharding import PartitionSpec as P

norm_eps = 1e-05
rope_base = 150000.0
glu_alpha = 1.702


def rope_tables(positions, head_size):
    half_size = head_size // 2
    exponent = jnp.arange(half_size, dtype=jnp.float32) * (2.0 / head_size)
    inverse = jnp.power(jnp.float32(rope_base), -exponent)
    angles = positions.astype(jnp.float32)[:, None] * inverse[None, :]
    return (jnp.cos(angles), jnp.sin(angles))


def rotate(values, cosine, sine_table):
    half_size = values.shape[-1] // 2
    first_half = values[..., :half_size]
    second_half = values[..., half_size:]
    return jnp.concatenate(
        [
            first_half * cosine - second_half * sine_table,
            second_half * cosine + first_half * sine_table,
        ],
        axis=-1,
    )


MESH = pl.DeviceIdType.MESH
CORES = 2


def greet(partners):
    barrier = pltpu.get_barrier_semaphore()
    for partner in partners:
        pl.semaphore_signal(barrier, inc=1, device_id=partner, device_id_type=MESH)
    pl.semaphore_wait(barrier, len(partners))


def feature_gather_kernel(tp, chunks, x_ref, out_ref, buf, own_sem, send_x, send_c, recv):
    chips = tp // CORES
    dp_id = lax.axis_index("dp")
    me = lax.axis_index("tp")
    core = lax.rem(me, CORES)
    chip = me // CORES
    rows, cols = x_ref.shape
    step = rows // chunks
    twin = (dp_id, chip * CORES + (1 - core))
    others = [lax.rem(chip + d, chips) * CORES + core for d in range(1, chips)]
    sources = [lax.rem(chip + chips - d, chips) * CORES + core for d in range(1, chips)]
    own = pltpu.make_async_copy(x_ref, buf.at[me], own_sem)
    own.start()
    greet([twin] + [(dp_id, other) for other in others])

    def piece(k):
        return pl.ds(k * step, step)

    def send(src, origin, k, sem, target):
        return pltpu.make_async_remote_copy(
            src_ref=src, dst_ref=buf.at[origin, piece(k)], send_sem=sem,
            recv_sem=recv.at[origin, k], device_id=target, device_id_type=MESH)

    sent = []
    for k in range(chunks):
        for d in range(chips - 1):
            sent.append(send(x_ref.at[piece(k)], me, k, send_x.at[d, k], (dp_id, others[d])))
            sent[-1].start()
    for k in range(chunks):
        sent.append(send(x_ref.at[piece(k)], me, k, send_c.at[0, k], twin))
        sent[-1].start()
    own.wait()
    for k in range(chunks):
        for d in range(chips - 1):
            origin = sources[d]
            forward = send(buf.at[origin, piece(k)], origin, k, send_c.at[d + 1, k], twin)
            forward.wait_recv()
            forward.start()
            sent.append(forward)
        if k:
            finish(tp, k - 1, step, chip, core, chips, buf, recv, out_ref, send, twin)
    finish(tp, chunks - 1, step, chip, core, chips, buf, recv, out_ref, send, twin)
    for copy in sent:
        copy.wait_send()


def finish(tp, k, step, chip, core, chips, buf, recv, out_ref, send, twin):
    cols = buf.shape[2]
    part = pl.ds(k * step, step)
    for d in range(chips):
        origin = lax.rem(chip + d, chips) * CORES + (1 - core)
        pltpu.make_async_remote_copy(
            src_ref=buf.at[origin, part], dst_ref=buf.at[origin, part], send_sem=recv.at[origin, k],
            recv_sem=recv.at[origin, k], device_id=twin, device_id_type=MESH).wait_recv()
    for t in range(tp):
        out_ref[part, t * cols:(t + 1) * cols] = buf[t, part, :]


def feature_gather(x, tp, chunks, collective_id):
    rows, cols = x.shape
    chips = tp // CORES
    return pl.pallas_call(
        functools.partial(feature_gather_kernel, tp, chunks),
        out_shape=jax.ShapeDtypeStruct((rows, tp * cols), x.dtype),
        in_specs=[pl.BlockSpec(memory_space=pltpu.VMEM)],
        out_specs=pl.BlockSpec(memory_space=pltpu.VMEM),
        scratch_shapes=[
            pltpu.VMEM((tp, rows, cols), x.dtype),
            pltpu.SemaphoreType.DMA,
            pltpu.SemaphoreType.DMA((max(chips - 1, 1), chunks)),
            pltpu.SemaphoreType.DMA((chips, chunks)),
            pltpu.SemaphoreType.DMA((tp, chunks)),
        ],
        compiler_params=pltpu.CompilerParams(
            collective_id=collective_id, has_side_effects=True, vmem_limit_bytes=48 * 2**20),
        cost_estimate=pl.CostEstimate(flops=0, bytes_accessed=rows * cols * tp * 16, transcendentals=0),
    )(x)


def share_sum_kernel(tp, scatter, x_ref, out_ref, buf, send_sem, recv_sem):
    chips = tp // CORES
    dp_id = lax.axis_index("dp")
    me = lax.axis_index("tp")
    core = lax.rem(me, CORES)
    chip = me // CORES
    others = [
        lax.rem(chip + d, chips) * CORES + c for d in range(1, chips) for c in range(CORES)
    ] + [chip * CORES + (1 - core)]
    greet([(dp_id, other) for other in others])
    sent = []
    for i, other in enumerate(others):
        sent.append(pltpu.make_async_remote_copy(
            src_ref=x_ref.at[other if scatter else 0], dst_ref=buf.at[me], send_sem=send_sem.at[i],
            recv_sem=recv_sem.at[me], device_id=(dp_id, other), device_id_type=MESH))
        sent[-1].start()
    total = x_ref[me if scatter else 0].astype(jnp.float32)
    for i in reversed(range(len(others))):
        other = others[i]
        pltpu.make_async_remote_copy(
            src_ref=buf.at[other], dst_ref=buf.at[other], send_sem=send_sem.at[i],
            recv_sem=recv_sem.at[other], device_id=(dp_id, other), device_id_type=MESH).wait_recv()
        total = total + buf[other].astype(jnp.float32)
    out_ref[...] = total
    for copy in sent:
        copy.wait_send()


def share_sum(x, tp, scatter, collective_id):
    rows, cols = x.shape[1:]
    return pl.pallas_call(
        functools.partial(share_sum_kernel, tp, scatter),
        out_shape=jax.ShapeDtypeStruct((rows, cols), jnp.float32),
        in_specs=[pl.BlockSpec(memory_space=pltpu.VMEM)],
        out_specs=pl.BlockSpec(memory_space=pltpu.VMEM),
        scratch_shapes=[
            pltpu.VMEM((tp, rows, cols), x.dtype),
            pltpu.SemaphoreType.DMA((tp - 1,)),
            pltpu.SemaphoreType.DMA((tp,)),
        ],
        compiler_params=pltpu.CompilerParams(
            collective_id=collective_id, has_side_effects=True, vmem_limit_bytes=16 * 2**20),
        cost_estimate=pl.CostEstimate(flops=0, bytes_accessed=rows * cols * tp * 16, transcendentals=0),
    )(x)


def full_gather_kernel(dp, ny, tp, x_ref, out_ref, buf, own_sem, send_z, send_x, send_y, send_c, recv):
    nz, nx = dp // ny, tp // CORES
    dp_id = lax.axis_index("dp")
    me = lax.axis_index("tp")
    core, x = lax.rem(me, CORES), me // CORES
    z, y = dp_id // ny, lax.rem(dp_id, ny)
    rows, cols = x_ref.shape
    half = rows // 2

    def place(pz, py, px, pc=core):
        return (pz * ny + py, px * CORES + pc)

    def around(v, d, n):
        return lax.rem(v + d, n)

    own = pltpu.make_async_copy(x_ref, buf.at[dp_id, me], own_sem)
    own.start()
    twin = place(z, y, x, 1 - core)
    x_others = [place(z, y, around(x, d, nx)) for d in range(1, nx)]
    y_others = [place(z, around(y, d, ny), x) for d in range(1, ny)]
    ring = [place(lax.rem(z + d, nz), y, x) for d in sorted({1 % nz, nz - 1} - {0})]
    greet([twin] + x_others + y_others + ring)
    own.wait()

    def copy(origin, h, sem, target):
        view = buf.at[origin[0], origin[1], pl.ds(h * half, half)]
        return pltpu.make_async_remote_copy(
            src_ref=view, dst_ref=view, send_sem=sem.at[origin[0], origin[1] // CORES, h],
            recv_sem=recv.at[origin[0], origin[1], h], device_id=target, device_id_type=MESH)

    def arrived(origin, h):
        view = buf.at[origin[0], origin[1], pl.ds(h * half, half)]
        pltpu.make_async_remote_copy(
            src_ref=view, dst_ref=view, send_sem=recv.at[origin[0], origin[1], h],
            recv_sem=recv.at[origin[0], origin[1], h], device_id=twin, device_id_type=MESH).wait_recv()

    def to_x(origin, h, act):
        for d in range(nx - 1):
            act(copy(origin, h, send_x.at[d], x_others[d]))

    def to_y(origin, h, act):
        for d in range(ny - 1):
            act(copy(origin, h, send_y.at[d], y_others[d]))

    def to_twin(origin, h, act):
        act(copy(origin, h, send_c, twin))

    def start(c):
        c.start()

    def ended(c):
        c.wait_send()

    def spread(origin, act):
        to_x(origin, 0, act)
        to_y(origin, 1, act)
        to_y(origin, 0, act)
        to_x(origin, 1, act)
        for h in range(2):
            to_twin(origin, h, act)

    def sideways(pz, act, wait):
        for d in range(1, nx):
            origin = place(pz, y, around(x, d, nx))
            if wait:
                arrived(origin, 0)
            to_y(origin, 0, act)
            to_twin(origin, 0, act)
        for d in range(1, ny):
            origin = place(pz, around(y, d, ny), x)
            if wait:
                arrived(origin, 1)
            to_x(origin, 1, act)
            to_twin(origin, 1, act)

    def last(pz, act, wait):
        for d in range(1, ny):
            for e in range(nx):
                origin = place(pz, around(y, d, ny), around(x, e, nx))
                if wait:
                    arrived(origin, 0)
                to_twin(origin, 0, act)
        for d in range(1, nx):
            for e in range(ny):
                origin = place(pz, around(y, e, ny), around(x, d, nx))
                if wait:
                    arrived(origin, 1)
                to_twin(origin, 1, act)

    def above(pz, act):
        @pl.when(z > 0)
        def _():
            for h in range(2):
                act(copy(place(pz, y, x), h, send_z.at[0], place(z - 1, y, x)))

    def below(pz, act):
        @pl.when(z < nz - 1)
        def _():
            for h in range(2):
                act(copy(place(pz, y, x), h, send_z.at[1], place(z + 1, y, x)))

    mine = place(z, y, x)
    above(z, start)
    below(z, start)
    spread(mine, start)

    def first_wave(pz, onward):
        origin = place(pz, y, x)
        arrived(origin, 0)
        arrived(origin, 1)
        onward(pz, start)
        spread(origin, start)

    sideways(z, start, True)
    for s in range(1, nz):
        for pz, ok, onward in ((z - s, z - s >= 0, below), (z + s, z + s < nz, above)):
            pl.when(ok)(functools.partial(first_wave, pz, onward))
        for pz, ok in ((z - s, z - s >= 0), (z + s, z + s < nz)):
            pl.when(ok)(functools.partial(sideways, pz, start, True))
        if s == 1:
            last(z, start, True)
        else:
            for pz, ok in ((z - s + 1, z - s + 1 >= 0), (z + s - 1, z + s - 1 < nz)):
                pl.when(ok)(functools.partial(last, pz, start, True))
    for pz, ok in ((z - nz + 1, z - nz + 1 >= 0), (z + nz - 1, z + nz - 1 < nz)):
        pl.when(ok)(functools.partial(last, pz, start, True))

    for b in range(dp):
        for px in range(nx):
            for h in range(2):
                arrived((b, px * CORES + 1 - core), h)
        for h in range(2):
            start_row = (h * dp + b) * half
            for t in range(tp):
                out_ref[start_row:start_row + half, t * cols:(t + 1) * cols] = buf[
                    b, t, h * half:(h + 1) * half
                ]

    def ends(pz, onward=None):
        if onward is not None:
            onward(pz, ended)
        spread(place(pz, y, x), ended)
        sideways(pz, ended, False)
        last(pz, ended, False)

    above(z, ended)
    below(z, ended)
    ends(z)
    for s in range(1, nz):
        for pz, ok, onward in ((z - s, z - s >= 0, below), (z + s, z + s < nz, above)):
            pl.when(ok)(functools.partial(ends, pz, onward))


def full_gather(x, dp, tp, collective_id):
    rows, cols = x.shape
    nx = tp // CORES
    ny = 2 ** (int(math.log2(dp)) // 2)
    per_piece = (dp, nx, 2)
    return pl.pallas_call(
        functools.partial(full_gather_kernel, dp, ny, tp),
        out_shape=jax.ShapeDtypeStruct((dp * rows, tp * cols), x.dtype),
        in_specs=[pl.BlockSpec(memory_space=pltpu.VMEM)],
        out_specs=pl.BlockSpec(memory_space=pltpu.VMEM),
        scratch_shapes=[
            pltpu.VMEM((dp, tp, rows, cols), x.dtype),
            pltpu.SemaphoreType.DMA,
            pltpu.SemaphoreType.DMA((2,) + per_piece),
            pltpu.SemaphoreType.DMA((max(nx - 1, 1),) + per_piece),
            pltpu.SemaphoreType.DMA((max(ny - 1, 1),) + per_piece),
            pltpu.SemaphoreType.DMA(per_piece),
            pltpu.SemaphoreType.DMA((dp, tp, 2)),
        ],
        compiler_params=pltpu.CompilerParams(
            collective_id=collective_id, has_side_effects=True, vmem_limit_bytes=48 * 2**20),
        cost_estimate=pl.CostEstimate(flops=0, bytes_accessed=rows * cols * dp * tp * 8, transcendentals=0),
    )(x)


LANE = 128


def pad_up(n, m):
    return -(-n // m) * m


def dot_t(a, b):
    return lax.dot_general(a, b, (((1,), (1,)), ((), ())), preferred_element_type=jnp.float32)


def moe_kernel(
    dp, ny, tp, experts,
    res_ref, gain_ref, router_ref, ids_ref, gu_hbm, wd_hbm, out_ref,
    rows_buf, gu_raw, gu_pad, wd_raw, wd_pad, act_buf, out_buf, back_buf,
    load_sem, s_twin, s_x, s_y, s_z, r_rows, s_act, r_act, s_out, r_out,
):
    nz = dp // ny
    dp_id = lax.axis_index("dp")
    me = lax.axis_index("tp")
    core, chip = lax.rem(me, CORES), me // CORES
    z, y = dp_id // ny, lax.rem(dp_id, ny)
    seq, wide = res_ref.shape
    cols = out_ref.shape[1]
    full = gu_hbm.shape[2]
    twin_t = chip * CORES + 1 - core
    across_t = (1 - chip) * CORES + core
    corner_t = (1 - chip) * CORES + 1 - core
    twin, across = (dp_id, twin_t), (dp_id, across_t)
    y_peer = (z * ny + 1 - y, me)

    gu_load = pltpu.make_async_copy(gu_hbm, gu_raw, load_sem.at[0])
    wd_load = pltpu.make_async_copy(wd_hbm, wd_raw, load_sem.at[1])
    gu_load.start()
    wd_load.start()

    barrier = pltpu.get_barrier_semaphore()
    for d in range(1, dp):
        pl.semaphore_signal(barrier, inc=1, device_id=(lax.rem(dp_id + d, dp), me), device_id_type=MESH)
    for other in (twin, across):
        pl.semaphore_signal(barrier, inc=1, device_id=other, device_id_type=MESH)

    res = res_ref[...]
    gain = gain_ref[:, :cols]
    for t in range(1, tp):
        gain = jnp.where(me == t, gain_ref[:, t * cols:(t + 1) * cols], gain)
    gained = res * jnp.concatenate([gain, jnp.zeros((1, wide - cols), jnp.float32)], axis=1)
    values = [jnp.sum(res * res, axis=1, keepdims=True)]
    router = jnp.concatenate(
        [router_ref[...].astype(jnp.float32), jnp.zeros((experts, wide - cols), jnp.float32)], axis=1)
    for e in range(experts):
        values.append(jnp.sum(gained * router[e:e + 1, :], axis=1, keepdims=True))
    tail = cols - (wide - LANE)
    lanes = lax.broadcasted_iota(jnp.int32, (seq, LANE), 1)
    group = (LANE - tail) // 3
    spread = jnp.zeros((seq, LANE), jnp.float32)
    for j, v in enumerate(values):
        for g in range(3):
            spread = jnp.where(lanes == tail + g * group + j, v, spread)
    high = spread.astype(jnp.bfloat16).astype(jnp.float32)
    middle = (spread - high).astype(jnp.bfloat16).astype(jnp.float32)
    low = spread - high - middle
    last = jnp.where(lanes < tail, gained[:, wide - LANE:], jnp.where(
        lanes < tail + group, high, jnp.where(lanes < tail + 2 * group, middle, low)))
    rows_buf[dp_id, me, :, :wide - LANE] = gained[:, :wide - LANE].astype(jnp.bfloat16)
    rows_buf[dp_id, me, :, wide - LANE:] = last.astype(jnp.bfloat16)

    pl.semaphore_wait(barrier, dp + 1)

    def piece(b, t, sem, target):
        view = rows_buf.at[b, t]
        return pltpu.make_async_remote_copy(
            src_ref=view, dst_ref=view, send_sem=sem, recv_sem=r_rows.at[b, t],
            device_id=target, device_id_type=MESH)

    def to_twin(b, t):
        return piece(b, t, s_twin.at[b, t], twin)

    def to_y(b, t):
        return piece(b, t, s_y.at[b, t // CORES], y_peer)

    def to_z(t, d):
        return piece(dp_id, t, s_z.at[t // CORES, d], (lax.rem(z + d, nz) * ny + y, me))

    def arrived(b, t):
        piece(b, t, r_rows.at[b, t], twin).wait_recv()

    def plane(k):
        near = jnp.minimum(z, nz - 1 - z)
        step = (k + 1) // 2
        swing = jnp.where(lax.rem(k, 2) == 1, z - step, z + step)
        rest = jnp.where(z < nz - 1 - z, k, nz - 1 - k)
        return jnp.where(k <= 2 * near, swing, rest)

    piece(dp_id, me, s_x, across).start()
    to_y(dp_id, me).start()
    to_twin(dp_id, me).start()

    def send_far(t):
        def body(k, carry):
            d = lax.rem(plane(k) - z + nz, nz)
            to_z(t, d).start()
            return carry
        lax.fori_loop(1, nz, body, 0)

    send_far(me)

    gu_load.wait()
    wd_load.wait()

    def widen(raw, padded, lead):
        block = 48
        blocks = raw.shape[-2] // block

        def body(i, carry):
            at = pl.ds(pl.multiple_of(i * block, 16), block)
            v = raw[lead + (at, slice(None))]
            for t in range(tp):
                part = v[:, t * cols:(t + 1) * cols]
                padded[lead + (at, pl.ds(t * wide, wide))] = jnp.concatenate(
                    [part, jnp.zeros((block, wide - cols), v.dtype)], axis=1)
            return carry
        lax.fori_loop(0, blocks, body, 0)
        rest = padded.shape[-2] - raw.shape[-2]
        padded[lead + (pl.ds(raw.shape[-2], rest), slice(None))] = jnp.zeros((rest, tp * wide), padded.dtype)

    widen(gu_raw, gu_pad, (0,))
    widen(gu_raw, gu_pad, (1,))

    arrived(dp_id, across_t)
    to_y(dp_id, across_t).start()
    to_twin(dp_id, across_t).start()
    send_far(across_t)
    widen(wd_raw, wd_pad, ())

    def far_arrival(k, t):
        b = plane(k) * ny + y
        arrived(b, t)
        to_y(b, t).start()
        to_twin(b, t).start()

    def act_copy(t, p, sem, target):
        view = act_buf.at[t, p]
        return pltpu.make_async_remote_copy(
            src_ref=view, dst_ref=view, send_sem=sem, recv_sem=r_act.at[t, p],
            device_id=target, device_id_type=MESH)

    def act_arrived(t, p):
        act_copy(t, p, r_act.at[t, p], twin).wait_recv()

    def out_copy(b):
        return pltpu.make_async_remote_copy(
            src_ref=out_buf.at[b], dst_ref=back_buf.at[dp_id], send_sem=s_out.at[b],
            recv_sem=r_out.at[dp_id], device_id=(b, me), device_id_type=MESH)

    def stats_tile(b):
        total = rows_buf[b, 0, :, wide - LANE:].astype(jnp.float32)
        for t in range(1, tp):
            total = total + rows_buf[b, t, :, wide - LANE:].astype(jnp.float32)
        total = jnp.where(lanes >= tail, total, 0.0)
        return total

    def row_scale(total):
        hit = (lanes == tail) | (lanes == tail + group) | (lanes == tail + 2 * group)
        squares = jnp.sum(jnp.where(hit, total, 0.0), axis=1, keepdims=True)
        return lax.rsqrt(squares / full + norm_eps)

    tile_n = 256
    n_tiles = wide // tile_n

    def up_project(p):
        scale = jnp.concatenate([row_scale(stats_tile(p * ny + b)) for b in range(ny)], axis=0)

        def body(n, carry):
            at = pl.ds(pl.multiple_of(n * tile_n, tile_n), tile_n)
            lhs = jnp.concatenate([
                jnp.concatenate([rows_buf[p * ny + b, t] for t in range(tp)], axis=1)
                for b in range(ny)], axis=0)
            gate = dot_t(lhs, gu_pad[0, at, :]) * scale
            up = dot_t(lhs, gu_pad[1, at, :]) * scale
            act_buf[me, p, :, at] = (gate * jax.nn.sigmoid(glu_alpha * gate) * (up + 1.0)).astype(jnp.bfloat16)
            return carry
        lax.fori_loop(0, n_tiles, body, 0)

    def down_project(p):
        def body(n, carry):
            at = pl.ds(pl.multiple_of(n * tile_n, tile_n), tile_n)
            lhs = jnp.concatenate([act_buf[t, p] for t in range(tp)], axis=1)
            out = dot_t(lhs, wd_pad[at, :]).astype(jnp.bfloat16)
            for b in range(ny):
                out_buf[p * ny + b, :, at] = out[b * seq:(b + 1) * seq]
            return carry
        lax.fori_loop(0, n_tiles, body, 0)

    def stage(k, carry):
        @pl.when(k < nz - 1)
        def _():
            far_arrival(k + 1, me)

        @pl.when(k < nz)
        def _():
            p = plane(k)
            for t in (me, across_t):
                b = p * ny + 1 - y
                arrived(b, t)
                to_twin(b, t).start()
            for b in range(ny):
                for t in (twin_t, corner_t):
                    arrived(p * ny + b, t)
            up_project(p)
            act_copy(me, p, s_act.at[0, p], across).start()
            act_copy(me, p, s_act.at[1, p], twin).start()

        @pl.when(k < nz - 1)
        def _():
            far_arrival(k + 1, across_t)

        @pl.when(k > 0)
        def _():
            p = plane(k - 1)
            act_arrived(across_t, p)
            act_copy(across_t, p, s_act.at[2, p], twin).start()
            act_arrived(twin_t, p)
            act_arrived(corner_t, p)
            down_project(p)
            for b in range(ny):
                @pl.when(p * ny + b != dp_id)
                def _():
                    out_copy(p * ny + b).start()

                @pl.when(p * ny + b == dp_id)
                def _():
                    back_buf[dp_id] = out_buf[dp_id]
        return carry

    lax.fori_loop(0, nz + 1, stage, 0)

    total = stats_tile(dp_id)
    scale = row_scale(total)
    shift = LANE - group
    summed = total + pltpu.roll(total, shift, 1) + pltpu.roll(pltpu.roll(total, shift, 1), shift, 1)
    square = lax.broadcasted_iota(jnp.int32, (seq, seq), 0) == lax.broadcasted_iota(jnp.int32, (seq, seq), 1)
    chosen = lanes < 0
    for k in range(ids_ref.shape[0]):
        named = ids_ref[k:k + 1, :].astype(jnp.float32)
        named = jnp.sum(jnp.where(square, named, 0.0), axis=1, keepdims=True).astype(jnp.int32)
        chosen = chosen | (lanes == named + tail + 1)
    raised = jnp.where(chosen, jnp.exp(jnp.where(chosen, summed * scale, 0.0)), 0.0)
    weights = raised / jnp.sum(raised, axis=1, keepdims=True)

    def wait_out(d, carry):
        b = lax.rem(dp_id + d, dp)
        pltpu.make_async_remote_copy(
            src_ref=back_buf.at[b], dst_ref=back_buf.at[b], send_sem=r_out.at[b],
            recv_sem=r_out.at[b], device_id=twin, device_id_type=MESH).wait_recv()
        return carry

    lax.fori_loop(1, dp, wait_out, 0)
    answer = res
    for e in range(dp):
        answer = answer + weights[:, tail + 1 + e:tail + 2 + e] * back_buf[e].astype(jnp.float32)
    out_ref[...] = answer[:, :cols]

    piece(dp_id, me, s_x, across).wait_send()
    for t in (me, across_t):
        for d in range(1, nz):
            to_z(t, d).wait_send()
        for p in range(nz):
            to_y(p * ny + y, t).wait_send()
            for b in range(ny):
                to_twin(p * ny + b, t).wait_send()
    for p in range(nz):
        act_copy(me, p, s_act.at[0, p], across).wait_send()
        act_copy(me, p, s_act.at[1, p], twin).wait_send()
        act_copy(across_t, p, s_act.at[2, p], twin).wait_send()
    for d in range(1, dp):
        out_copy(lax.rem(dp_id + d, dp)).wait_send()


def moe(res, gain, router, ids, gate_up, w_down, dp, ny, tp, collective_id):
    seq, wide = res.shape
    cols = gain.shape[0] // tp
    full = gate_up.shape[2]
    experts = router.shape[0]
    nz = dp // ny
    bf = jnp.bfloat16
    dma = pltpu.SemaphoreType.DMA
    return pl.pallas_call(
        functools.partial(moe_kernel, dp, ny, tp, experts),
        out_shape=jax.ShapeDtypeStruct((seq, cols), jnp.float32),
        in_specs=[pl.BlockSpec(memory_space=pltpu.VMEM)] * 4 + [pl.BlockSpec(memory_space=pl.ANY)] * 2,
        out_specs=pl.BlockSpec(memory_space=pltpu.VMEM),
        scratch_shapes=[
            pltpu.VMEM((dp, tp, seq, wide), bf),
            pltpu.VMEM((2, cols, full), bf),
            pltpu.VMEM((2, wide, tp * wide), bf),
            pltpu.VMEM((cols, full), bf),
            pltpu.VMEM((wide, tp * wide), bf),
            pltpu.VMEM((tp, nz, ny * seq, wide), bf),
            pltpu.VMEM((dp, seq, wide), bf),
            pltpu.VMEM((dp, seq, wide), bf),
            dma((2,)), dma((dp, tp)), dma, dma((dp, tp // CORES)), dma((tp // CORES, nz)), dma((dp, tp)),
            dma((3, nz)), dma((tp, nz)), dma((dp,)), dma((dp,)),
        ],
        compiler_params=pltpu.CompilerParams(
            collective_id=collective_id, has_side_effects=True, vmem_limit_bytes=56 * 2**20),
        cost_estimate=pl.CostEstimate(flops=6 * dp * seq * full * cols, bytes_accessed=6 * full * cols, transcendentals=0),
    )(res, gain[None, :], router, ids, gate_up, w_down)


def attend_kernel(
    tp, kv_heads, group_size, head_size,
    tok_ref, gain_ref, inverse_ref, pos_ref, sink_ref, wq_hbm, wkv_hbm, wo_hbm, cache_hbm, out_ref,
    tok_buf, wq_buf, wkv_raw, wkv_wide, wkv_buf, wo_buf, cache_buf, q_rows, new_rows, pos_rows, att_rows,
    part_buf, got_buf, load_sem, send_sem, recv_tok, recv_part,
):
    dp_id = lax.axis_index("dp")
    me = lax.axis_index("tp")
    core, chip = lax.rem(me, CORES), me // CORES
    seq, cols = tok_ref.shape
    wide = out_ref.shape[1]
    window = cache_hbm.shape[2]
    heads = kv_heads * group_size
    twin_t = chip * CORES + 1 - core
    across_t = (1 - chip) * CORES + core
    corner_t = (1 - chip) * CORES + 1 - core
    twin, across = (dp_id, twin_t), (dp_id, across_t)

    loads = [
        pltpu.make_async_copy(src, dst, load_sem.at[i]) for i, (src, dst) in enumerate(
            [(wkv_hbm, wkv_raw), (wq_hbm, wq_buf), (cache_hbm, cache_buf), (wo_hbm, wo_buf)])
    ]
    for load in loads:
        load.start()
    own = pltpu.make_async_copy(tok_ref, tok_buf.at[me], load_sem.at[4])
    own.start()
    greet([twin, across])

    def token_copy(src, t, i, target):
        return pltpu.make_async_remote_copy(
            src_ref=src, dst_ref=tok_buf.at[t], send_sem=send_sem.at[i], recv_sem=recv_tok.at[t],
            device_id=target, device_id_type=MESH)

    def token_arrived(t):
        token_copy(tok_buf.at[t], t, 0, twin).wait_recv()

    sent = [token_copy(tok_ref, me, 0, across), token_copy(tok_ref, me, 1, twin)]
    for copy in sent:
        copy.start()

    lanes = lax.broadcasted_iota(jnp.int32, (seq, LANE), 1)

    def column(row):
        n = row.shape[1]
        square = lax.broadcasted_iota(jnp.int32, (n, n), 0) == lax.broadcasted_iota(jnp.int32, (n, n), 1)
        return jnp.sum(jnp.where(square, row, 0.0), axis=1, keepdims=True)

    position = jnp.broadcast_to(column(pos_ref[...].astype(jnp.float32)), (seq, LANE))
    angles = position * inverse_ref[...]
    cosine = jnp.cos(angles)
    front = lax.rem(lanes, head_size) < head_size // 2
    sine = jnp.where(front, -jnp.sin(angles), jnp.sin(angles))
    for h in range(heads):
        pos_rows[pl.ds(h, seq, stride=heads), :] = position
    sink = jnp.broadcast_to(column(sink_ref[...]), (heads, LANE))
    sink = jnp.concatenate([sink] * 8, axis=0)

    loads[0].wait()
    kv_rows = wkv_raw.shape[0]
    step = kv_rows // 30

    def split(i, carry):
        at = pl.multiple_of(i * step, 16)
        wkv_wide[...] = wkv_raw[pl.ds(at, step), :].astype(jnp.float32)
        half = pl.ds(pl.multiple_of(i * (step // kv_heads), 16), step // kv_heads)
        for h in range(kv_heads):
            wkv_buf[half, h * LANE:(h + 1) * LANE] = wkv_wide[
                pl.ds(h, step // kv_heads, stride=kv_heads), :].astype(jnp.bfloat16)
        return carry
    lax.fori_loop(0, 30, split, 0)

    token_arrived(across_t)
    forward = token_copy(tok_buf.at[across_t], across_t, 2, twin)
    forward.start()
    sent.append(forward)
    own.wait()
    token_arrived(twin_t)
    token_arrived(corner_t)
    loads[1].wait()

    pieces = [tok_buf[t].astype(jnp.float32) for t in range(tp)]
    squares = jnp.sum(pieces[0] * pieces[0], axis=1, keepdims=True)
    for v in pieces[1:]:
        squares = squares + jnp.sum(v * v, axis=1, keepdims=True)
    scale = lax.rsqrt(squares / (tp * cols) + norm_eps)
    queries, fresh = 0.0, 0.0
    for t in range(tp):
        at = slice(t * cols, (t + 1) * cols)
        normed = (pieces[t] * scale * gain_ref[:, at]).astype(jnp.bfloat16)
        queries = queries + jnp.dot(normed, wq_buf[at, :], preferred_element_type=jnp.float32)
        fresh = fresh + jnp.dot(normed, wkv_buf[at, :], preferred_element_type=jnp.float32)

    def turned(v):
        swapped = jnp.where(
            front, pltpu.roll(v, LANE - head_size // 2, 1), pltpu.roll(v, head_size // 2, 1))
        return v * cosine + swapped * sine

    def rounded(v):
        return v.astype(jnp.bfloat16).astype(jnp.float32)

    low = lanes < head_size
    for h in range(heads):
        if h % 2 == 0:
            pair = rounded(turned(queries[:, h // 2 * LANE:(h // 2 + 1) * LANE]))
        if h % group_size == 0:
            k = h // group_size
            entry = fresh[:, k * LANE:(k + 1) * LANE]
            entry = rounded(jnp.where(low, turned(entry), entry))
        own_q = pair if h % 2 == 0 else pltpu.roll(pair, head_size, 1)
        q_rows[pl.ds(h, seq, stride=heads), :] = jnp.where(low, own_q, 0.0)
        new_rows[pl.ds(h, seq, stride=heads), :] = entry

    loads[2].wait()
    batch = 8
    rows = batch * heads
    slot = lax.broadcasted_iota(jnp.int32, (rows, LANE), 1)
    upper = lax.broadcasted_iota(jnp.int32, (heads, LANE), 0) < group_size
    score_scale = head_size ** (-0.5)

    def attend(i, carry):
        at = pl.ds(pl.multiple_of(i * rows, rows), rows)
        q = q_rows[at, :]
        entry = new_rows[at, :]
        pos = pos_rows[at, :].astype(jnp.int32)
        raw = []
        for s in range(batch):
            qs = q[s * heads:(s + 1) * heads]
            lhs = jnp.concatenate(
                [jnp.where(upper, qs, 0.0), jnp.where(upper, 0.0, qs)], axis=1).astype(jnp.bfloat16)
            rhs = jnp.concatenate([cache_buf[i * batch + s, k] for k in range(kv_heads)], axis=1)
            raw.append(dot_t(lhs, rhs))
        scores = jnp.concatenate(raw, axis=0) * score_scale
        fresh_score = jnp.sum(q * entry, axis=1, keepdims=True) * score_scale
        current = slot == lax.rem(pos, window)
        scores = jnp.where(current, fresh_score, jnp.where(slot <= pos, scores, -jnp.inf))
        peak = jnp.maximum(jnp.max(scores, axis=1, keepdims=True), sink)
        raised = jnp.exp(scores - peak)
        denominator = jnp.sum(raised, axis=1, keepdims=True) + jnp.exp(sink - peak)
        probs = rounded(raised / denominator)
        fresh_prob = jnp.sum(jnp.where(current, probs, 0.0), axis=1, keepdims=True)
        probs = jnp.where(current, 0.0, probs)
        mixed = []
        for s in range(batch):
            lhs = probs[s * heads:(s + 1) * heads].astype(jnp.bfloat16)
            rhs = jnp.concatenate([cache_buf[i * batch + s, k] for k in range(kv_heads)], axis=1)
            both = jnp.dot(lhs, rhs, preferred_element_type=jnp.float32)
            mixed.append(jnp.where(upper, both[:, :LANE], both[:, LANE:]))
        att_rows[at, :] = jnp.concatenate(mixed, axis=0) + fresh_prob * entry
        return carry

    lax.fori_loop(0, seq // batch, attend, 0)

    tiles = []
    for j in range(heads // 2):
        even = att_rows[pl.ds(2 * j, seq, stride=heads), :]
        odd = att_rows[pl.ds(2 * j + 1, seq, stride=heads), :]
        tiles.append(jnp.where(low, pltpu.roll(even, head_size, 1), odd).astype(jnp.bfloat16))
    attended = jnp.concatenate(tiles, axis=1)
    loads[3].wait()

    def share(t):
        return dot_t(attended, wo_buf[pl.ds(pl.multiple_of(t * cols, 16), cols), :])

    def part_copy(i, target):
        return pltpu.make_async_remote_copy(
            src_ref=part_buf.at[i], dst_ref=got_buf.at[i], send_sem=send_sem.at[3 + i],
            recv_sem=recv_part.at[i], device_id=target, device_id_type=MESH)

    parts = [part_copy(0, twin), part_copy(1, across), part_copy(2, twin)]
    part_buf[0] = share(corner_t).astype(jnp.bfloat16)
    parts[0].start()
    far = share(across_t)
    parts[0].wait_recv()
    part_buf[1] = (far + got_buf[0].astype(jnp.float32)).astype(jnp.bfloat16)
    parts[1].start()
    part_buf[2] = share(twin_t).astype(jnp.bfloat16)
    parts[2].start()
    total = tok_ref[...].astype(jnp.float32) + share(me)
    parts[2].wait_recv()
    total = total + got_buf[2].astype(jnp.float32)
    parts[1].wait_recv()
    total = total + got_buf[1].astype(jnp.float32)
    out_ref[...] = jnp.concatenate([total, jnp.zeros((seq, wide - cols), jnp.float32)], axis=1)
    for copy in sent + parts:
        copy.wait_send()


def attend_block(tokens, gain, positions, sinks, w_query, w_keyvalue, w_out, cache, tp, collective_id):
    seq, cols = tokens.shape
    wide = pad_up(cols, 256)
    full = tp * cols
    kv_heads, window, entry = cache.shape[1:]
    head_size = entry // 2
    heads = w_query.shape[1] // head_size
    exponent = np.arange(LANE) % (head_size // 2) * (2.0 / head_size)
    inverse = jnp.asarray(rope_base ** -exponent, jnp.float32)[None, :]
    bf, f32 = jnp.bfloat16, jnp.float32
    dma = pltpu.SemaphoreType.DMA
    return pl.pallas_call(
        functools.partial(attend_kernel, tp, kv_heads, heads // kv_heads, head_size),
        out_shape=jax.ShapeDtypeStruct((seq, wide), f32),
        in_specs=[pl.BlockSpec(memory_space=pltpu.VMEM)] * 5 + [pl.BlockSpec(memory_space=pl.ANY)] * 4,
        out_specs=pl.BlockSpec(memory_space=pltpu.VMEM),
        scratch_shapes=[
            pltpu.VMEM((tp, seq, cols), bf),
            pltpu.VMEM(w_query.shape, bf),
            pltpu.VMEM((full * kv_heads, LANE), bf),
            pltpu.VMEM((full * kv_heads // 30, LANE), f32),
            pltpu.VMEM((full, kv_heads * LANE), bf),
            pltpu.VMEM((full, heads * head_size), bf),
            pltpu.VMEM(cache.shape, bf),
            pltpu.VMEM((seq * heads, LANE), f32),
            pltpu.VMEM((seq * heads, LANE), f32),
            pltpu.VMEM((seq * heads, LANE), f32),
            pltpu.VMEM((seq * heads, LANE), f32),
            pltpu.VMEM((3, seq, cols), bf),
            pltpu.VMEM((3, seq, cols), bf),
            dma((5,)), dma((6,)), dma((tp,)), dma((3,)),
        ],
        compiler_params=pltpu.CompilerParams(
            collective_id=collective_id, has_side_effects=True, vmem_limit_bytes=63 * 2**20),
        cost_estimate=pl.CostEstimate(
            flops=2 * seq * full * heads * head_size * 3, bytes_accessed=8 * full * heads * head_size,
            transcendentals=0),
    )(tokens, gain[None, :], inverse, positions[None, :], sinks[None, :],
      w_query, w_keyvalue.reshape(full * kv_heads, LANE), w_out.T, cache)


def activate(mixed_in, ff_local):
    gate_part = mixed_in[..., :ff_local]
    up_part = mixed_in[..., ff_local:]
    return (gate_part * jax.nn.sigmoid(glu_alpha * gate_part) * (up_part + 1.0)).astype(
        jnp.bfloat16
    )


def on_device(
    tokens,
    attn_gain,
    w_query,
    w_keyvalue,
    attn_sinks,
    w_out,
    window_cache,
    positions,
    moe_gain,
    router,
    gate_up,
    w_down,
    expert_ids,
):
    tp_count = lax.axis_size("tp")
    dp_count = lax.axis_size("dp")
    seq_count, col_count = tokens.shape
    full_width = col_count * tp_count
    col_start = lax.axis_index("tp") * col_count
    head_size = w_keyvalue.shape[2] // 2
    kv_local = w_keyvalue.shape[1]
    q_local = w_query.shape[1] // head_size
    group_size = q_local // kv_local
    window = window_cache.shape[2]
    experts = router.shape[1]
    ny = 2 ** (int(math.log2(dp_count)) // 2)
    if (tp_count, ny, gate_up.shape[0], kv_local, group_size, window, 2 * head_size) == (
            2 * CORES, 2, 1, 2, 4, LANE, LANE):
        residual = attend_block(
            tokens, attn_gain, positions, attn_sinks, w_query, w_keyvalue, w_out, window_cache, tp_count, 0)
        return moe(
            residual, moe_gain, router.T, expert_ids.T, jnp.transpose(gate_up[0], (1, 2, 0)), w_down[0].T,
            dp_count, ny, tp_count, 1)
    moe_slice = lax.dynamic_slice_in_dim(moe_gain, col_start, col_count)
    tok_wide = tokens.astype(jnp.float32)
    kv_flat = w_keyvalue.reshape(full_width, kv_local * 2 * head_size)
    whole_rows = feature_gather(tokens, tp_count, 2, 0).astype(jnp.float32)
    attn_sq = jnp.sum(whole_rows * whole_rows, axis=1, keepdims=True)
    piece_rows = (
        whole_rows * lax.rsqrt(attn_sq / full_width + norm_eps) * attn_gain[None, :]
    ).astype(jnp.bfloat16)
    queries = jnp.dot(piece_rows, w_query, preferred_element_type=jnp.float32)
    fresh_rows = jnp.dot(piece_rows, kv_flat, preferred_element_type=jnp.float32)
    cosine, sine_table = rope_tables(positions, head_size)
    rot_queries = rotate(
        queries.reshape(seq_count, q_local, head_size), cosine[:, None, :], sine_table[:, None, :]
    ).astype(jnp.bfloat16)
    fresh_rows = fresh_rows.reshape(seq_count, kv_local, 2 * head_size)
    new_key = rotate(fresh_rows[..., :head_size], cosine[:, None, :], sine_table[:, None, :])
    new_entry = jnp.concatenate([new_key, fresh_rows[..., head_size:]], axis=-1).astype(
        jnp.bfloat16
    )
    slot_ids = jnp.arange(window, dtype=jnp.int32)
    is_current = slot_ids[None, :] == (positions % window)[:, None]
    is_valid = (positions[:, None] - slot_ids[None, :]) % window <= positions[:, None]
    is_valid = is_valid & ~is_current
    grouped = rot_queries.reshape(seq_count, kv_local, group_size, head_size)
    scores = jnp.einsum(
        "skgh,skwh->skgw", grouped, window_cache[..., :head_size], preferred_element_type=jnp.float32
    ) * head_size ** (-0.5)
    scores = jnp.where(is_valid[:, None, None, :], scores, -jnp.inf)
    new_wide = new_entry.astype(jnp.float32)[:, :, None, :]
    new_score = jnp.sum(
        grouped.astype(jnp.float32) * new_wide[..., :head_size], axis=-1, keepdims=True
    ) * head_size ** (-0.5)
    sink_col = attn_sinks.reshape(kv_local, group_size)[None, :, :, None]
    peak_score = jnp.maximum(
        jnp.maximum(jnp.max(scores, axis=-1, keepdims=True), new_score), sink_col
    )
    raised = jnp.exp(scores - peak_score)
    raised_new = jnp.exp(new_score - peak_score)
    denominator = (
        jnp.sum(raised, axis=-1, keepdims=True) + raised_new + jnp.exp(sink_col - peak_score)
    )
    prob_bf = (raised / denominator).astype(jnp.bfloat16)
    prob_new = (raised_new / denominator).astype(jnp.bfloat16).astype(jnp.float32)
    attended = jnp.einsum(
        "skgw,skwh->skgh", prob_bf, window_cache[..., head_size:], preferred_element_type=jnp.float32
    )
    attended = (attended + prob_new * new_wide[..., head_size:]).astype(jnp.bfloat16)
    partial_out = jnp.einsum(
        "sh,htc->tsc",
        attended.reshape(seq_count, q_local * head_size),
        w_out.reshape(q_local * head_size, tp_count, col_count),
        preferred_element_type=jnp.float32,
    ).astype(jnp.bfloat16)
    residual = tok_wide + share_sum(partial_out, tp_count, True, 2)
    top_count = expert_ids.shape[1]
    local_experts = gate_up.shape[0]
    ff_local = gate_up.shape[3]
    capacity = min(seq_count, max(2, 8 * seq_count * top_count // (3 * experts)))
    moe_sq = jnp.sum(residual * residual, axis=1)
    router_wide = router.astype(jnp.float32)
    gained = residual * moe_slice[None, :]
    raw_logits = jnp.dot(gained, router_wide, precision=lax.Precision.HIGHEST)
    stats = share_sum(
        jnp.concatenate([moe_sq[:, None], raw_logits], axis=1)[None], tp_count, False, 3
    )
    moe_scale = lax.rsqrt(stats[:, :1] / full_width + norm_eps)
    logits = stats[:, 1:] * moe_scale
    hidden_rows = (gained * moe_scale).astype(jnp.bfloat16)
    expert_iota = jnp.arange(experts, dtype=jnp.int32)
    chosen = expert_ids[:, :, None] == expert_iota[None, None, :]
    picked = jnp.sum(jnp.where(chosen, logits[:, None, :], 0.0), axis=-1)
    raised_logits = jnp.exp(picked)
    route_weights = raised_logits / jnp.sum(raised_logits, axis=1, keepdims=True)
    gate_up_flat = gate_up.reshape(local_experts, full_width, 2 * ff_local)
    if capacity >= seq_count:
        token_weights = jnp.sum(jnp.where(chosen, route_weights[:, :, None], 0.0), axis=1)
        all_rows = full_gather(hidden_rows, dp_count, tp_count, 1)
        half = seq_count // 2
        part = dp_count * half
        acts = [
            activate(
                jnp.dot(all_rows, gate_up_flat[e], preferred_element_type=jnp.float32), ff_local
            )
            for e in range(local_experts)
        ]
        pieces = []
        for h in range(2):
            outs = []
            for e in range(local_experts):
                act_all = feature_gather(
                    acts[e][h * part : (h + 1) * part], tp_count, dp_count // 2, 4 + 2 * e + h
                )
                out = jnp.dot(act_all, w_down[e], preferred_element_type=jnp.float32)
                outs.append(out.astype(jnp.bfloat16).reshape(dp_count, half, col_count))
            returned = lax.all_to_all(
                jnp.stack(outs, axis=1), "dp", split_axis=0, concat_axis=0, tiled=True
            )
            back = returned.reshape(experts, half, col_count)
            mine = slice(h * half, (h + 1) * half)
            total = residual[mine]
            for e in range(experts):
                total = total + token_weights[mine, e : e + 1] * back[e].astype(jnp.float32)
            pieces.append(total)
        total = jnp.concatenate(pieces, axis=0)
        return total
    assign = expert_ids.reshape(-1)
    onehot = (assign[:, None] == expert_iota[None, :]).astype(jnp.int32)
    earlier = jnp.cumsum(onehot, axis=0) - onehot
    slot_of = jnp.sum(earlier * onehot, axis=1)
    target = (assign * capacity + slot_of).reshape(seq_count, top_count)
    spot_ids = jnp.arange(experts * capacity, dtype=jnp.int32)
    slot_hits = target[:, :, None] == spot_ids[None, None, :]
    placer = jnp.transpose(jnp.any(slot_hits, axis=1)).astype(jnp.bfloat16)
    combiner = jnp.sum(jnp.where(slot_hits, route_weights[:, :, None], 0.0), axis=1)
    placed = jnp.dot(placer, hidden_rows, preferred_element_type=jnp.float32).astype(jnp.bfloat16)
    mixed_in = jnp.einsum(
        "gecd,edf->gecf",
        lax.all_gather(
            lax.all_to_all(
                placed.reshape(dp_count, local_experts, capacity, hidden_rows.shape[1]),
                "dp",
                split_axis=0,
                concat_axis=0,
                tiled=True,
            ),
            "tp",
            axis=3,
            tiled=True,
        ),
        gate_up_flat,
        preferred_element_type=jnp.float32,
    )
    act_rows = activate(mixed_in, ff_local)
    answered = jnp.einsum(
        "gecf,efd->gecd",
        lax.all_gather(act_rows, "tp", axis=3, tiled=True),
        w_down,
        preferred_element_type=jnp.float32,
    ).astype(jnp.bfloat16)
    returned = lax.all_to_all(answered, "dp", split_axis=0, concat_axis=0, tiled=True)
    flat_back = returned.reshape(experts * capacity, col_count).astype(jnp.float32)
    moe_out = jnp.dot(combiner, flat_back, precision=lax.Precision.HIGHEST)
    return residual + moe_out


def solution(mesh):
    in_specs = (
        P("dp", "tp"),
        P(),
        P(None, "tp"),
        P(None, "tp", None),
        P("tp"),
        P("tp", None),
        P("dp", "tp", None, None),
        P("dp"),
        P(),
        P("tp", None),
        P("dp", None, None, "tp"),
        P("dp", None, "tp"),
        P("dp", None),
    )
    out_specs = P("dp", "tp")
    return jax.shard_map(
        on_device, mesh=mesh, in_specs=in_specs, out_specs=out_specs, check_vma=False
    )
```

```python
import functools
import math

import jax
import jax.numpy as jnp
import numpy as np
from jax import lax
from jax.experimental import pallas as pl
from jax.experimental.pallas import tpu as pltpu
from jax.sharding import PartitionSpec as P

norm_eps = 1e-05
rope_base = 150000.0
glu_alpha = 1.702


def rope_tables(positions, head_size):
    half_size = head_size // 2
    exponent = jnp.arange(half_size, dtype=jnp.float32) * (2.0 / head_size)
    inverse = jnp.power(jnp.float32(rope_base), -exponent)
    angles = positions.astype(jnp.float32)[:, None] * inverse[None, :]
    return (jnp.cos(angles), jnp.sin(angles))


def rotate(values, cosine, sine_table):
    half_size = values.shape[-1] // 2
    first_half = values[..., :half_size]
    second_half = values[..., half_size:]
    return jnp.concatenate(
        [
            first_half * cosine - second_half * sine_table,
            second_half * cosine + first_half * sine_table,
        ],
        axis=-1,
    )


MESH = pl.DeviceIdType.MESH
CORES = 2


def greet(partners):
    barrier = pltpu.get_barrier_semaphore()
    for partner in partners:
        pl.semaphore_signal(barrier, inc=1, device_id=partner, device_id_type=MESH)
    pl.semaphore_wait(barrier, len(partners))


def feature_gather_kernel(tp, chunks, x_ref, out_ref, buf, own_sem, send_x, send_c, recv):
    chips = tp // CORES
    dp_id = lax.axis_index("dp")
    me = lax.axis_index("tp")
    core = lax.rem(me, CORES)
    chip = me // CORES
    rows, cols = x_ref.shape
    step = rows // chunks
    twin = (dp_id, chip * CORES + (1 - core))
    others = [lax.rem(chip + d, chips) * CORES + core for d in range(1, chips)]
    sources = [lax.rem(chip + chips - d, chips) * CORES + core for d in range(1, chips)]
    own = pltpu.make_async_copy(x_ref, buf.at[me], own_sem)
    own.start()
    greet([twin] + [(dp_id, other) for other in others])

    def piece(k):
        return pl.ds(k * step, step)

    def send(src, origin, k, sem, target):
        return pltpu.make_async_remote_copy(
            src_ref=src, dst_ref=buf.at[origin, piece(k)], send_sem=sem,
            recv_sem=recv.at[origin, k], device_id=target, device_id_type=MESH)

    sent = []
    for k in range(chunks):
        for d in range(chips - 1):
            sent.append(send(x_ref.at[piece(k)], me, k, send_x.at[d, k], (dp_id, others[d])))
            sent[-1].start()
    for k in range(chunks):
        sent.append(send(x_ref.at[piece(k)], me, k, send_c.at[0, k], twin))
        sent[-1].start()
    own.wait()
    for k in range(chunks):
        for d in range(chips - 1):
            origin = sources[d]
            forward = send(buf.at[origin, piece(k)], origin, k, send_c.at[d + 1, k], twin)
            forward.wait_recv()
            forward.start()
            sent.append(forward)
        if k:
            finish(tp, k - 1, step, chip, core, chips, buf, recv, out_ref, send, twin)
    finish(tp, chunks - 1, step, chip, core, chips, buf, recv, out_ref, send, twin)
    for copy in sent:
        copy.wait_send()


def finish(tp, k, step, chip, core, chips, buf, recv, out_ref, send, twin):
    cols = buf.shape[2]
    part = pl.ds(k * step, step)
    for d in range(chips):
        origin = lax.rem(chip + d, chips) * CORES + (1 - core)
        pltpu.make_async_remote_copy(
            src_ref=buf.at[origin, part], dst_ref=buf.at[origin, part], send_sem=recv.at[origin, k],
            recv_sem=recv.at[origin, k], device_id=twin, device_id_type=MESH).wait_recv()
    for t in range(tp):
        out_ref[part, t * cols:(t + 1) * cols] = buf[t, part, :]


def feature_gather(x, tp, chunks, collective_id):
    rows, cols = x.shape
    chips = tp // CORES
    return pl.pallas_call(
        functools.partial(feature_gather_kernel, tp, chunks),
        out_shape=jax.ShapeDtypeStruct((rows, tp * cols), x.dtype),
        in_specs=[pl.BlockSpec(memory_space=pltpu.VMEM)],
        out_specs=pl.BlockSpec(memory_space=pltpu.VMEM),
        scratch_shapes=[
            pltpu.VMEM((tp, rows, cols), x.dtype),
            pltpu.SemaphoreType.DMA,
            pltpu.SemaphoreType.DMA((max(chips - 1, 1), chunks)),
            pltpu.SemaphoreType.DMA((chips, chunks)),
            pltpu.SemaphoreType.DMA((tp, chunks)),
        ],
        compiler_params=pltpu.CompilerParams(
            collective_id=collective_id, has_side_effects=True, vmem_limit_bytes=48 * 2**20),
        cost_estimate=pl.CostEstimate(flops=0, bytes_accessed=rows * cols * tp * 16, transcendentals=0),
    )(x)


def share_sum_kernel(tp, scatter, x_ref, out_ref, buf, send_sem, recv_sem):
    chips = tp // CORES
    dp_id = lax.axis_index("dp")
    me = lax.axis_index("tp")
    core = lax.rem(me, CORES)
    chip = me // CORES
    others = [
        lax.rem(chip + d, chips) * CORES + c for d in range(1, chips) for c in range(CORES)
    ] + [chip * CORES + (1 - core)]
    greet([(dp_id, other) for other in others])
    sent = []
    for i, other in enumerate(others):
        sent.append(pltpu.make_async_remote_copy(
            src_ref=x_ref.at[other if scatter else 0], dst_ref=buf.at[me], send_sem=send_sem.at[i],
            recv_sem=recv_sem.at[me], device_id=(dp_id, other), device_id_type=MESH))
        sent[-1].start()
    total = x_ref[me if scatter else 0].astype(jnp.float32)
    for i in reversed(range(len(others))):
        other = others[i]
        pltpu.make_async_remote_copy(
            src_ref=buf.at[other], dst_ref=buf.at[other], send_sem=send_sem.at[i],
            recv_sem=recv_sem.at[other], device_id=(dp_id, other), device_id_type=MESH).wait_recv()
        total = total + buf[other].astype(jnp.float32)
    out_ref[...] = total
    for copy in sent:
        copy.wait_send()


def share_sum(x, tp, scatter, collective_id):
    rows, cols = x.shape[1:]
    return pl.pallas_call(
        functools.partial(share_sum_kernel, tp, scatter),
        out_shape=jax.ShapeDtypeStruct((rows, cols), jnp.float32),
        in_specs=[pl.BlockSpec(memory_space=pltpu.VMEM)],
        out_specs=pl.BlockSpec(memory_space=pltpu.VMEM),
        scratch_shapes=[
            pltpu.VMEM((tp, rows, cols), x.dtype),
            pltpu.SemaphoreType.DMA((tp - 1,)),
            pltpu.SemaphoreType.DMA((tp,)),
        ],
        compiler_params=pltpu.CompilerParams(
            collective_id=collective_id, has_side_effects=True, vmem_limit_bytes=16 * 2**20),
        cost_estimate=pl.CostEstimate(flops=0, bytes_accessed=rows * cols * tp * 16, transcendentals=0),
    )(x)


def full_gather_kernel(dp, ny, tp, x_ref, out_ref, buf, own_sem, send_z, send_x, send_y, send_c, recv):
    nz, nx = dp // ny, tp // CORES
    dp_id = lax.axis_index("dp")
    me = lax.axis_index("tp")
    core, x = lax.rem(me, CORES), me // CORES
    z, y = dp_id // ny, lax.rem(dp_id, ny)
    rows, cols = x_ref.shape
    half = rows // 2

    def place(pz, py, px, pc=core):
        return (pz * ny + py, px * CORES + pc)

    def around(v, d, n):
        return lax.rem(v + d, n)

    own = pltpu.make_async_copy(x_ref, buf.at[dp_id, me], own_sem)
    own.start()
    twin = place(z, y, x, 1 - core)
    x_others = [place(z, y, around(x, d, nx)) for d in range(1, nx)]
    y_others = [place(z, around(y, d, ny), x) for d in range(1, ny)]
    ring = [place(lax.rem(z + d, nz), y, x) for d in sorted({1 % nz, nz - 1} - {0})]
    greet([twin] + x_others + y_others + ring)
    own.wait()

    def copy(origin, h, sem, target):
        view = buf.at[origin[0], origin[1], pl.ds(h * half, half)]
        return pltpu.make_async_remote_copy(
            src_ref=view, dst_ref=view, send_sem=sem.at[origin[0], origin[1] // CORES, h],
            recv_sem=recv.at[origin[0], origin[1], h], device_id=target, device_id_type=MESH)

    def arrived(origin, h):
        view = buf.at[origin[0], origin[1], pl.ds(h * half, half)]
        pltpu.make_async_remote_copy(
            src_ref=view, dst_ref=view, send_sem=recv.at[origin[0], origin[1], h],
            recv_sem=recv.at[origin[0], origin[1], h], device_id=twin, device_id_type=MESH).wait_recv()

    def to_x(origin, h, act):
        for d in range(nx - 1):
            act(copy(origin, h, send_x.at[d], x_others[d]))

    def to_y(origin, h, act):
        for d in range(ny - 1):
            act(copy(origin, h, send_y.at[d], y_others[d]))

    def to_twin(origin, h, act):
        act(copy(origin, h, send_c, twin))

    def start(c):
        c.start()

    def ended(c):
        c.wait_send()

    def spread(origin, act):
        to_x(origin, 0, act)
        to_y(origin, 1, act)
        to_y(origin, 0, act)
        to_x(origin, 1, act)
        for h in range(2):
            to_twin(origin, h, act)

    def sideways(pz, act, wait):
        for d in range(1, nx):
            origin = place(pz, y, around(x, d, nx))
            if wait:
                arrived(origin, 0)
            to_y(origin, 0, act)
            to_twin(origin, 0, act)
        for d in range(1, ny):
            origin = place(pz, around(y, d, ny), x)
            if wait:
                arrived(origin, 1)
            to_x(origin, 1, act)
            to_twin(origin, 1, act)

    def last(pz, act, wait):
        for d in range(1, ny):
            for e in range(nx):
                origin = place(pz, around(y, d, ny), around(x, e, nx))
                if wait:
                    arrived(origin, 0)
                to_twin(origin, 0, act)
        for d in range(1, nx):
            for e in range(ny):
                origin = place(pz, around(y, e, ny), around(x, d, nx))
                if wait:
                    arrived(origin, 1)
                to_twin(origin, 1, act)

    def above(pz, act):
        @pl.when(z > 0)
        def _():
            for h in range(2):
                act(copy(place(pz, y, x), h, send_z.at[0], place(z - 1, y, x)))

    def below(pz, act):
        @pl.when(z < nz - 1)
        def _():
            for h in range(2):
                act(copy(place(pz, y, x), h, send_z.at[1], place(z + 1, y, x)))

    mine = place(z, y, x)
    above(z, start)
    below(z, start)
    spread(mine, start)

    def first_wave(pz, onward):
        origin = place(pz, y, x)
        arrived(origin, 0)
        arrived(origin, 1)
        onward(pz, start)
        spread(origin, start)

    sideways(z, start, True)
    for s in range(1, nz):
        for pz, ok, onward in ((z - s, z - s >= 0, below), (z + s, z + s < nz, above)):
            pl.when(ok)(functools.partial(first_wave, pz, onward))
        for pz, ok in ((z - s, z - s >= 0), (z + s, z + s < nz)):
            pl.when(ok)(functools.partial(sideways, pz, start, True))
        if s == 1:
            last(z, start, True)
        else:
            for pz, ok in ((z - s + 1, z - s + 1 >= 0), (z + s - 1, z + s - 1 < nz)):
                pl.when(ok)(functools.partial(last, pz, start, True))
    for pz, ok in ((z - nz + 1, z - nz + 1 >= 0), (z + nz - 1, z + nz - 1 < nz)):
        pl.when(ok)(functools.partial(last, pz, start, True))

    for b in range(dp):
        for px in range(nx):
            for h in range(2):
                arrived((b, px * CORES + 1 - core), h)
        for h in range(2):
            start_row = (h * dp + b) * half
            for t in range(tp):
                out_ref[start_row:start_row + half, t * cols:(t + 1) * cols] = buf[
                    b, t, h * half:(h + 1) * half
                ]

    def ends(pz, onward=None):
        if onward is not None:
            onward(pz, ended)
        spread(place(pz, y, x), ended)
        sideways(pz, ended, False)
        last(pz, ended, False)

    above(z, ended)
    below(z, ended)
    ends(z)
    for s in range(1, nz):
        for pz, ok, onward in ((z - s, z - s >= 0, below), (z + s, z + s < nz, above)):
            pl.when(ok)(functools.partial(ends, pz, onward))


def full_gather(x, dp, tp, collective_id):
    rows, cols = x.shape
    nx = tp // CORES
    ny = 2 ** (int(math.log2(dp)) // 2)
    per_piece = (dp, nx, 2)
    return pl.pallas_call(
        functools.partial(full_gather_kernel, dp, ny, tp),
        out_shape=jax.ShapeDtypeStruct((dp * rows, tp * cols), x.dtype),
        in_specs=[pl.BlockSpec(memory_space=pltpu.VMEM)],
        out_specs=pl.BlockSpec(memory_space=pltpu.VMEM),
        scratch_shapes=[
            pltpu.VMEM((dp, tp, rows, cols), x.dtype),
            pltpu.SemaphoreType.DMA,
            pltpu.SemaphoreType.DMA((2,) + per_piece),
            pltpu.SemaphoreType.DMA((max(nx - 1, 1),) + per_piece),
            pltpu.SemaphoreType.DMA((max(ny - 1, 1),) + per_piece),
            pltpu.SemaphoreType.DMA(per_piece),
            pltpu.SemaphoreType.DMA((dp, tp, 2)),
        ],
        compiler_params=pltpu.CompilerParams(
            collective_id=collective_id, has_side_effects=True, vmem_limit_bytes=48 * 2**20),
        cost_estimate=pl.CostEstimate(flops=0, bytes_accessed=rows * cols * dp * tp * 8, transcendentals=0),
    )(x)


LANE = 128


def pad_up(n, m):
    return -(-n // m) * m


def dot_t(a, b):
    return lax.dot_general(a, b, (((1,), (1,)), ((), ())), preferred_element_type=jnp.float32)


def widen(tp, cols, wide, raw, padded, lead):
    block = 48
    blocks = raw.shape[-2] // block

    def body(i, carry):
        at = pl.ds(pl.multiple_of(i * block, 16), block)
        v = raw[lead + (at, slice(None))]
        for t in range(tp):
            part = v[:, t * cols:(t + 1) * cols]
            padded[lead + (at, pl.ds(t * wide, wide))] = jnp.concatenate(
                [part, jnp.zeros((block, wide - cols), v.dtype)], axis=1)
        return carry
    lax.fori_loop(0, blocks, body, 0)
    rest = padded.shape[-2] - raw.shape[-2]
    padded[lead + (pl.ds(raw.shape[-2], rest), slice(None))] = jnp.zeros((rest, tp * wide), padded.dtype)


def attend_part(
    tp, kv_heads, group_size, head_size, meet, meanwhile, res_buf,
    tok_ref, gain_ref, inverse_ref, pos_ref, sink_ref, wq_hbm, wkv_hbm, wo_hbm, cache_hbm,
    tok_buf, wq_buf, wkv_raw, wkv_wide, wkv_buf, wo_buf, cache_buf, q_rows, new_rows, pos_rows, att_rows,
    part_buf, got_buf, load_sem, send_sem, recv_tok, recv_part,
):
    dp_id = lax.axis_index("dp")
    me = lax.axis_index("tp")
    core, chip = lax.rem(me, CORES), me // CORES
    seq, cols = tok_ref.shape
    wide = res_buf.shape[1]
    window = cache_hbm.shape[2]
    heads = kv_heads * group_size
    twin_t = chip * CORES + 1 - core
    across_t = (1 - chip) * CORES + core
    corner_t = (1 - chip) * CORES + 1 - core
    twin, across = (dp_id, twin_t), (dp_id, across_t)

    loads = [
        pltpu.make_async_copy(src, dst, load_sem.at[i]) for i, (src, dst) in enumerate(
            [(wkv_hbm, wkv_raw), (wq_hbm, wq_buf), (cache_hbm, cache_buf), (wo_hbm, wo_buf)])
    ]
    for load in loads:
        load.start()
    own = pltpu.make_async_copy(tok_ref, tok_buf.at[me], load_sem.at[4])
    own.start()
    meet()

    def token_copy(src, t, i, target):
        return pltpu.make_async_remote_copy(
            src_ref=src, dst_ref=tok_buf.at[t], send_sem=send_sem.at[i], recv_sem=recv_tok.at[t],
            device_id=target, device_id_type=MESH)

    def token_arrived(t):
        token_copy(tok_buf.at[t], t, 0, twin).wait_recv()

    sent = [token_copy(tok_ref, me, 0, across), token_copy(tok_ref, me, 1, twin)]
    for copy in sent:
        copy.start()

    lanes = lax.broadcasted_iota(jnp.int32, (seq, LANE), 1)

    def column(row):
        n = row.shape[1]
        square = lax.broadcasted_iota(jnp.int32, (n, n), 0) == lax.broadcasted_iota(jnp.int32, (n, n), 1)
        return jnp.sum(jnp.where(square, row, 0.0), axis=1, keepdims=True)

    position = jnp.broadcast_to(column(pos_ref[...].astype(jnp.float32)), (seq, LANE))
    angles = position * inverse_ref[...]
    cosine = jnp.cos(angles)
    front = lax.rem(lanes, head_size) < head_size // 2
    sine = jnp.where(front, -jnp.sin(angles), jnp.sin(angles))
    for h in range(heads):
        pos_rows[pl.ds(h, seq, stride=heads), :] = position
    sink = jnp.broadcast_to(column(sink_ref[...]), (heads, LANE))
    sink = jnp.concatenate([sink] * 8, axis=0)

    loads[0].wait()
    kv_rows = wkv_raw.shape[0]
    step = kv_rows // 30

    def split(i, carry):
        at = pl.multiple_of(i * step, 16)
        wkv_wide[...] = wkv_raw[pl.ds(at, step), :].astype(jnp.float32)
        half = pl.ds(pl.multiple_of(i * (step // kv_heads), 16), step // kv_heads)
        for h in range(kv_heads):
            wkv_buf[half, h * LANE:(h + 1) * LANE] = wkv_wide[
                pl.ds(h, step // kv_heads, stride=kv_heads), :].astype(jnp.bfloat16)
        return carry
    lax.fori_loop(0, 30, split, 0)

    token_arrived(across_t)
    forward = token_copy(tok_buf.at[across_t], across_t, 2, twin)
    forward.start()
    sent.append(forward)
    own.wait()
    token_arrived(twin_t)
    token_arrived(corner_t)
    loads[1].wait()

    pieces = [tok_buf[t].astype(jnp.float32) for t in range(tp)]
    squares = jnp.sum(pieces[0] * pieces[0], axis=1, keepdims=True)
    for v in pieces[1:]:
        squares = squares + jnp.sum(v * v, axis=1, keepdims=True)
    scale = lax.rsqrt(squares / (tp * cols) + norm_eps)
    gains = gain_ref[...].reshape(1, tp * cols)
    queries, fresh = 0.0, 0.0
    for t in range(tp):
        at = slice(t * cols, (t + 1) * cols)
        normed = (pieces[t] * scale * gains[:, at]).astype(jnp.bfloat16)
        queries = queries + jnp.dot(normed, wq_buf[at, :], preferred_element_type=jnp.float32)
        fresh = fresh + jnp.dot(normed, wkv_buf[at, :], preferred_element_type=jnp.float32)

    def turned(v):
        swapped = jnp.where(
            front, pltpu.roll(v, LANE - head_size // 2, 1), pltpu.roll(v, head_size // 2, 1))
        return v * cosine + swapped * sine

    def rounded(v):
        return v.astype(jnp.bfloat16).astype(jnp.float32)

    low = lanes < head_size
    for h in range(heads):
        if h % 2 == 0:
            pair = rounded(turned(queries[:, h // 2 * LANE:(h // 2 + 1) * LANE]))
        if h % group_size == 0:
            k = h // group_size
            entry = fresh[:, k * LANE:(k + 1) * LANE]
            entry = rounded(jnp.where(low, turned(entry), entry))
        own_q = pair if h % 2 == 0 else pltpu.roll(pair, head_size, 1)
        q_rows[pl.ds(h, seq, stride=heads), :] = jnp.where(low, own_q, 0.0)
        new_rows[pl.ds(h, seq, stride=heads), :] = entry

    loads[2].wait()
    batch = 8
    rows = batch * heads
    slot = lax.broadcasted_iota(jnp.int32, (rows, LANE), 1)
    upper = lax.broadcasted_iota(jnp.int32, (heads, LANE), 0) < group_size
    score_scale = head_size ** (-0.5)

    def attend(i, carry):
        at = pl.ds(pl.multiple_of(i * rows, rows), rows)
        q = q_rows[at, :]
        entry = new_rows[at, :]
        pos = pos_rows[at, :].astype(jnp.int32)
        raw = []
        for s in range(batch):
            qs = q[s * heads:(s + 1) * heads]
            lhs = jnp.concatenate(
                [jnp.where(upper, qs, 0.0), jnp.where(upper, 0.0, qs)], axis=1).astype(jnp.bfloat16)
            rhs = jnp.concatenate([cache_buf[i * batch + s, k] for k in range(kv_heads)], axis=1)
            raw.append(dot_t(lhs, rhs))
        scores = jnp.concatenate(raw, axis=0) * score_scale
        fresh_score = jnp.sum(q * entry, axis=1, keepdims=True) * score_scale
        current = slot == lax.rem(pos, window)
        scores = jnp.where(current, fresh_score, jnp.where(slot <= pos, scores, -jnp.inf))
        peak = jnp.maximum(jnp.max(scores, axis=1, keepdims=True), sink)
        raised = jnp.exp(scores - peak)
        denominator = jnp.sum(raised, axis=1, keepdims=True) + jnp.exp(sink - peak)
        probs = rounded(raised / denominator)
        fresh_prob = jnp.sum(jnp.where(current, probs, 0.0), axis=1, keepdims=True)
        probs = jnp.where(current, 0.0, probs)
        mixed = []
        for s in range(batch):
            lhs = probs[s * heads:(s + 1) * heads].astype(jnp.bfloat16)
            rhs = jnp.concatenate([cache_buf[i * batch + s, k] for k in range(kv_heads)], axis=1)
            both = jnp.dot(lhs, rhs, preferred_element_type=jnp.float32)
            mixed.append(jnp.where(upper, both[:, :LANE], both[:, LANE:]))
        att_rows[at, :] = jnp.concatenate(mixed, axis=0) + fresh_prob * entry
        return carry

    lax.fori_loop(0, seq // batch, attend, 0)

    tiles = []
    for j in range(heads // 2):
        even = att_rows[pl.ds(2 * j, seq, stride=heads), :]
        odd = att_rows[pl.ds(2 * j + 1, seq, stride=heads), :]
        tiles.append(jnp.where(low, pltpu.roll(even, head_size, 1), odd).astype(jnp.bfloat16))
    attended = jnp.concatenate(tiles, axis=1)
    loads[3].wait()

    def share(t):
        return dot_t(attended, wo_buf[pl.ds(pl.multiple_of(t * cols, 16), cols), :])

    def part_copy(i, target):
        return pltpu.make_async_remote_copy(
            src_ref=part_buf.at[i], dst_ref=got_buf.at[i], send_sem=send_sem.at[3 + i],
            recv_sem=recv_part.at[i], device_id=target, device_id_type=MESH)

    parts = [part_copy(0, twin), part_copy(1, across), part_copy(2, twin)]
    part_buf[0] = share(corner_t).astype(jnp.bfloat16)
    parts[0].start()
    far = share(across_t)
    parts[0].wait_recv()
    part_buf[1] = (far + got_buf[0].astype(jnp.float32)).astype(jnp.bfloat16)
    parts[1].start()
    part_buf[2] = share(twin_t).astype(jnp.bfloat16)
    parts[2].start()
    total = tok_ref[...].astype(jnp.float32) + share(me)
    meanwhile()
    parts[2].wait_recv()
    total = total + got_buf[2].astype(jnp.float32)
    parts[1].wait_recv()
    total = total + got_buf[1].astype(jnp.float32)
    res_buf[...] = jnp.concatenate([total, jnp.zeros((seq, wide - cols), jnp.float32)], axis=1)
    for copy in sent + parts:
        copy.wait_send()


def moe_part(
    dp, ny, tp, experts, cuts, full,
    res_ref, gain_ref, router_ref, ids_ref, wd_load, out_ref,
    rows_buf, gu_pad, wd_raw, wd_pad, act_buf, out_buf, back_buf,
    s_twin, s_x, s_y, s_z, r_rows, s_act, r_act, s_out, r_out,
):
    nz = dp // ny
    dp_id = lax.axis_index("dp")
    me = lax.axis_index("tp")
    core, chip = lax.rem(me, CORES), me // CORES
    z, y = dp_id // ny, lax.rem(dp_id, ny)
    seq, wide = res_ref.shape
    cols = out_ref.shape[1]
    twin_t = chip * CORES + 1 - core
    across_t = (1 - chip) * CORES + core
    corner_t = (1 - chip) * CORES + 1 - core
    twin, across = (dp_id, twin_t), (dp_id, across_t)
    y_peer = (z * ny + 1 - y, me)

    res = res_ref[...]
    gains = gain_ref[...].reshape(1, full)
    gain = gains[:, :cols]
    for t in range(1, tp):
        gain = jnp.where(me == t, gains[:, t * cols:(t + 1) * cols], gain)
    gained = res * jnp.concatenate([gain, jnp.zeros((1, wide - cols), jnp.float32)], axis=1)
    values = [jnp.sum(res * res, axis=1, keepdims=True)]
    router = jnp.concatenate(
        [router_ref[...].astype(jnp.float32), jnp.zeros((experts, wide - cols), jnp.float32)], axis=1)
    for e in range(experts):
        values.append(jnp.sum(gained * router[e:e + 1, :], axis=1, keepdims=True))
    tail = cols - (wide - LANE)
    lanes = lax.broadcasted_iota(jnp.int32, (seq, LANE), 1)
    group = (LANE - tail) // 3
    spread = jnp.zeros((seq, LANE), jnp.float32)
    for j, v in enumerate(values):
        for g in range(3):
            spread = jnp.where(lanes == tail + g * group + j, v, spread)
    high = spread.astype(jnp.bfloat16).astype(jnp.float32)
    middle = (spread - high).astype(jnp.bfloat16).astype(jnp.float32)
    low = spread - high - middle
    last = jnp.where(lanes < tail, gained[:, wide - LANE:], jnp.where(
        lanes < tail + group, high, jnp.where(lanes < tail + 2 * group, middle, low)))
    rows_buf[dp_id, me, :, :wide - LANE] = gained[:, :wide - LANE].astype(jnp.bfloat16)
    rows_buf[dp_id, me, :, wide - LANE:] = last.astype(jnp.bfloat16)

    share = seq // cuts

    def piece(b, t, h, sem, target):
        view = rows_buf.at[b, t, pl.ds(h * share, share)]
        return pltpu.make_async_remote_copy(
            src_ref=view, dst_ref=view, send_sem=sem, recv_sem=r_rows.at[b, t, h],
            device_id=target, device_id_type=MESH)

    def to_twin(b, t, h):
        return piece(b, t, h, s_twin.at[b, t, h], twin)

    def to_x(p, h):
        return piece(p * ny + y, me, h, s_x.at[p, h], across)

    def to_y(b, t, h):
        return piece(b, t, h, s_y.at[b, t // CORES, h], y_peer)

    def to_z(p, h):
        return piece(dp_id, me, h, s_z.at[p, h], (p * ny + y, me))

    def arrived(b, t, h):
        piece(b, t, h, r_rows.at[b, t, h], twin).wait_recv()

    def plane(k):
        return jnp.where(2 * z < nz, lax.rem(z + k, nz), lax.rem(z - k + nz, nz))

    for h in range(cuts):
        to_x(z, h).start()
        to_y(dp_id, me, h).start()
        to_twin(dp_id, me, h).start()

    def send_far(k, carry):
        for h in range(cuts):
            to_z(plane(k), h).start()
        return carry
    lax.fori_loop(1, nz, send_far, 0)

    def column_in(k, y_too):
        p = plane(k)
        for h in range(cuts):
            arrived(p * ny + y, me, h)
            to_x(p, h).start()
            if y_too:
                to_y(p * ny + y, me, h).start()
            to_twin(p * ny + y, me, h).start()

    def column_to_y(k):
        for h in range(cuts):
            to_y(plane(k) * ny + y, me, h).start()

    def across_in(k):
        b = plane(k) * ny + y
        for h in range(cuts):
            arrived(b, across_t, h)
            to_y(b, across_t, h).start()
            to_twin(b, across_t, h).start()

    column_in(1, True)
    for k in range(2, nz):
        column_in(k, False)
        across_in(k - 1)
        if k == 2:
            across_in(0)
        column_to_y(k)
        if k == 2:
            wd_load.wait()
            widen(tp, cols, wide, wd_raw, wd_pad, ())

    tile_n = 256
    n_tiles = wide // tile_n

    def act_copy(t, p, n, i, target):
        view = act_buf.at[t, p, n]
        return pltpu.make_async_remote_copy(
            src_ref=view, dst_ref=view, send_sem=s_act.at[i, p, n], recv_sem=r_act.at[t, p, n],
            device_id=target, device_id_type=MESH)

    def act_arrived(t, p, n):
        act_copy(t, p, n, 0, twin).wait_recv()

    def out_copy(b, n):
        return pltpu.make_async_remote_copy(
            src_ref=out_buf.at[b, n], dst_ref=back_buf.at[dp_id, n], send_sem=s_out.at[b, n],
            recv_sem=r_out.at[dp_id, n], device_id=(b, me), device_id_type=MESH)

    def stats_tile(b):
        total = rows_buf[b, 0, :, wide - LANE:].astype(jnp.float32)
        for t in range(1, tp):
            total = total + rows_buf[b, t, :, wide - LANE:].astype(jnp.float32)
        total = jnp.where(lanes >= tail, total, 0.0)
        return total

    def row_scale(total):
        hit = (lanes == tail) | (lanes == tail + group) | (lanes == tail + 2 * group)
        squares = jnp.sum(jnp.where(hit, total, 0.0), axis=1, keepdims=True)
        return lax.rsqrt(squares / full + norm_eps)

    def up_project(p):
        scale = jnp.concatenate([row_scale(stats_tile(p * ny + b)) for b in range(ny)], axis=0)

        def body(n, carry):
            at = pl.ds(pl.multiple_of(n * tile_n, tile_n), tile_n)
            lhs = jnp.concatenate([
                jnp.concatenate([rows_buf[p * ny + b, t] for t in range(tp)], axis=1)
                for b in range(ny)], axis=0)
            gate = dot_t(lhs, gu_pad[0, at, :]) * scale
            up = dot_t(lhs, gu_pad[1, at, :]) * scale
            act_buf[me, p, n] = (gate * jax.nn.sigmoid(glu_alpha * gate) * (up + 1.0)).astype(jnp.bfloat16)
            act_copy(me, p, n, 0, across).start()
            act_copy(me, p, n, 1, twin).start()
            return carry
        lax.fori_loop(0, n_tiles, body, 0)

    def down_project(p):
        def body(n, carry):
            at = pl.ds(pl.multiple_of(n * tile_n, tile_n), tile_n)
            lhs = jnp.concatenate([act_buf[t, p, i] for t in range(tp) for i in range(n_tiles)], axis=1)
            out = dot_t(lhs, wd_pad[at, :]).astype(jnp.bfloat16)
            for b in range(ny):
                out_buf[p * ny + b, n] = out[b * seq:(b + 1) * seq]
            for b in range(ny):
                @pl.when(p * ny + b != dp_id)
                def _():
                    out_copy(p * ny + b, n).start()

                @pl.when(p * ny + b == dp_id)
                def _():
                    back_buf[dp_id, n] = out[b * seq:(b + 1) * seq]
            return carry
        lax.fori_loop(0, n_tiles, body, 0)

    def stage(k, carry):
        @pl.when(k < nz)
        def _():
            p = plane(k + 1)
            for t in (me, across_t):
                b = p * ny + 1 - y
                for h in range(cuts):
                    arrived(b, t, h)
                    to_twin(b, t, h).start()
            for b in range(ny):
                for t in (twin_t, corner_t):
                    for h in range(cuts):
                        arrived(p * ny + b, t, h)
            up_project(p)

        @pl.when(k == 0)
        def _():
            across_in(nz - 1)

        @pl.when(k > 0)
        def _():
            p = plane(k)
            for n in range(n_tiles):
                act_arrived(across_t, p, n)
                act_copy(across_t, p, n, 2, twin).start()
            for n in range(n_tiles):
                act_arrived(twin_t, p, n)
                act_arrived(corner_t, p, n)
            down_project(p)
        return carry

    lax.fori_loop(0, nz + 1, stage, 0)

    total = stats_tile(dp_id)
    scale = row_scale(total)
    shift = LANE - group
    summed = total + pltpu.roll(total, shift, 1) + pltpu.roll(pltpu.roll(total, shift, 1), shift, 1)
    square = lax.broadcasted_iota(jnp.int32, (seq, seq), 0) == lax.broadcasted_iota(jnp.int32, (seq, seq), 1)
    chosen = lanes < 0
    for k in range(ids_ref.shape[0]):
        named = ids_ref[k:k + 1, :].astype(jnp.float32)
        named = jnp.sum(jnp.where(square, named, 0.0), axis=1, keepdims=True).astype(jnp.int32)
        chosen = chosen | (lanes == named + tail + 1)
    raised = jnp.where(chosen, jnp.exp(jnp.where(chosen, summed * scale, 0.0)), 0.0)
    weights = raised / jnp.sum(raised, axis=1, keepdims=True)

    def wait_out(d, carry):
        b = lax.rem(dp_id + d, dp)
        for n in range(n_tiles):
            view = back_buf.at[b, n]
            pltpu.make_async_remote_copy(
                src_ref=view, dst_ref=view, send_sem=r_out.at[b, n], recv_sem=r_out.at[b, n],
                device_id=twin, device_id_type=MESH).wait_recv()
        return carry

    lax.fori_loop(1, dp, wait_out, 0)
    parts = []
    for n in range(n_tiles):
        part = res[:, n * tile_n:(n + 1) * tile_n]
        for e in range(dp):
            part = part + weights[:, tail + 1 + e:tail + 2 + e] * back_buf[e, n].astype(jnp.float32)
        parts.append(part)
    out_ref[...] = jnp.concatenate(parts, axis=1)[:, :cols]

    def drain(p, carry):
        for h in range(cuts):
            to_x(p, h).wait_send()

            @pl.when(p != z)
            def _():
                to_z(p, h).wait_send()
            for t in (me, across_t):
                to_y(p * ny + y, t, h).wait_send()
                for b in range(ny):
                    to_twin(p * ny + b, t, h).wait_send()
        return carry
    lax.fori_loop(0, nz, drain, 0)
    def drain_acts(p, carry):
        for n in range(n_tiles):
            act_copy(me, p, n, 0, across).wait_send()
            act_copy(me, p, n, 1, twin).wait_send()
            act_copy(across_t, p, n, 2, twin).wait_send()
        return carry
    lax.fori_loop(0, nz, drain_acts, 0)

    def drain_outs(d, carry):
        for n in range(n_tiles):
            out_copy(lax.rem(dp_id + d, dp), n).wait_send()
        return carry
    lax.fori_loop(1, dp, drain_outs, 0)


def layer_kernel(
    dp, ny, tp, experts, cuts, kv_heads, group_size, head_size,
    tok_ref, gain_ref, inverse_ref, pos_ref, sink_ref, moe_gain_ref, router_ref, ids_ref,
    wq_hbm, wkv_hbm, wo_hbm, cache_hbm, gu_hbm, wd_hbm, out_ref, *scratch,
):
    res_buf, gu_raw, wd_raw, load_sem = scratch[:4]
    attend_scratch, (rows_buf, gu_pad, wd_pad, *rest) = scratch[4:21], scratch[21:]
    dp_id, me = lax.axis_index("dp"), lax.axis_index("tp")
    core, chip = lax.rem(me, CORES), me // CORES
    cols, full = gu_hbm.shape[1:]
    wide = res_buf.shape[1]
    gu_load = pltpu.make_async_copy(gu_hbm, gu_raw, load_sem.at[0])
    wd_load = pltpu.make_async_copy(wd_hbm, wd_raw, load_sem.at[1])

    def meet():
        gu_load.start()
        wd_load.start()
        near = [(dp_id, chip * CORES + 1 - core), (dp_id, (1 - chip) * CORES + core)]
        greet(near + [(lax.rem(dp_id + d, dp), me) for d in range(1, dp)])

    def meanwhile():
        gu_load.wait()
        for half in range(2):
            widen(tp, cols, wide, gu_raw, gu_pad, (half,))

    attend_part(
        tp, kv_heads, group_size, head_size, meet, meanwhile, res_buf,
        tok_ref, gain_ref, inverse_ref, pos_ref, sink_ref, wq_hbm, wkv_hbm, wo_hbm, cache_hbm, *attend_scratch)
    moe_part(
        dp, ny, tp, experts, cuts, full, res_buf, moe_gain_ref, router_ref, ids_ref, wd_load, out_ref,
        rows_buf, gu_pad, wd_raw, wd_pad, *rest)


def layer(tokens, gain, positions, sinks, moe_gain, router, ids, w_query, w_keyvalue, w_out, cache, gate_up, w_down, dp, ny, tp):
    seq, cols = tokens.shape
    wide = pad_up(cols, 256)
    full = tp * cols
    kv_heads, window, entry = cache.shape[1:]
    head_size = entry // 2
    heads = w_query.shape[1] // head_size
    exponent = np.arange(LANE) % (head_size // 2) * (2.0 / head_size)
    inverse = jnp.asarray(rope_base ** -exponent, jnp.float32)[None, :]
    nz, cuts, tiles = dp // ny, 2, wide // 256
    bf, f32 = jnp.bfloat16, jnp.float32
    dma, vmem = pltpu.SemaphoreType.DMA, pltpu.VMEM
    return pl.pallas_call(
        functools.partial(
            layer_kernel, dp, ny, tp, router.shape[0], cuts, kv_heads, heads // kv_heads, head_size),
        out_shape=jax.ShapeDtypeStruct((seq, cols), f32),
        in_specs=[pl.BlockSpec(memory_space=pltpu.VMEM)] * 8 + [pl.BlockSpec(memory_space=pl.ANY)] * 6,
        out_specs=pl.BlockSpec(memory_space=pltpu.VMEM),
        scratch_shapes=[
            vmem((seq, wide), f32), vmem((2, cols, full), bf), vmem((cols, full), bf), dma((2,)),
            vmem((tp, seq, cols), bf), vmem(w_query.shape, bf), vmem((full * kv_heads, LANE), bf),
            vmem((full * kv_heads // 30, LANE), f32), vmem((full, kv_heads * LANE), bf),
            vmem((full, heads * head_size), bf), vmem(cache.shape, bf),
            vmem((seq * heads, LANE), f32), vmem((seq * heads, LANE), f32),
            vmem((seq * heads, LANE), f32), vmem((seq * heads, LANE), f32),
            vmem((3, seq, cols), bf), vmem((3, seq, cols), bf),
            dma((5,)), dma((6,)), dma((tp,)), dma((3,)),
            vmem((dp, tp, seq, wide), bf), vmem((2, wide, tp * wide), bf), vmem((wide, tp * wide), bf),
            vmem((tp, nz, tiles, ny * seq, 256), bf),
            vmem((dp, tiles, seq, 256), bf), vmem((dp, tiles, seq, 256), bf),
            dma((dp, tp, cuts)), dma((nz, cuts)), dma((dp, tp // CORES, cuts)),
            dma((nz, cuts)), dma((dp, tp, cuts)),
            dma((3, nz, tiles)), dma((tp, nz, tiles)), dma((dp, tiles)), dma((dp, tiles)),
        ],
        compiler_params=pltpu.CompilerParams(
            collective_id=0, has_side_effects=True, vmem_limit_bytes=67_000_000),
        cost_estimate=pl.CostEstimate(
            flops=6 * dp * seq * full * cols, bytes_accessed=6 * full * cols, transcendentals=0),
    )(tokens, gain, inverse, positions[None, :], sinks[None, :], moe_gain, router, ids,
      w_query, w_keyvalue.reshape(full * kv_heads, LANE), w_out.T, cache, gate_up, w_down)


def activate(mixed_in, ff_local):
    gate_part = mixed_in[..., :ff_local]
    up_part = mixed_in[..., ff_local:]
    return (gate_part * jax.nn.sigmoid(glu_alpha * gate_part) * (up_part + 1.0)).astype(
        jnp.bfloat16
    )


def on_device(
    tokens,
    attn_gain,
    w_query,
    w_keyvalue,
    attn_sinks,
    w_out,
    window_cache,
    positions,
    moe_gain,
    router,
    gate_up,
    w_down,
    expert_ids,
):
    tp_count = lax.axis_size("tp")
    dp_count = lax.axis_size("dp")
    seq_count, col_count = tokens.shape
    full_width = col_count * tp_count
    col_start = lax.axis_index("tp") * col_count
    head_size = w_keyvalue.shape[2] // 2
    kv_local = w_keyvalue.shape[1]
    q_local = w_query.shape[1] // head_size
    group_size = q_local // kv_local
    window = window_cache.shape[2]
    ny = 2 ** (int(math.log2(dp_count)) // 2)
    if (tp_count, ny, gate_up.shape[0], kv_local, group_size, window, 2 * head_size) == (
            2 * CORES, 2, 1, 2, 4, LANE, LANE) and dp_count > 2 * ny:
        return layer(
            tokens, attn_gain, positions, attn_sinks, moe_gain, router.T, expert_ids.T, w_query, w_keyvalue,
            w_out, window_cache, jnp.transpose(gate_up[0], (1, 2, 0)), w_down[0].T, dp_count, ny, tp_count)
    moe_slice = lax.dynamic_slice_in_dim(moe_gain, col_start, col_count)
    tok_wide = tokens.astype(jnp.float32)
    kv_flat = w_keyvalue.reshape(full_width, kv_local * 2 * head_size)
    whole_rows = feature_gather(tokens, tp_count, 2, 0).astype(jnp.float32)
    attn_sq = jnp.sum(whole_rows * whole_rows, axis=1, keepdims=True)
    piece_rows = (
        whole_rows * lax.rsqrt(attn_sq / full_width + norm_eps) * attn_gain[None, :]
    ).astype(jnp.bfloat16)
    queries = jnp.dot(piece_rows, w_query, preferred_element_type=jnp.float32)
    fresh_rows = jnp.dot(piece_rows, kv_flat, preferred_element_type=jnp.float32)
    cosine, sine_table = rope_tables(positions, head_size)
    rot_queries = rotate(
        queries.reshape(seq_count, q_local, head_size), cosine[:, None, :], sine_table[:, None, :]
    ).astype(jnp.bfloat16)
    fresh_rows = fresh_rows.reshape(seq_count, kv_local, 2 * head_size)
    new_key = rotate(fresh_rows[..., :head_size], cosine[:, None, :], sine_table[:, None, :])
    new_entry = jnp.concatenate([new_key, fresh_rows[..., head_size:]], axis=-1).astype(
        jnp.bfloat16
    )
    slot_ids = jnp.arange(window, dtype=jnp.int32)
    is_current = slot_ids[None, :] == (positions % window)[:, None]
    is_valid = (positions[:, None] - slot_ids[None, :]) % window <= positions[:, None]
    is_valid = is_valid & ~is_current
    grouped = rot_queries.reshape(seq_count, kv_local, group_size, head_size)
    scores = jnp.einsum(
        "skgh,skwh->skgw", grouped, window_cache[..., :head_size], preferred_element_type=jnp.float32
    ) * head_size ** (-0.5)
    scores = jnp.where(is_valid[:, None, None, :], scores, -jnp.inf)
    new_wide = new_entry.astype(jnp.float32)[:, :, None, :]
    new_score = jnp.sum(
        grouped.astype(jnp.float32) * new_wide[..., :head_size], axis=-1, keepdims=True
    ) * head_size ** (-0.5)
    sink_col = attn_sinks.reshape(kv_local, group_size)[None, :, :, None]
    peak_score = jnp.maximum(
        jnp.maximum(jnp.max(scores, axis=-1, keepdims=True), new_score), sink_col
    )
    raised = jnp.exp(scores - peak_score)
    raised_new = jnp.exp(new_score - peak_score)
    denominator = (
        jnp.sum(raised, axis=-1, keepdims=True) + raised_new + jnp.exp(sink_col - peak_score)
    )
    prob_bf = (raised / denominator).astype(jnp.bfloat16)
    prob_new = (raised_new / denominator).astype(jnp.bfloat16).astype(jnp.float32)
    attended = jnp.einsum(
        "skgw,skwh->skgh", prob_bf, window_cache[..., head_size:], preferred_element_type=jnp.float32
    )
    attended = (attended + prob_new * new_wide[..., head_size:]).astype(jnp.bfloat16)
    partial_out = jnp.einsum(
        "sh,htc->tsc",
        attended.reshape(seq_count, q_local * head_size),
        w_out.reshape(q_local * head_size, tp_count, col_count),
        preferred_element_type=jnp.float32,
    ).astype(jnp.bfloat16)
    residual = tok_wide + share_sum(partial_out, tp_count, True, 2)
    experts = router.shape[1]
    top_count = expert_ids.shape[1]
    local_experts = gate_up.shape[0]
    ff_local = gate_up.shape[3]
    capacity = min(seq_count, max(2, 8 * seq_count * top_count // (3 * experts)))
    moe_sq = jnp.sum(residual * residual, axis=1)
    router_wide = router.astype(jnp.float32)
    gained = residual * moe_slice[None, :]
    raw_logits = jnp.dot(gained, router_wide, precision=lax.Precision.HIGHEST)
    stats = share_sum(
        jnp.concatenate([moe_sq[:, None], raw_logits], axis=1)[None], tp_count, False, 3
    )
    moe_scale = lax.rsqrt(stats[:, :1] / full_width + norm_eps)
    logits = stats[:, 1:] * moe_scale
    hidden_rows = (gained * moe_scale).astype(jnp.bfloat16)
    expert_iota = jnp.arange(experts, dtype=jnp.int32)
    chosen = expert_ids[:, :, None] == expert_iota[None, None, :]
    picked = jnp.sum(jnp.where(chosen, logits[:, None, :], 0.0), axis=-1)
    raised_logits = jnp.exp(picked)
    route_weights = raised_logits / jnp.sum(raised_logits, axis=1, keepdims=True)
    gate_up_flat = gate_up.reshape(local_experts, full_width, 2 * ff_local)
    if capacity >= seq_count:
        token_weights = jnp.sum(jnp.where(chosen, route_weights[:, :, None], 0.0), axis=1)
        all_rows = full_gather(hidden_rows, dp_count, tp_count, 1)
        half = seq_count // 2
        part = dp_count * half
        acts = [
            activate(
                jnp.dot(all_rows, gate_up_flat[e], preferred_element_type=jnp.float32), ff_local
            )
            for e in range(local_experts)
        ]
        pieces = []
        for h in range(2):
            outs = []
            for e in range(local_experts):
                act_all = feature_gather(
                    acts[e][h * part : (h + 1) * part], tp_count, dp_count // 2, 4 + 2 * e + h
                )
                out = jnp.dot(act_all, w_down[e], preferred_element_type=jnp.float32)
                outs.append(out.astype(jnp.bfloat16).reshape(dp_count, half, col_count))
            returned = lax.all_to_all(
                jnp.stack(outs, axis=1), "dp", split_axis=0, concat_axis=0, tiled=True
            )
            back = returned.reshape(experts, half, col_count)
            mine = slice(h * half, (h + 1) * half)
            total = residual[mine]
            for e in range(experts):
                total = total + token_weights[mine, e : e + 1] * back[e].astype(jnp.float32)
            pieces.append(total)
        total = jnp.concatenate(pieces, axis=0)
        return total
    assign = expert_ids.reshape(-1)
    onehot = (assign[:, None] == expert_iota[None, :]).astype(jnp.int32)
    earlier = jnp.cumsum(onehot, axis=0) - onehot
    slot_of = jnp.sum(earlier * onehot, axis=1)
    target = (assign * capacity + slot_of).reshape(seq_count, top_count)
    spot_ids = jnp.arange(experts * capacity, dtype=jnp.int32)
    slot_hits = target[:, :, None] == spot_ids[None, None, :]
    placer = jnp.transpose(jnp.any(slot_hits, axis=1)).astype(jnp.bfloat16)
    combiner = jnp.sum(jnp.where(slot_hits, route_weights[:, :, None], 0.0), axis=1)
    placed = jnp.dot(placer, hidden_rows, preferred_element_type=jnp.float32).astype(jnp.bfloat16)
    mixed_in = jnp.einsum(
        "gecd,edf->gecf",
        lax.all_gather(
            lax.all_to_all(
                placed.reshape(dp_count, local_experts, capacity, hidden_rows.shape[1]),
                "dp",
                split_axis=0,
                concat_axis=0,
                tiled=True,
            ),
            "tp",
            axis=3,
            tiled=True,
        ),
        gate_up_flat,
        preferred_element_type=jnp.float32,
    )
    act_rows = activate(mixed_in, ff_local)
    answered = jnp.einsum(
        "gecf,efd->gecd",
        lax.all_gather(act_rows, "tp", axis=3, tiled=True),
        w_down,
        preferred_element_type=jnp.float32,
    ).astype(jnp.bfloat16)
    returned = lax.all_to_all(answered, "dp", split_axis=0, concat_axis=0, tiled=True)
    flat_back = returned.reshape(experts * capacity, col_count).astype(jnp.float32)
    moe_out = jnp.dot(combiner, flat_back, precision=lax.Precision.HIGHEST)
    return residual + moe_out


def solution(mesh):
    in_specs = (
        P("dp", "tp"),
        P(),
        P(None, "tp"),
        P(None, "tp", None),
        P("tp"),
        P("tp", None),
        P("dp", "tp", None, None),
        P("dp"),
        P(),
        P("tp", None),
        P("dp", None, None, "tp"),
        P("dp", None, "tp"),
        P("dp", None),
    )
    out_specs = P("dp", "tp")
    return jax.shard_map(
        on_device, mesh=mesh, in_specs=in_specs, out_specs=out_specs, check_vma=False
    )
```

```python
import functools
import math

import jax
import jax.numpy as jnp
import numpy as np
from jax import lax
from jax.experimental import pallas as pl
from jax.experimental.pallas import tpu as pltpu
from jax.sharding import PartitionSpec as P

norm_eps = 1e-05
rope_base = 150000.0
glu_alpha = 1.702


def rope_tables(positions, head_size):
    half_size = head_size // 2
    exponent = jnp.arange(half_size, dtype=jnp.float32) * (2.0 / head_size)
    inverse = jnp.power(jnp.float32(rope_base), -exponent)
    angles = positions.astype(jnp.float32)[:, None] * inverse[None, :]
    return (jnp.cos(angles), jnp.sin(angles))


def rotate(values, cosine, sine_table):
    half_size = values.shape[-1] // 2
    first_half = values[..., :half_size]
    second_half = values[..., half_size:]
    return jnp.concatenate(
        [
            first_half * cosine - second_half * sine_table,
            second_half * cosine + first_half * sine_table,
        ],
        axis=-1,
    )


MESH = pl.DeviceIdType.MESH
CORES = 2


def greet(partners):
    barrier = pltpu.get_barrier_semaphore()
    for partner in partners:
        pl.semaphore_signal(barrier, inc=1, device_id=partner, device_id_type=MESH)
    pl.semaphore_wait(barrier, len(partners))


def feature_gather_kernel(tp, chunks, x_ref, out_ref, buf, own_sem, send_x, send_c, recv):
    chips = tp // CORES
    dp_id = lax.axis_index("dp")
    me = lax.axis_index("tp")
    core = lax.rem(me, CORES)
    chip = me // CORES
    rows, cols = x_ref.shape
    step = rows // chunks
    twin = (dp_id, chip * CORES + (1 - core))
    others = [lax.rem(chip + d, chips) * CORES + core for d in range(1, chips)]
    sources = [lax.rem(chip + chips - d, chips) * CORES + core for d in range(1, chips)]
    own = pltpu.make_async_copy(x_ref, buf.at[me], own_sem)
    own.start()
    greet([twin] + [(dp_id, other) for other in others])

    def piece(k):
        return pl.ds(k * step, step)

    def send(src, origin, k, sem, target):
        return pltpu.make_async_remote_copy(
            src_ref=src, dst_ref=buf.at[origin, piece(k)], send_sem=sem,
            recv_sem=recv.at[origin, k], device_id=target, device_id_type=MESH)

    sent = []
    for k in range(chunks):
        for d in range(chips - 1):
            sent.append(send(x_ref.at[piece(k)], me, k, send_x.at[d, k], (dp_id, others[d])))
            sent[-1].start()
    for k in range(chunks):
        sent.append(send(x_ref.at[piece(k)], me, k, send_c.at[0, k], twin))
        sent[-1].start()
    own.wait()
    for k in range(chunks):
        for d in range(chips - 1):
            origin = sources[d]
            forward = send(buf.at[origin, piece(k)], origin, k, send_c.at[d + 1, k], twin)
            forward.wait_recv()
            forward.start()
            sent.append(forward)
        if k:
            finish(tp, k - 1, step, chip, core, chips, buf, recv, out_ref, send, twin)
    finish(tp, chunks - 1, step, chip, core, chips, buf, recv, out_ref, send, twin)
    for copy in sent:
        copy.wait_send()


def finish(tp, k, step, chip, core, chips, buf, recv, out_ref, send, twin):
    cols = buf.shape[2]
    part = pl.ds(k * step, step)
    for d in range(chips):
        origin = lax.rem(chip + d, chips) * CORES + (1 - core)
        pltpu.make_async_remote_copy(
            src_ref=buf.at[origin, part], dst_ref=buf.at[origin, part], send_sem=recv.at[origin, k],
            recv_sem=recv.at[origin, k], device_id=twin, device_id_type=MESH).wait_recv()
    for t in range(tp):
        out_ref[part, t * cols:(t + 1) * cols] = buf[t, part, :]


def feature_gather(x, tp, chunks, collective_id):
    rows, cols = x.shape
    chips = tp // CORES
    return pl.pallas_call(
        functools.partial(feature_gather_kernel, tp, chunks),
        out_shape=jax.ShapeDtypeStruct((rows, tp * cols), x.dtype),
        in_specs=[pl.BlockSpec(memory_space=pltpu.VMEM)],
        out_specs=pl.BlockSpec(memory_space=pltpu.VMEM),
        scratch_shapes=[
            pltpu.VMEM((tp, rows, cols), x.dtype),
            pltpu.SemaphoreType.DMA,
            pltpu.SemaphoreType.DMA((max(chips - 1, 1), chunks)),
            pltpu.SemaphoreType.DMA((chips, chunks)),
            pltpu.SemaphoreType.DMA((tp, chunks)),
        ],
        compiler_params=pltpu.CompilerParams(
            collective_id=collective_id, has_side_effects=True, vmem_limit_bytes=48 * 2**20),
        cost_estimate=pl.CostEstimate(flops=0, bytes_accessed=rows * cols * tp * 16, transcendentals=0),
    )(x)


def share_sum_kernel(tp, scatter, x_ref, out_ref, buf, send_sem, recv_sem):
    chips = tp // CORES
    dp_id = lax.axis_index("dp")
    me = lax.axis_index("tp")
    core = lax.rem(me, CORES)
    chip = me // CORES
    others = [
        lax.rem(chip + d, chips) * CORES + c for d in range(1, chips) for c in range(CORES)
    ] + [chip * CORES + (1 - core)]
    greet([(dp_id, other) for other in others])
    sent = []
    for i, other in enumerate(others):
        sent.append(pltpu.make_async_remote_copy(
            src_ref=x_ref.at[other if scatter else 0], dst_ref=buf.at[me], send_sem=send_sem.at[i],
            recv_sem=recv_sem.at[me], device_id=(dp_id, other), device_id_type=MESH))
        sent[-1].start()
    total = x_ref[me if scatter else 0].astype(jnp.float32)
    for i in reversed(range(len(others))):
        other = others[i]
        pltpu.make_async_remote_copy(
            src_ref=buf.at[other], dst_ref=buf.at[other], send_sem=send_sem.at[i],
            recv_sem=recv_sem.at[other], device_id=(dp_id, other), device_id_type=MESH).wait_recv()
        total = total + buf[other].astype(jnp.float32)
    out_ref[...] = total
    for copy in sent:
        copy.wait_send()


def share_sum(x, tp, scatter, collective_id):
    rows, cols = x.shape[1:]
    return pl.pallas_call(
        functools.partial(share_sum_kernel, tp, scatter),
        out_shape=jax.ShapeDtypeStruct((rows, cols), jnp.float32),
        in_specs=[pl.BlockSpec(memory_space=pltpu.VMEM)],
        out_specs=pl.BlockSpec(memory_space=pltpu.VMEM),
        scratch_shapes=[
            pltpu.VMEM((tp, rows, cols), x.dtype),
            pltpu.SemaphoreType.DMA((tp - 1,)),
            pltpu.SemaphoreType.DMA((tp,)),
        ],
        compiler_params=pltpu.CompilerParams(
            collective_id=collective_id, has_side_effects=True, vmem_limit_bytes=16 * 2**20),
        cost_estimate=pl.CostEstimate(flops=0, bytes_accessed=rows * cols * tp * 16, transcendentals=0),
    )(x)


def full_gather_kernel(dp, ny, tp, x_ref, out_ref, buf, own_sem, send_z, send_x, send_y, send_c, recv):
    nz, nx = dp // ny, tp // CORES
    dp_id = lax.axis_index("dp")
    me = lax.axis_index("tp")
    core, x = lax.rem(me, CORES), me // CORES
    z, y = dp_id // ny, lax.rem(dp_id, ny)
    rows, cols = x_ref.shape
    half = rows // 2

    def place(pz, py, px, pc=core):
        return (pz * ny + py, px * CORES + pc)

    def around(v, d, n):
        return lax.rem(v + d, n)

    own = pltpu.make_async_copy(x_ref, buf.at[dp_id, me], own_sem)
    own.start()
    twin = place(z, y, x, 1 - core)
    x_others = [place(z, y, around(x, d, nx)) for d in range(1, nx)]
    y_others = [place(z, around(y, d, ny), x) for d in range(1, ny)]
    ring = [place(lax.rem(z + d, nz), y, x) for d in sorted({1 % nz, nz - 1} - {0})]
    greet([twin] + x_others + y_others + ring)
    own.wait()

    def copy(origin, h, sem, target):
        view = buf.at[origin[0], origin[1], pl.ds(h * half, half)]
        return pltpu.make_async_remote_copy(
            src_ref=view, dst_ref=view, send_sem=sem.at[origin[0], origin[1] // CORES, h],
            recv_sem=recv.at[origin[0], origin[1], h], device_id=target, device_id_type=MESH)

    def arrived(origin, h):
        view = buf.at[origin[0], origin[1], pl.ds(h * half, half)]
        pltpu.make_async_remote_copy(
            src_ref=view, dst_ref=view, send_sem=recv.at[origin[0], origin[1], h],
            recv_sem=recv.at[origin[0], origin[1], h], device_id=twin, device_id_type=MESH).wait_recv()

    def to_x(origin, h, act):
        for d in range(nx - 1):
            act(copy(origin, h, send_x.at[d], x_others[d]))

    def to_y(origin, h, act):
        for d in range(ny - 1):
            act(copy(origin, h, send_y.at[d], y_others[d]))

    def to_twin(origin, h, act):
        act(copy(origin, h, send_c, twin))

    def start(c):
        c.start()

    def ended(c):
        c.wait_send()

    def spread(origin, act):
        to_x(origin, 0, act)
        to_y(origin, 1, act)
        to_y(origin, 0, act)
        to_x(origin, 1, act)
        for h in range(2):
            to_twin(origin, h, act)

    def sideways(pz, act, wait):
        for d in range(1, nx):
            origin = place(pz, y, around(x, d, nx))
            if wait:
                arrived(origin, 0)
            to_y(origin, 0, act)
            to_twin(origin, 0, act)
        for d in range(1, ny):
            origin = place(pz, around(y, d, ny), x)
            if wait:
                arrived(origin, 1)
            to_x(origin, 1, act)
            to_twin(origin, 1, act)

    def last(pz, act, wait):
        for d in range(1, ny):
            for e in range(nx):
                origin = place(pz, around(y, d, ny), around(x, e, nx))
                if wait:
                    arrived(origin, 0)
                to_twin(origin, 0, act)
        for d in range(1, nx):
            for e in range(ny):
                origin = place(pz, around(y, e, ny), around(x, d, nx))
                if wait:
                    arrived(origin, 1)
                to_twin(origin, 1, act)

    def above(pz, act):
        @pl.when(z > 0)
        def _():
            for h in range(2):
                act(copy(place(pz, y, x), h, send_z.at[0], place(z - 1, y, x)))

    def below(pz, act):
        @pl.when(z < nz - 1)
        def _():
            for h in range(2):
                act(copy(place(pz, y, x), h, send_z.at[1], place(z + 1, y, x)))

    mine = place(z, y, x)
    above(z, start)
    below(z, start)
    spread(mine, start)

    def first_wave(pz, onward):
        origin = place(pz, y, x)
        arrived(origin, 0)
        arrived(origin, 1)
        onward(pz, start)
        spread(origin, start)

    sideways(z, start, True)
    for s in range(1, nz):
        for pz, ok, onward in ((z - s, z - s >= 0, below), (z + s, z + s < nz, above)):
            pl.when(ok)(functools.partial(first_wave, pz, onward))
        for pz, ok in ((z - s, z - s >= 0), (z + s, z + s < nz)):
            pl.when(ok)(functools.partial(sideways, pz, start, True))
        if s == 1:
            last(z, start, True)
        else:
            for pz, ok in ((z - s + 1, z - s + 1 >= 0), (z + s - 1, z + s - 1 < nz)):
                pl.when(ok)(functools.partial(last, pz, start, True))
    for pz, ok in ((z - nz + 1, z - nz + 1 >= 0), (z + nz - 1, z + nz - 1 < nz)):
        pl.when(ok)(functools.partial(last, pz, start, True))

    for b in range(dp):
        for px in range(nx):
            for h in range(2):
                arrived((b, px * CORES + 1 - core), h)
        for h in range(2):
            start_row = (h * dp + b) * half
            for t in range(tp):
                out_ref[start_row:start_row + half, t * cols:(t + 1) * cols] = buf[
                    b, t, h * half:(h + 1) * half
                ]

    def ends(pz, onward=None):
        if onward is not None:
            onward(pz, ended)
        spread(place(pz, y, x), ended)
        sideways(pz, ended, False)
        last(pz, ended, False)

    above(z, ended)
    below(z, ended)
    ends(z)
    for s in range(1, nz):
        for pz, ok, onward in ((z - s, z - s >= 0, below), (z + s, z + s < nz, above)):
            pl.when(ok)(functools.partial(ends, pz, onward))


def full_gather(x, dp, tp, collective_id):
    rows, cols = x.shape
    nx = tp // CORES
    ny = 2 ** (int(math.log2(dp)) // 2)
    per_piece = (dp, nx, 2)
    return pl.pallas_call(
        functools.partial(full_gather_kernel, dp, ny, tp),
        out_shape=jax.ShapeDtypeStruct((dp * rows, tp * cols), x.dtype),
        in_specs=[pl.BlockSpec(memory_space=pltpu.VMEM)],
        out_specs=pl.BlockSpec(memory_space=pltpu.VMEM),
        scratch_shapes=[
            pltpu.VMEM((dp, tp, rows, cols), x.dtype),
            pltpu.SemaphoreType.DMA,
            pltpu.SemaphoreType.DMA((2,) + per_piece),
            pltpu.SemaphoreType.DMA((max(nx - 1, 1),) + per_piece),
            pltpu.SemaphoreType.DMA((max(ny - 1, 1),) + per_piece),
            pltpu.SemaphoreType.DMA(per_piece),
            pltpu.SemaphoreType.DMA((dp, tp, 2)),
        ],
        compiler_params=pltpu.CompilerParams(
            collective_id=collective_id, has_side_effects=True, vmem_limit_bytes=48 * 2**20),
        cost_estimate=pl.CostEstimate(flops=0, bytes_accessed=rows * cols * dp * tp * 8, transcendentals=0),
    )(x)


LANE = 128


def pad_up(n, m):
    return -(-n // m) * m


def dot_t(a, b):
    return lax.dot_general(a, b, (((1,), (1,)), ((), ())), preferred_element_type=jnp.float32)


def widen(tp, cols, wide, raw, padded, lead):
    block = 48
    blocks = raw.shape[-2] // block

    def body(i, carry):
        at = pl.ds(pl.multiple_of(i * block, 16), block)
        v = raw[lead + (at, slice(None))]
        for t in range(tp):
            part = v[:, t * cols:(t + 1) * cols]
            padded[lead + (at, pl.ds(t * wide, wide))] = jnp.concatenate(
                [part, jnp.zeros((block, wide - cols), v.dtype)], axis=1)
        return carry
    lax.fori_loop(0, blocks, body, 0)
    rest = padded.shape[-2] - raw.shape[-2]
    padded[lead + (pl.ds(raw.shape[-2], rest), slice(None))] = jnp.zeros((rest, tp * wide), padded.dtype)


def attend_part(
    tp, kv_heads, group_size, head_size, meet, meanwhile, res_buf,
    tok_ref, gain_ref, inverse_ref, pos_ref, sink_ref, wq_hbm, wkv_hbm, wo_hbm, cache_hbm,
    tok_buf, wq_buf, wkv_raw, wkv_wide, wkv_buf, wo_buf, cache_buf, q_rows, new_rows, pos_rows, att_rows,
    part_buf, got_buf, load_sem, send_sem, recv_tok, recv_part,
):
    dp_id = lax.axis_index("dp")
    me = lax.axis_index("tp")
    core, chip = lax.rem(me, CORES), me // CORES
    seq, cols = tok_ref.shape
    wide = res_buf.shape[1]
    window = cache_hbm.shape[2]
    heads = kv_heads * group_size
    twin_t = chip * CORES + 1 - core
    across_t = (1 - chip) * CORES + core
    corner_t = (1 - chip) * CORES + 1 - core
    twin, across = (dp_id, twin_t), (dp_id, across_t)

    loads = [
        pltpu.make_async_copy(src, dst, load_sem.at[i]) for i, (src, dst) in enumerate(
            [(wkv_hbm, wkv_raw), (wq_hbm, wq_buf), (cache_hbm, cache_buf), (wo_hbm, wo_buf)])
    ]
    for load in loads:
        load.start()
    own = pltpu.make_async_copy(tok_ref, tok_buf.at[me], load_sem.at[4])
    own.start()
    meet()

    def token_copy(src, t, i, target):
        return pltpu.make_async_remote_copy(
            src_ref=src, dst_ref=tok_buf.at[t], send_sem=send_sem.at[i], recv_sem=recv_tok.at[t],
            device_id=target, device_id_type=MESH)

    def token_arrived(t):
        token_copy(tok_buf.at[t], t, 0, twin).wait_recv()

    sent = [token_copy(tok_ref, me, 0, across), token_copy(tok_ref, me, 1, twin)]
    for copy in sent:
        copy.start()

    lanes = lax.broadcasted_iota(jnp.int32, (seq, LANE), 1)

    def column(row):
        n = row.shape[1]
        square = lax.broadcasted_iota(jnp.int32, (n, n), 0) == lax.broadcasted_iota(jnp.int32, (n, n), 1)
        return jnp.sum(jnp.where(square, row, 0.0), axis=1, keepdims=True)

    position = jnp.broadcast_to(column(pos_ref[...].astype(jnp.float32)), (seq, LANE))
    angles = position * inverse_ref[...]
    cosine = jnp.cos(angles)
    front = lax.rem(lanes, head_size) < head_size // 2
    sine = jnp.where(front, -jnp.sin(angles), jnp.sin(angles))
    for h in range(heads):
        pos_rows[pl.ds(h, seq, stride=heads), :] = position
    sink = jnp.broadcast_to(column(sink_ref[...]), (heads, LANE))
    sink = jnp.concatenate([sink] * 8, axis=0)

    loads[0].wait()
    kv_rows = wkv_raw.shape[0]
    step = kv_rows // 30

    def split(i, carry):
        at = pl.multiple_of(i * step, 16)
        wkv_wide[...] = wkv_raw[pl.ds(at, step), :].astype(jnp.float32)
        half = pl.ds(pl.multiple_of(i * (step // kv_heads), 16), step // kv_heads)
        for h in range(kv_heads):
            wkv_buf[half, h * LANE:(h + 1) * LANE] = wkv_wide[
                pl.ds(h, step // kv_heads, stride=kv_heads), :].astype(jnp.bfloat16)
        return carry
    lax.fori_loop(0, 30, split, 0)

    gains = gain_ref[...].reshape(1, tp * cols)
    loads[1].wait()

    def project(t):
        v = tok_buf[t].astype(jnp.float32)
        gain = gains[:, :cols]
        for i in range(1, tp):
            gain = jnp.where(t == i, gains[:, i * cols:(i + 1) * cols], gain)
        gained = (v * gain).astype(jnp.bfloat16)
        at = pl.ds(pl.multiple_of(t * cols, 16), cols)
        return (
            jnp.sum(v * v, axis=1, keepdims=True),
            jnp.dot(gained, wq_buf[at, :], preferred_element_type=jnp.float32),
            jnp.dot(gained, wkv_buf[at, :], preferred_element_type=jnp.float32))

    own.wait()
    token_arrived(twin_t)
    sums = [project(me), project(twin_t)]
    token_arrived(across_t)
    forward = token_copy(tok_buf.at[across_t], across_t, 2, twin)
    forward.start()
    sent.append(forward)
    sums.append(project(across_t))
    token_arrived(corner_t)
    sums.append(project(corner_t))
    squares, queries, fresh = [a + b + c + d for a, b, c, d in zip(*sums)]
    scale = lax.rsqrt(squares / (tp * cols) + norm_eps)
    queries, fresh = queries * scale, fresh * scale

    def turned(v):
        swapped = jnp.where(
            front, pltpu.roll(v, LANE - head_size // 2, 1), pltpu.roll(v, head_size // 2, 1))
        return v * cosine + swapped * sine

    def rounded(v):
        return v.astype(jnp.bfloat16).astype(jnp.float32)

    low = lanes < head_size
    for h in range(heads):
        if h % 2 == 0:
            pair = rounded(turned(queries[:, h // 2 * LANE:(h // 2 + 1) * LANE]))
        if h % group_size == 0:
            k = h // group_size
            entry = fresh[:, k * LANE:(k + 1) * LANE]
            entry = rounded(jnp.where(low, turned(entry), entry))
        own_q = pair if h % 2 == 0 else pltpu.roll(pair, head_size, 1)
        q_rows[pl.ds(h, seq, stride=heads), :] = jnp.where(low, own_q, 0.0)
        new_rows[pl.ds(h, seq, stride=heads), :] = entry

    loads[2].wait()
    batch = 8
    rows = batch * heads
    slot = lax.broadcasted_iota(jnp.int32, (rows, LANE), 1)
    upper = lax.broadcasted_iota(jnp.int32, (heads, LANE), 0) < group_size
    score_scale = head_size ** (-0.5)

    def attend(i, carry):
        at = pl.ds(pl.multiple_of(i * rows, rows), rows)
        q = q_rows[at, :]
        entry = new_rows[at, :]
        pos = pos_rows[at, :].astype(jnp.int32)
        raw = []
        for s in range(batch):
            qs = q[s * heads:(s + 1) * heads]
            lhs = jnp.concatenate(
                [jnp.where(upper, qs, 0.0), jnp.where(upper, 0.0, qs)], axis=1).astype(jnp.bfloat16)
            rhs = jnp.concatenate([cache_buf[i * batch + s, k] for k in range(kv_heads)], axis=1)
            raw.append(dot_t(lhs, rhs))
        scores = jnp.concatenate(raw, axis=0) * score_scale
        fresh_score = jnp.sum(q * entry, axis=1, keepdims=True) * score_scale
        current = slot == lax.rem(pos, window)
        scores = jnp.where(current, fresh_score, jnp.where(slot <= pos, scores, -jnp.inf))
        peak = jnp.maximum(jnp.max(scores, axis=1, keepdims=True), sink)
        raised = jnp.exp(scores - peak)
        denominator = jnp.sum(raised, axis=1, keepdims=True) + jnp.exp(sink - peak)
        probs = rounded(raised / denominator)
        fresh_prob = jnp.sum(jnp.where(current, probs, 0.0), axis=1, keepdims=True)
        probs = jnp.where(current, 0.0, probs)
        mixed = []
        for s in range(batch):
            lhs = probs[s * heads:(s + 1) * heads].astype(jnp.bfloat16)
            rhs = jnp.concatenate([cache_buf[i * batch + s, k] for k in range(kv_heads)], axis=1)
            both = jnp.dot(lhs, rhs, preferred_element_type=jnp.float32)
            mixed.append(jnp.where(upper, both[:, :LANE], both[:, LANE:]))
        att_rows[at, :] = jnp.concatenate(mixed, axis=0) + fresh_prob * entry
        return carry

    lax.fori_loop(0, seq // batch, attend, 0)

    tiles = []
    for j in range(heads // 2):
        even = att_rows[pl.ds(2 * j, seq, stride=heads), :]
        odd = att_rows[pl.ds(2 * j + 1, seq, stride=heads), :]
        tiles.append(jnp.where(low, pltpu.roll(even, head_size, 1), odd).astype(jnp.bfloat16))
    attended = jnp.concatenate(tiles, axis=1)
    loads[3].wait()

    def share(t):
        return dot_t(attended, wo_buf[pl.ds(pl.multiple_of(t * cols, 16), cols), :])

    def part_copy(i, target):
        return pltpu.make_async_remote_copy(
            src_ref=part_buf.at[i], dst_ref=got_buf.at[i], send_sem=send_sem.at[3 + i],
            recv_sem=recv_part.at[i], device_id=target, device_id_type=MESH)

    parts = [part_copy(0, twin), part_copy(1, across), part_copy(2, twin)]
    part_buf[0] = share(corner_t).astype(jnp.bfloat16)
    parts[0].start()
    far = share(across_t)
    parts[0].wait_recv()
    part_buf[1] = (far + got_buf[0].astype(jnp.float32)).astype(jnp.bfloat16)
    parts[1].start()
    part_buf[2] = share(twin_t).astype(jnp.bfloat16)
    parts[2].start()
    total = tok_ref[...].astype(jnp.float32) + share(me)
    meanwhile()
    parts[2].wait_recv()
    total = total + got_buf[2].astype(jnp.float32)
    parts[1].wait_recv()
    total = total + got_buf[1].astype(jnp.float32)
    res_buf[...] = jnp.concatenate([total, jnp.zeros((seq, wide - cols), jnp.float32)], axis=1)
    for copy in sent + parts:
        copy.wait_send()


def moe_part(
    dp, ny, tp, experts, cuts, full,
    res_ref, gain_ref, router_ref, ids_ref, wd_load, out_ref,
    rows_buf, gu_pad, wd_raw, wd_pad, act_buf, out_buf, back_buf,
    s_twin, s_x, s_y, s_z, r_rows, s_act, r_act, s_out, r_out,
):
    nz = dp // ny
    dp_id = lax.axis_index("dp")
    me = lax.axis_index("tp")
    core, chip = lax.rem(me, CORES), me // CORES
    z, y = dp_id // ny, lax.rem(dp_id, ny)
    seq, wide = res_ref.shape
    cols = out_ref.shape[1]
    twin_t = chip * CORES + 1 - core
    across_t = (1 - chip) * CORES + core
    corner_t = (1 - chip) * CORES + 1 - core
    twin, across = (dp_id, twin_t), (dp_id, across_t)
    y_peer = (z * ny + 1 - y, me)

    res = res_ref[...]
    gains = gain_ref[...].reshape(1, full)
    gain = gains[:, :cols]
    for t in range(1, tp):
        gain = jnp.where(me == t, gains[:, t * cols:(t + 1) * cols], gain)
    gained = res * jnp.concatenate([gain, jnp.zeros((1, wide - cols), jnp.float32)], axis=1)
    values = [jnp.sum(res * res, axis=1, keepdims=True)]
    router = jnp.concatenate(
        [router_ref[...].astype(jnp.float32), jnp.zeros((experts, wide - cols), jnp.float32)], axis=1)
    for e in range(experts):
        values.append(jnp.sum(gained * router[e:e + 1, :], axis=1, keepdims=True))
    tail = cols - (wide - LANE)
    lanes = lax.broadcasted_iota(jnp.int32, (seq, LANE), 1)
    group = (LANE - tail) // 3
    spread = jnp.zeros((seq, LANE), jnp.float32)
    for j, v in enumerate(values):
        for g in range(3):
            spread = jnp.where(lanes == tail + g * group + j, v, spread)
    high = spread.astype(jnp.bfloat16).astype(jnp.float32)
    middle = (spread - high).astype(jnp.bfloat16).astype(jnp.float32)
    low = spread - high - middle
    last = jnp.where(lanes < tail, gained[:, wide - LANE:], jnp.where(
        lanes < tail + group, high, jnp.where(lanes < tail + 2 * group, middle, low)))
    rows_buf[dp_id, me, :, :wide - LANE] = gained[:, :wide - LANE].astype(jnp.bfloat16)
    rows_buf[dp_id, me, :, wide - LANE:] = last.astype(jnp.bfloat16)

    share = seq // cuts

    def piece(b, t, h, sem, target):
        view = rows_buf.at[b, t, pl.ds(h * share, share)]
        return pltpu.make_async_remote_copy(
            src_ref=view, dst_ref=view, send_sem=sem, recv_sem=r_rows.at[b, t, h],
            device_id=target, device_id_type=MESH)

    def to_twin(b, t, h):
        return piece(b, t, h, s_twin.at[b, t, h], twin)

    def to_x(p, h):
        return piece(p * ny + y, me, h, s_x.at[p, h], across)

    def to_y(b, t, h):
        return piece(b, t, h, s_y.at[b, t // CORES, h], y_peer)

    def to_z(p, h):
        return piece(dp_id, me, h, s_z.at[p, h], (p * ny + y, me))

    def arrived(b, t, h):
        piece(b, t, h, r_rows.at[b, t, h], twin).wait_recv()

    def plane(k):
        return jnp.where(2 * z < nz, lax.rem(z + k, nz), lax.rem(z - k + nz, nz))

    for h in range(cuts):
        to_x(z, h).start()
        to_y(dp_id, me, h).start()
        to_twin(dp_id, me, h).start()

    def send_far(k, carry):
        for h in range(cuts):
            to_z(plane(k), h).start()
        return carry
    lax.fori_loop(1, nz, send_far, 0)

    def column_in(k, y_too):
        p = plane(k)
        for h in range(cuts):
            arrived(p * ny + y, me, h)
            to_x(p, h).start()
            if y_too:
                to_y(p * ny + y, me, h).start()
            to_twin(p * ny + y, me, h).start()

    def column_to_y(k):
        for h in range(cuts):
            to_y(plane(k) * ny + y, me, h).start()

    def across_in(k):
        b = plane(k) * ny + y
        for h in range(cuts):
            arrived(b, across_t, h)
            to_y(b, across_t, h).start()
            to_twin(b, across_t, h).start()

    column_in(1, True)
    for k in range(2, nz):
        column_in(k, False)
        across_in(k - 1)
        if k == 2:
            across_in(0)
        column_to_y(k)
        if k == 2:
            wd_load.wait()
            widen(tp, cols, wide, wd_raw, wd_pad, ())

    tile_n = 256
    n_tiles = wide // tile_n

    def act_copy(t, p, n, i, target):
        view = act_buf.at[t, p, n]
        return pltpu.make_async_remote_copy(
            src_ref=view, dst_ref=view, send_sem=s_act.at[i, p, n], recv_sem=r_act.at[t, p, n],
            device_id=target, device_id_type=MESH)

    def act_arrived(t, p, n):
        act_copy(t, p, n, 0, twin).wait_recv()

    def out_copy(b, n):
        return pltpu.make_async_remote_copy(
            src_ref=out_buf.at[b, n], dst_ref=back_buf.at[dp_id, n], send_sem=s_out.at[b, n],
            recv_sem=r_out.at[dp_id, n], device_id=(b, me), device_id_type=MESH)

    def stats_tile(b):
        total = rows_buf[b, 0, :, wide - LANE:].astype(jnp.float32)
        for t in range(1, tp):
            total = total + rows_buf[b, t, :, wide - LANE:].astype(jnp.float32)
        total = jnp.where(lanes >= tail, total, 0.0)
        return total

    def row_scale(total):
        hit = (lanes == tail) | (lanes == tail + group) | (lanes == tail + 2 * group)
        squares = jnp.sum(jnp.where(hit, total, 0.0), axis=1, keepdims=True)
        return lax.rsqrt(squares / full + norm_eps)

    def up_project(p):
        scale = jnp.concatenate([row_scale(stats_tile(p * ny + b)) for b in range(ny)], axis=0)

        def body(n, carry):
            at = pl.ds(pl.multiple_of(n * tile_n, tile_n), tile_n)
            lhs = jnp.concatenate([
                jnp.concatenate([rows_buf[p * ny + b, t] for t in range(tp)], axis=1)
                for b in range(ny)], axis=0)
            gate = dot_t(lhs, gu_pad[0, at, :]) * scale
            up = dot_t(lhs, gu_pad[1, at, :]) * scale
            act_buf[me, p, n] = (gate * jax.nn.sigmoid(glu_alpha * gate) * (up + 1.0)).astype(jnp.bfloat16)
            act_copy(me, p, n, 0, across).start()
            act_copy(me, p, n, 1, twin).start()
            return carry
        lax.fori_loop(0, n_tiles, body, 0)

    def down_project(p):
        def body(n, carry):
            at = pl.ds(pl.multiple_of(n * tile_n, tile_n), tile_n)
            lhs = jnp.concatenate([act_buf[t, p, i] for t in range(tp) for i in range(n_tiles)], axis=1)
            out = dot_t(lhs, wd_pad[at, :]).astype(jnp.bfloat16)
            for b in range(ny):
                out_buf[p * ny + b, n] = out[b * seq:(b + 1) * seq]
            for b in range(ny):
                @pl.when(p * ny + b != dp_id)
                def _():
                    out_copy(p * ny + b, n).start()

                @pl.when(p * ny + b == dp_id)
                def _():
                    back_buf[dp_id, n] = out[b * seq:(b + 1) * seq]
            return carry
        lax.fori_loop(0, n_tiles, body, 0)

    def stage(k, carry):
        @pl.when(k < nz)
        def _():
            p = plane(k + 1)
            for t in (me, across_t):
                b = p * ny + 1 - y
                for h in range(cuts):
                    arrived(b, t, h)
                    to_twin(b, t, h).start()
            for b in range(ny):
                for t in (twin_t, corner_t):
                    for h in range(cuts):
                        arrived(p * ny + b, t, h)
            up_project(p)

        @pl.when(k == 0)
        def _():
            across_in(nz - 1)

        @pl.when(k > 0)
        def _():
            p = plane(k)
            for n in range(n_tiles):
                act_arrived(across_t, p, n)
                act_copy(across_t, p, n, 2, twin).start()
            for n in range(n_tiles):
                act_arrived(twin_t, p, n)
                act_arrived(corner_t, p, n)
            down_project(p)
        return carry

    lax.fori_loop(0, nz + 1, stage, 0)

    total = stats_tile(dp_id)
    scale = row_scale(total)
    shift = LANE - group
    summed = total + pltpu.roll(total, shift, 1) + pltpu.roll(pltpu.roll(total, shift, 1), shift, 1)
    square = lax.broadcasted_iota(jnp.int32, (seq, seq), 0) == lax.broadcasted_iota(jnp.int32, (seq, seq), 1)
    chosen = lanes < 0
    for k in range(ids_ref.shape[0]):
        named = ids_ref[k:k + 1, :].astype(jnp.float32)
        named = jnp.sum(jnp.where(square, named, 0.0), axis=1, keepdims=True).astype(jnp.int32)
        chosen = chosen | (lanes == named + tail + 1)
    raised = jnp.where(chosen, jnp.exp(jnp.where(chosen, summed * scale, 0.0)), 0.0)
    weights = raised / jnp.sum(raised, axis=1, keepdims=True)

    out_ref[...] = res[:, :cols]

    def add_back(b, fetch):
        weight = jnp.sum(jnp.where(lanes == tail + 1 + b, weights, 0.0), axis=1, keepdims=True)
        for n in range(n_tiles):
            if fetch:
                view = back_buf.at[b, n]
                pltpu.make_async_remote_copy(
                    src_ref=view, dst_ref=view, send_sem=r_out.at[b, n], recv_sem=r_out.at[b, n],
                    device_id=twin, device_id_type=MESH).wait_recv()
            used = min(tile_n, cols - n * tile_n)
            at = slice(n * tile_n, n * tile_n + used)
            out_ref[:, at] = out_ref[:, at] + weight * back_buf[b, n].astype(jnp.float32)[:, :used]

    def add_far(i, carry):
        add_back(plane(1 + i // ny) * ny + lax.rem(i, ny), True)
        return carry

    add_back(dp_id, False)
    lax.fori_loop(0, dp - ny, add_far, 0)
    add_back(z * ny + 1 - y, True)

    def drain(p, carry):
        for h in range(cuts):
            to_x(p, h).wait_send()

            @pl.when(p != z)
            def _():
                to_z(p, h).wait_send()
            for t in (me, across_t):
                to_y(p * ny + y, t, h).wait_send()
                for b in range(ny):
                    to_twin(p * ny + b, t, h).wait_send()
        return carry
    lax.fori_loop(0, nz, drain, 0)
    def drain_acts(p, carry):
        for n in range(n_tiles):
            act_copy(me, p, n, 0, across).wait_send()
            act_copy(me, p, n, 1, twin).wait_send()
            act_copy(across_t, p, n, 2, twin).wait_send()
        return carry
    lax.fori_loop(0, nz, drain_acts, 0)

    def drain_outs(d, carry):
        for n in range(n_tiles):
            out_copy(lax.rem(dp_id + d, dp), n).wait_send()
        return carry
    lax.fori_loop(1, dp, drain_outs, 0)


def layer_kernel(
    dp, ny, tp, experts, cuts, kv_heads, group_size, head_size,
    tok_ref, gain_ref, inverse_ref, pos_ref, sink_ref, moe_gain_ref, router_ref, ids_ref,
    wq_hbm, wkv_hbm, wo_hbm, cache_hbm, gu_hbm, wd_hbm, out_ref, *scratch,
):
    res_buf, gu_raw, wd_raw, load_sem = scratch[:4]
    attend_scratch, (rows_buf, gu_pad, wd_pad, *rest) = scratch[4:21], scratch[21:]
    dp_id, me = lax.axis_index("dp"), lax.axis_index("tp")
    core, chip = lax.rem(me, CORES), me // CORES
    cols, full = gu_hbm.shape[1:]
    wide = res_buf.shape[1]
    gu_load = pltpu.make_async_copy(gu_hbm, gu_raw, load_sem.at[0])
    wd_load = pltpu.make_async_copy(wd_hbm, wd_raw, load_sem.at[1])

    def meet():
        gu_load.start()
        wd_load.start()
        near = [(dp_id, chip * CORES + 1 - core), (dp_id, (1 - chip) * CORES + core)]
        greet(near + [(lax.rem(dp_id + d, dp), me) for d in range(1, dp)])

    def meanwhile():
        gu_load.wait()
        for half in range(2):
            widen(tp, cols, wide, gu_raw, gu_pad, (half,))

    attend_part(
        tp, kv_heads, group_size, head_size, meet, meanwhile, res_buf,
        tok_ref, gain_ref, inverse_ref, pos_ref, sink_ref, wq_hbm, wkv_hbm, wo_hbm, cache_hbm, *attend_scratch)
    moe_part(
        dp, ny, tp, experts, cuts, full, res_buf, moe_gain_ref, router_ref, ids_ref, wd_load, out_ref,
        rows_buf, gu_pad, wd_raw, wd_pad, *rest)


def layer(tokens, gain, positions, sinks, moe_gain, router, ids, w_query, w_keyvalue, w_out, cache, gate_up, w_down, dp, ny, tp):
    seq, cols = tokens.shape
    wide = pad_up(cols, 256)
    full = tp * cols
    kv_heads, window, entry = cache.shape[1:]
    head_size = entry // 2
    heads = w_query.shape[1] // head_size
    exponent = np.arange(LANE) % (head_size // 2) * (2.0 / head_size)
    inverse = jnp.asarray(rope_base ** -exponent, jnp.float32)[None, :]
    nz, cuts, tiles = dp // ny, 2, wide // 256
    bf, f32 = jnp.bfloat16, jnp.float32
    dma, vmem = pltpu.SemaphoreType.DMA, pltpu.VMEM
    return pl.pallas_call(
        functools.partial(
            layer_kernel, dp, ny, tp, router.shape[0], cuts, kv_heads, heads // kv_heads, head_size),
        out_shape=jax.ShapeDtypeStruct((seq, cols), f32),
        in_specs=[pl.BlockSpec(memory_space=pltpu.VMEM)] * 8 + [pl.BlockSpec(memory_space=pl.ANY)] * 6,
        out_specs=pl.BlockSpec(memory_space=pltpu.VMEM),
        scratch_shapes=[
            vmem((seq, wide), f32), vmem((2, cols, full), bf), vmem((cols, full), bf), dma((2,)),
            vmem((tp, seq, cols), bf), vmem(w_query.shape, bf), vmem((full * kv_heads, LANE), bf),
            vmem((full * kv_heads // 30, LANE), f32), vmem((full, kv_heads * LANE), bf),
            vmem((full, heads * head_size), bf), vmem(cache.shape, bf),
            vmem((seq * heads, LANE), f32), vmem((seq * heads, LANE), f32),
            vmem((seq * heads, LANE), f32), vmem((seq * heads, LANE), f32),
            vmem((3, seq, cols), bf), vmem((3, seq, cols), bf),
            dma((5,)), dma((6,)), dma((tp,)), dma((3,)),
            vmem((dp, tp, seq, wide), bf), vmem((2, wide, tp * wide), bf), vmem((wide, tp * wide), bf),
            vmem((tp, nz, tiles, ny * seq, 256), bf),
            vmem((dp, tiles, seq, 256), bf), vmem((dp, tiles, seq, 256), bf),
            dma((dp, tp, cuts)), dma((nz, cuts)), dma((dp, tp // CORES, cuts)),
            dma((nz, cuts)), dma((dp, tp, cuts)),
            dma((3, nz, tiles)), dma((tp, nz, tiles)), dma((dp, tiles)), dma((dp, tiles)),
        ],
        compiler_params=pltpu.CompilerParams(
            collective_id=0, has_side_effects=True, vmem_limit_bytes=67_000_000),
        cost_estimate=pl.CostEstimate(
            flops=6 * dp * seq * full * cols, bytes_accessed=6 * full * cols, transcendentals=0),
    )(tokens, gain, inverse, positions[None, :], sinks[None, :], moe_gain, router, ids,
      w_query, w_keyvalue.reshape(full * kv_heads, LANE), w_out.T, cache, gate_up, w_down)


def activate(mixed_in, ff_local):
    gate_part = mixed_in[..., :ff_local]
    up_part = mixed_in[..., ff_local:]
    return (gate_part * jax.nn.sigmoid(glu_alpha * gate_part) * (up_part + 1.0)).astype(
        jnp.bfloat16
    )


def on_device(
    tokens,
    attn_gain,
    w_query,
    w_keyvalue,
    attn_sinks,
    w_out,
    window_cache,
    positions,
    moe_gain,
    router,
    gate_up,
    w_down,
    expert_ids,
):
    tp_count = lax.axis_size("tp")
    dp_count = lax.axis_size("dp")
    seq_count, col_count = tokens.shape
    full_width = col_count * tp_count
    col_start = lax.axis_index("tp") * col_count
    head_size = w_keyvalue.shape[2] // 2
    kv_local = w_keyvalue.shape[1]
    q_local = w_query.shape[1] // head_size
    group_size = q_local // kv_local
    window = window_cache.shape[2]
    ny = 2 ** (int(math.log2(dp_count)) // 2)
    if (tp_count, ny, gate_up.shape[0], kv_local, group_size, window, 2 * head_size) == (
            2 * CORES, 2, 1, 2, 4, LANE, LANE) and dp_count > 2 * ny:
        return layer(
            tokens, attn_gain, positions, attn_sinks, moe_gain, router.T, expert_ids.T, w_query, w_keyvalue,
            w_out, window_cache, jnp.transpose(gate_up[0], (1, 2, 0)), w_down[0].T, dp_count, ny, tp_count)
    moe_slice = lax.dynamic_slice_in_dim(moe_gain, col_start, col_count)
    tok_wide = tokens.astype(jnp.float32)
    kv_flat = w_keyvalue.reshape(full_width, kv_local * 2 * head_size)
    whole_rows = feature_gather(tokens, tp_count, 2, 0).astype(jnp.float32)
    attn_sq = jnp.sum(whole_rows * whole_rows, axis=1, keepdims=True)
    piece_rows = (
        whole_rows * lax.rsqrt(attn_sq / full_width + norm_eps) * attn_gain[None, :]
    ).astype(jnp.bfloat16)
    queries = jnp.dot(piece_rows, w_query, preferred_element_type=jnp.float32)
    fresh_rows = jnp.dot(piece_rows, kv_flat, preferred_element_type=jnp.float32)
    cosine, sine_table = rope_tables(positions, head_size)
    rot_queries = rotate(
        queries.reshape(seq_count, q_local, head_size), cosine[:, None, :], sine_table[:, None, :]
    ).astype(jnp.bfloat16)
    fresh_rows = fresh_rows.reshape(seq_count, kv_local, 2 * head_size)
    new_key = rotate(fresh_rows[..., :head_size], cosine[:, None, :], sine_table[:, None, :])
    new_entry = jnp.concatenate([new_key, fresh_rows[..., head_size:]], axis=-1).astype(
        jnp.bfloat16
    )
    slot_ids = jnp.arange(window, dtype=jnp.int32)
    is_current = slot_ids[None, :] == (positions % window)[:, None]
    is_valid = (positions[:, None] - slot_ids[None, :]) % window <= positions[:, None]
    is_valid = is_valid & ~is_current
    grouped = rot_queries.reshape(seq_count, kv_local, group_size, head_size)
    scores = jnp.einsum(
        "skgh,skwh->skgw", grouped, window_cache[..., :head_size], preferred_element_type=jnp.float32
    ) * head_size ** (-0.5)
    scores = jnp.where(is_valid[:, None, None, :], scores, -jnp.inf)
    new_wide = new_entry.astype(jnp.float32)[:, :, None, :]
    new_score = jnp.sum(
        grouped.astype(jnp.float32) * new_wide[..., :head_size], axis=-1, keepdims=True
    ) * head_size ** (-0.5)
    sink_col = attn_sinks.reshape(kv_local, group_size)[None, :, :, None]
    peak_score = jnp.maximum(
        jnp.maximum(jnp.max(scores, axis=-1, keepdims=True), new_score), sink_col
    )
    raised = jnp.exp(scores - peak_score)
    raised_new = jnp.exp(new_score - peak_score)
    denominator = (
        jnp.sum(raised, axis=-1, keepdims=True) + raised_new + jnp.exp(sink_col - peak_score)
    )
    prob_bf = (raised / denominator).astype(jnp.bfloat16)
    prob_new = (raised_new / denominator).astype(jnp.bfloat16).astype(jnp.float32)
    attended = jnp.einsum(
        "skgw,skwh->skgh", prob_bf, window_cache[..., head_size:], preferred_element_type=jnp.float32
    )
    attended = (attended + prob_new * new_wide[..., head_size:]).astype(jnp.bfloat16)
    partial_out = jnp.einsum(
        "sh,htc->tsc",
        attended.reshape(seq_count, q_local * head_size),
        w_out.reshape(q_local * head_size, tp_count, col_count),
        preferred_element_type=jnp.float32,
    ).astype(jnp.bfloat16)
    residual = tok_wide + share_sum(partial_out, tp_count, True, 2)
    experts = router.shape[1]
    top_count = expert_ids.shape[1]
    local_experts = gate_up.shape[0]
    ff_local = gate_up.shape[3]
    capacity = min(seq_count, max(2, 8 * seq_count * top_count // (3 * experts)))
    moe_sq = jnp.sum(residual * residual, axis=1)
    router_wide = router.astype(jnp.float32)
    gained = residual * moe_slice[None, :]
    raw_logits = jnp.dot(gained, router_wide, precision=lax.Precision.HIGHEST)
    stats = share_sum(
        jnp.concatenate([moe_sq[:, None], raw_logits], axis=1)[None], tp_count, False, 3
    )
    moe_scale = lax.rsqrt(stats[:, :1] / full_width + norm_eps)
    logits = stats[:, 1:] * moe_scale
    hidden_rows = (gained * moe_scale).astype(jnp.bfloat16)
    expert_iota = jnp.arange(experts, dtype=jnp.int32)
    chosen = expert_ids[:, :, None] == expert_iota[None, None, :]
    picked = jnp.sum(jnp.where(chosen, logits[:, None, :], 0.0), axis=-1)
    raised_logits = jnp.exp(picked)
    route_weights = raised_logits / jnp.sum(raised_logits, axis=1, keepdims=True)
    gate_up_flat = gate_up.reshape(local_experts, full_width, 2 * ff_local)
    if capacity >= seq_count:
        token_weights = jnp.sum(jnp.where(chosen, route_weights[:, :, None], 0.0), axis=1)
        all_rows = full_gather(hidden_rows, dp_count, tp_count, 1)
        half = seq_count // 2
        part = dp_count * half
        acts = [
            activate(
                jnp.dot(all_rows, gate_up_flat[e], preferred_element_type=jnp.float32), ff_local
            )
            for e in range(local_experts)
        ]
        pieces = []
        for h in range(2):
            outs = []
            for e in range(local_experts):
                act_all = feature_gather(
                    acts[e][h * part : (h + 1) * part], tp_count, dp_count // 2, 4 + 2 * e + h
                )
                out = jnp.dot(act_all, w_down[e], preferred_element_type=jnp.float32)
                outs.append(out.astype(jnp.bfloat16).reshape(dp_count, half, col_count))
            returned = lax.all_to_all(
                jnp.stack(outs, axis=1), "dp", split_axis=0, concat_axis=0, tiled=True
            )
            back = returned.reshape(experts, half, col_count)
            mine = slice(h * half, (h + 1) * half)
            total = residual[mine]
            for e in range(experts):
                total = total + token_weights[mine, e : e + 1] * back[e].astype(jnp.float32)
            pieces.append(total)
        total = jnp.concatenate(pieces, axis=0)
        return total
    assign = expert_ids.reshape(-1)
    onehot = (assign[:, None] == expert_iota[None, :]).astype(jnp.int32)
    earlier = jnp.cumsum(onehot, axis=0) - onehot
    slot_of = jnp.sum(earlier * onehot, axis=1)
    target = (assign * capacity + slot_of).reshape(seq_count, top_count)
    spot_ids = jnp.arange(experts * capacity, dtype=jnp.int32)
    slot_hits = target[:, :, None] == spot_ids[None, None, :]
    placer = jnp.transpose(jnp.any(slot_hits, axis=1)).astype(jnp.bfloat16)
    combiner = jnp.sum(jnp.where(slot_hits, route_weights[:, :, None], 0.0), axis=1)
    placed = jnp.dot(placer, hidden_rows, preferred_element_type=jnp.float32).astype(jnp.bfloat16)
    mixed_in = jnp.einsum(
        "gecd,edf->gecf",
        lax.all_gather(
            lax.all_to_all(
                placed.reshape(dp_count, local_experts, capacity, hidden_rows.shape[1]),
                "dp",
                split_axis=0,
                concat_axis=0,
                tiled=True,
            ),
            "tp",
            axis=3,
            tiled=True,
        ),
        gate_up_flat,
        preferred_element_type=jnp.float32,
    )
    act_rows = activate(mixed_in, ff_local)
    answered = jnp.einsum(
        "gecf,efd->gecd",
        lax.all_gather(act_rows, "tp", axis=3, tiled=True),
        w_down,
        preferred_element_type=jnp.float32,
    ).astype(jnp.bfloat16)
    returned = lax.all_to_all(answered, "dp", split_axis=0, concat_axis=0, tiled=True)
    flat_back = returned.reshape(experts * capacity, col_count).astype(jnp.float32)
    moe_out = jnp.dot(combiner, flat_back, precision=lax.Precision.HIGHEST)
    return residual + moe_out


def solution(mesh):
    in_specs = (
        P("dp", "tp"),
        P(),
        P(None, "tp"),
        P(None, "tp", None),
        P("tp"),
        P("tp", None),
        P("dp", "tp", None, None),
        P("dp"),
        P(),
        P("tp", None),
        P("dp", None, None, "tp"),
        P("dp", None, "tp"),
        P("dp", None),
    )
    out_specs = P("dp", "tp")
    return jax.shard_map(
        on_device, mesh=mesh, in_specs=in_specs, out_specs=out_specs, check_vma=False
    )
```
